16 devices in a mesh: mp: 2 (over y, z), dp: 8 (over x, core).
Axes of the slice: x: 4, y: 2, z: 1, core: 2. Of those that a mesh axis runs over, the one named last changes fastest.
The devices are a block of a 4x4x8 slice.
Arguments:
- grad_partial: float32 [16, 1, 2048, 7168], P(('mp', 'dp')), parts along dimension 0
- momentum: float32 [2, 2048, 7168], P('mp', 'dp'), parts along dimension 0
- weight: float32 [2, 2048, 7168], P('mp', 'dp'), parts along dimension 0
Outputs:
- output 1: float32 [2, 2048, 7168], P('mp', 'dp'), parts along dimension 0
- output 2: float32 [2, 2048, 7168], P('mp', 'dp'), parts along dimension 0
- output 3: bfloat16 [2, 2048, 7168], P('mp'), parts along dimension 0
There are 2 independent parts. The reference program is written for one: setup_inputs(seed, part) draws one part's arguments, and reference() takes and returns one part's arrays. A program takes and returns all parts, laid end to end along the dimension named above; each array names one.
All inputs are finite; a program needn't handle non-finite values.
Results may differ from the reference program's by a relative error of at most 0.0174769.
Values are sent between devices in bfloat16 or wider.
A program may use at most 768 MiB of HBM per device.

```python
import math
import jax
import jax.numpy as jnp
from jax import lax

GROUP_SIZE = 8
NUM_MATS = 1
MAT_ROWS = 2048
MAT_COLS = 7168
NS_STEPS = 5
MOMENTUM = 0.95
LEARN_RATE = 2.0
WEIGHT_DECAY = 0.25
COEF_A = 3.4445
COEF_B = -4.7750
COEF_C = 2.0315


def setup_inputs(seed: int = 0, part: int = 0) -> dict:
    part_key = jax.random.fold_in(jax.random.key(seed), part)
    key_grad, key_moment, key_weight = jax.random.split(part_key, 3)
    mat_shape = (NUM_MATS, MAT_ROWS, MAT_COLS)
    grad_partial = jax.random.normal(key_grad, (GROUP_SIZE,) + mat_shape, jnp.float32) * math.sqrt(GROUP_SIZE)
    momentum = jax.random.normal(key_moment, mat_shape, jnp.float32)
    weight = jax.random.normal(key_weight, mat_shape, jnp.float32)
    return {'grad_partial': grad_partial, 'momentum': momentum, 'weight': weight}


def newton_schulz(direction):
    num_rows, num_cols = direction.shape
    as_float = direction.astype(jnp.float32)
    norm = jnp.sqrt(jnp.sum(as_float * as_float))
    ortho = (as_float / (norm + 1e-7)).astype(jnp.bfloat16)
    if num_rows > num_cols:
        ortho = ortho.T
    for _ in range(NS_STEPS):
        gram = jnp.dot(ortho, ortho.T, preferred_element_type=jnp.float32).astype(jnp.bfloat16)
        gram_sq = jnp.dot(gram, gram, preferred_element_type=jnp.float32)
        poly = (COEF_B * gram.astype(jnp.float32) + COEF_C * gram_sq).astype(jnp.bfloat16)
        ortho = (COEF_A * ortho.astype(jnp.float32) + jnp.dot(poly, ortho, preferred_element_type=jnp.float32)).astype(jnp.bfloat16)
    if num_rows > num_cols:
        ortho = ortho.T
    return ortho


def reference(grad_partial, momentum, weight):
    grad = jnp.sum(grad_partial, axis=0) / GROUP_SIZE
    new_momentum = MOMENTUM * momentum + grad
    direction = (grad + MOMENTUM * new_momentum).astype(jnp.bfloat16)
    ortho = lax.map(newton_schulz, direction)
    scale = 0.2 * math.sqrt(max(MAT_ROWS, MAT_COLS))
    new_weight = weight - LEARN_RATE * (scale * ortho.astype(jnp.float32) + WEIGHT_DECAY * weight)
    return new_momentum, new_weight, new_weight.astype(jnp.bfloat16)
```

```python
import math
import jax
import jax.numpy as jnp
from jax import lax
from jax.experimental import pallas as pl
from jax.experimental.pallas import tpu as pltpu
from jax.sharding import PartitionSpec as P

MOMENTUM = 0.95
LEARN_RATE = 2.0
WEIGHT_DECAY = 0.25
NS_STEPS = 5
COEF_A = 3.4445
COEF_B = -4.7750
COEF_C = 2.0315

MESH = pl.DeviceIdType.MESH
F32, BF16 = jnp.float32, jnp.bfloat16
CORES = 2
BLOCK = 512
CHUNK = 512
BLOCKS = (((0, 0), (2, 0), (1, 1), (3, 1), (3, 3)), ((1, 0), (3, 0), (2, 1), (2, 2), (3, 2)))


def lookup(index, values):
    packed = 0
    for place, value in enumerate(values):
        packed += value * 4 ** place
    result = jnp.int32(values[0])
    for place, value in enumerate(values[1:], 1):
        result = jnp.where(index == place, jnp.int32(value), result)
    return result


def block_of(core, index):
    row = jnp.where(core == 0, lookup(index, [b[0] for b in BLOCKS[0]]), lookup(index, [b[0] for b in BLOCKS[1]]))
    col = jnp.where(core == 0, lookup(index, [b[1] for b in BLOCKS[0]]), lookup(index, [b[1] for b in BLOCKS[1]]))
    return row, col


def span(index, size):
    return pl.ds(pl.multiple_of(index * size, size), size)


def newton_schulz(group, rows, half, scale, u_ref, sq_ref, w_ref, wb_ref, xrow_ref, wcol_ref,
                  x_ref, gram, poly, part_out, part_in, w_tile, o_tile, norm_buf,
                  load_sem, part_send, part_recv, gram_send, gram_recv, poly_send, poly_recv,
                  w_send, w_recv, w_fwd_send, w_fwd_recv, tile_sem, out_sem, out_send, out_recv, row_sem, row_send, row_recv):
    me = lax.axis_index('dp')
    core, chip = lax.rem(me, CORES), me // CORES
    chips = group // CORES
    slab = rows // group
    partner = chip * CORES + (1 - core)
    right_chip, left_chip = lax.rem(chip + 1, chips), lax.rem(chip + chips - 1, chips)
    num_chunks = half // CHUNK
    slots = num_chunks + 1

    def remote(src, dst, send, recv, device):
        return pltpu.make_async_remote_copy(src, dst, send, recv, device_id={'dp': device}, device_id_type=MESH)

    barrier = pltpu.get_barrier_semaphore()
    peers = [partner] + [c * CORES + h for c in (right_chip, left_chip) for h in range(CORES)]
    for peer in peers:
        pl.semaphore_signal(barrier, inc=1, device_id={'dp': peer}, device_id_type=MESH)
    pl.semaphore_wait(barrier, len(peers))

    piece = slab // 2

    def w_first(side, h, part):
        to_chip = right_chip if side == 0 else left_chip
        row0 = me * slab + part * piece
        return remote(w_ref.at[pl.ds(part * piece, piece), pl.ds(h * half, half)],
                      wcol_ref.at[pl.ds(pl.multiple_of(row0, piece), piece), :],
                      w_send.at[side, h, part], w_recv.at[side, core, part], to_chip * CORES + h)

    def w_first_arrival(side, from_core, part):
        from_chip = left_chip if side == 0 else right_chip
        row0 = (from_chip * CORES + from_core) * slab + part * piece
        where = wcol_ref.at[pl.ds(pl.multiple_of(row0, piece), piece), :]
        return remote(where, where, w_send.at[side, 0, part], w_recv.at[side, from_core, part], partner)

    def w_forward(side, from_core):
        from_chip = left_chip if side == 0 else right_chip
        to_chip = right_chip if side == 0 else left_chip
        row0 = (from_chip * CORES + from_core) * slab + side * piece
        where = wcol_ref.at[pl.ds(pl.multiple_of(row0, piece), piece), :]
        return remote(where, where, w_fwd_send.at[side, from_core], w_fwd_recv.at[side, from_core], to_chip * CORES + core)

    def w_pair():
        return remote(w_ref.at[:, pl.ds(pl.multiple_of((1 - core) * half, half), half)],
                      wcol_ref.at[span(me, slab), :], tile_sem.at[3], tile_sem.at[4], partner)

    def w_own():
        return pltpu.make_async_copy(w_ref.at[:, pl.ds(pl.multiple_of(core * half, half), half)],
                                     wcol_ref.at[span(me, slab), :], tile_sem.at[2])

    loads = [pltpu.make_async_copy(u_ref.at[:, pl.ds(pl.multiple_of(core * half + c * CHUNK, CHUNK), CHUNK)], x_ref.at[c], load_sem.at[c])
             for c in range(num_chunks)]
    norm_load = pltpu.make_async_copy(sq_ref, norm_buf, load_sem.at[num_chunks])
    norm_load.start()
    for load in loads:
        load.start()
    for part in (0, 1):
        for side in (0, 1):
            for h in range(CORES):
                w_first(side, h, part if side == 0 else 1 - part).start()
    w_pair().start()
    w_own().start()
    norm_load.wait()
    inverse = 1.0 / (jnp.sqrt(norm_buf[0:1, 0:1]) + 1e-7)
    for c in range(num_chunks):
        loads[c].wait()

        def scale_rows(i, _, c=c):
            r = span(i, 256)
            x_ref[c, r, :] = (x_ref[c, r, :].astype(F32) * inverse).astype(BF16)
            return 0
        lax.fori_loop(0, rows // 256, scale_rows, 0)

    def slot_of(c, t):
        return lax.rem(c + 2 * slots - t, slots)

    def gram_send_copy(b, index, row, col):
        return remote(gram.at[span(row, BLOCK), span(col, BLOCK)], gram.at[span(row, BLOCK), span(col, BLOCK)],
                      gram_send.at[index, b], gram_recv.at[index, b], partner)

    def poly_send_copy(b, index, row, col):
        return remote(poly.at[span(row, BLOCK), span(col, BLOCK)], poly.at[span(row, BLOCK), span(col, BLOCK)],
                      poly_send.at[index, b], poly_recv.at[index, b], partner)

    def both(copy, owner, index, act):
        row, col = block_of(owner, index)
        act(copy(0, index, row, col))

        @pl.when(row != col)
        def _():
            act(copy(1, index, col, row))

    def part_copy(index):
        return remote(part_out.at[index], part_in.at[index], part_send.at[index], part_recv.at[index], partner)

    def step(t, _):
        def gram_block(row, col):
            ri, rj = span(row, BLOCK), span(col, BLOCK)
            xi = jnp.concatenate([x_ref[slot_of(c, t), ri, :] for c in range(num_chunks)], axis=1)
            xj = jnp.concatenate([x_ref[slot_of(c, t), rj, :] for c in range(num_chunks)], axis=1)
            return lax.dot_general(xi, xj, (((1,), (1,)), ((), ())), preferred_element_type=F32)

        @pl.when(t == 2)
        def _():
            for side in (0, 1):
                for from_core in range(CORES):
                    w_first_arrival(side, from_core, side).wait_recv()
                    w_forward(side, from_core).start()

        def gram_step(index, _):
            owner = jnp.where(index < 5, 1 - core, core)
            place = lax.rem(index, 5)
            row, col = block_of(owner, place)
            value = gram_block(row, col)

            @pl.when(index < 5)
            def _():
                part_out[place] = value
                part_copy(place).start()

            @pl.when(index >= 5)
            def _():
                part_copy(place).wait_recv()
                block = (value + part_in[place]).astype(BF16)
                gram[span(row, BLOCK), span(col, BLOCK)] = block

                @pl.when(row != col)
                def _():
                    gram[span(col, BLOCK), span(row, BLOCK)] = block.T
                both(gram_send_copy, core, place, lambda cp: cp.start())
            return 0
        lax.fori_loop(0, 10, gram_step, 0)

        def poly_step(index, _):
            @pl.when(index == 0)
            def _():
                for i in range(4):
                    both(gram_send_copy, 1 - core, i, lambda cp: cp.wait_recv())

            @pl.when(index == 1)
            def _():
                both(gram_send_copy, 1 - core, 4, lambda cp: cp.wait_recv())
            row, col = block_of(core, index)
            ri, rj = span(row, BLOCK), span(col, BLOCK)
            square = jnp.dot(gram[ri, :], gram[:, rj], preferred_element_type=F32)
            block = (COEF_B * gram[ri, rj].astype(F32) + COEF_C * square).astype(BF16)
            poly[ri, rj] = block

            @pl.when(row != col)
            def _():
                poly[rj, ri] = block.T
            both(poly_send_copy, core, index, lambda cp: cp.start())
            return 0
        lax.fori_loop(0, 5, poly_step, 0)

        tall = 1024

        def poly_waits(q):
            @pl.when(q == 0)
            def _():
                for i in range(4):
                    both(poly_send_copy, 1 - core, i, lambda cp: cp.wait_recv())

            @pl.when(q == 1)
            def _():
                both(poly_send_copy, 1 - core, 4, lambda cp: cp.wait_recv())

        def apply_block(q):
            c, m = q // 2, lax.rem(q, 2)
            rm = span(m, tall)
            src, dst = slot_of(c, t), slot_of(c, t + 1)
            total = jnp.dot(poly[rm, :], x_ref[src], preferred_element_type=F32)
            return c, m, rm, dst, (COEF_A * x_ref[src, rm, :].astype(F32) + total).astype(BF16)

        @pl.when(t < NS_STEPS - 1)
        def _():
            def apply_step(q, _):
                poly_waits(q)
                c, m, rm, dst, value = apply_block(q)
                x_ref[dst, rm, :] = value
                return 0
            lax.fori_loop(0, 2 * num_chunks, apply_step, 0)

        @pl.when(t == NS_STEPS - 1)
        def _():
            for side in (0, 1):
                for from_core in range(CORES):
                    w_first_arrival(side, from_core, 1 - side).wait_recv()
                    w_forward(side, from_core).wait_recv()
            w_pair().wait_recv()
            w_own().wait()

            def tile_load(q):
                c, m = q // 2, lax.rem(q, 2)
                return pltpu.make_async_copy(wcol_ref.at[span(m, tall), span(c, CHUNK)], w_tile.at[lax.rem(q, 2)], tile_sem.at[lax.rem(q, 2)])

            def out_pair(q, slot):
                c, m = q // 2, lax.rem(q, 2)
                where = wb_ref.at[span(m, tall), pl.ds(pl.multiple_of(core * half + c * CHUNK, CHUNK), CHUNK)]
                return (pltpu.make_async_copy(o_tile.at[slot], where, out_sem.at[slot]),
                        remote(o_tile.at[slot], where, out_send.at[slot], out_recv.at[q], partner))

            def row_pair(c):
                slot = slot_of(c, t + 1)
                cols = pl.ds(pl.multiple_of(core * half + c * CHUNK, CHUNK), CHUNK)
                return (pltpu.make_async_copy(x_ref.at[slot, span(me, slab), :], xrow_ref.at[:, cols], row_sem.at[c]),
                        remote(x_ref.at[slot, span(partner, slab), :], xrow_ref.at[:, cols], row_send.at[c], row_recv.at[c], partner))

            tile_load(0).start()

            def last_step(q, _):
                poly_waits(q)

                @pl.when(q + 1 < 2 * num_chunks)
                def _():
                    tile_load(q + 1).start()
                c, m, rm, dst, value = apply_block(q)
                x_ref[dst, rm, :] = value
                slot = lax.rem(q, 2)
                tile_load(q).wait()

                @pl.when(q >= 2)
                def _():
                    here, there = out_pair(q - 2, slot)
                    here.wait()
                    there.wait_send()
                old = w_tile[slot]
                new = old - LEARN_RATE * (scale * value.astype(F32) + WEIGHT_DECAY * old)
                o_tile[slot] = new.astype(BF16)
                here, there = out_pair(q, slot)
                here.start()
                there.start()

                @pl.when(m == 1)
                def _():
                    here, there = row_pair(c)
                    here.start()
                    there.start()
                return 0
            lax.fori_loop(0, 2 * num_chunks, last_step, 0)
            for q in (2 * num_chunks - 2, 2 * num_chunks - 1):
                here, there = out_pair(q, q % 2)
                here.wait()
                there.wait_send()

            def out_arrival(q, _):
                c, m = q // 2, lax.rem(q, 2)
                where = wb_ref.at[span(m, tall), pl.ds(pl.multiple_of((1 - core) * half + c * CHUNK, CHUNK), CHUNK)]
                remote(o_tile.at[0], where, out_send.at[0], out_recv.at[q], partner).wait_recv()
                return 0
            lax.fori_loop(0, 2 * num_chunks, out_arrival, 0)

            def row_end(c, _):
                here, there = row_pair(c)
                here.wait()
                there.wait()
                return 0
            lax.fori_loop(0, num_chunks, row_end, 0)

        def drain(i, _):
            part_copy(i).wait_send()
            both(gram_send_copy, core, i, lambda cp: cp.wait_send())
            both(poly_send_copy, core, i, lambda cp: cp.wait_send())
            return 0
        lax.fori_loop(0, 5, drain, 0)
        return 0
    lax.fori_loop(0, NS_STEPS, step, 0)

    for part in (0, 1):
        for side in (0, 1):
            for h in range(CORES):
                w_first(side, h, part).wait_send()
    for side in (0, 1):
        for from_core in range(CORES):
            w_forward(side, from_core).wait_send()
    w_pair().wait_send()


def solution(mesh):
    group = mesh.shape['dp']

    def orthogonal_update(direction, sq_norm, weight):
        slab, num_cols = weight.shape
        rows = slab * group
        half = num_cols // CORES
        scale = 0.2 * math.sqrt(max(rows, num_cols))
        num_chunks = half // CHUNK
        anywhere = pl.BlockSpec(memory_space=pl.ANY)
        dma = pltpu.SemaphoreType.DMA

        def kernel(*refs):
            newton_schulz(group, rows, half, scale, *refs)
        shape = jax.ShapeDtypeStruct
        return pl.pallas_call(
            kernel,
            name='newton_schulz',
            out_shape=(shape((rows, num_cols), BF16), shape((slab, num_cols), BF16), shape((rows, half), F32)),
            in_specs=[anywhere] * 3,
            out_specs=(anywhere,) * 3,
            scratch_shapes=[
                pltpu.VMEM((num_chunks + 1, rows, CHUNK), BF16),
                pltpu.VMEM((rows, rows), BF16),
                pltpu.VMEM((rows, rows), BF16),
                pltpu.VMEM((5, BLOCK, BLOCK), F32),
                pltpu.VMEM((5, BLOCK, BLOCK), F32),
                pltpu.VMEM((2, 1024, CHUNK), F32),
                pltpu.VMEM((2, 1024, CHUNK), BF16),
                pltpu.VMEM((8, 128), F32),
                dma((num_chunks + 1,)),
                dma((5,)), dma((5,)), dma((5, 2)), dma((5, 2)), dma((5, 2)), dma((5, 2)),
                dma((2, 2, 2)), dma((2, 2, 2)), dma((2, 2)), dma((2, 2)),
                dma((5,)),
                dma((2,)), dma((2,)), dma((2 * num_chunks,)),
                dma((num_chunks,)), dma((num_chunks,)), dma((num_chunks,)),
            ],
            compiler_params=pltpu.CompilerParams(collective_id=1, has_side_effects=True, vmem_limit_bytes=60 * 2 ** 20),
        )(direction, sq_norm, weight)

    def local_step(grad_part, momentum, weight):
        grad = lax.psum_scatter(grad_part[0], 'dp', scatter_dimension=1, tiled=True) / group
        new_momentum = MOMENTUM * momentum + grad
        direction = (grad + MOMENTUM * new_momentum).astype(BF16)
        as_float = direction.astype(F32)
        sq_norm = lax.psum(jnp.sum(as_float * as_float), 'dp')
        whole = lax.all_gather(direction[0], 'dp', axis=0, tiled=True)
        weight_bf16, ortho, _ = orthogonal_update(whole, jnp.full((8, 128), sq_norm, F32), weight[0])
        scale = 0.2 * math.sqrt(max(weight_bf16.shape))
        new_weight = weight - LEARN_RATE * (scale * ortho[None].astype(F32) + WEIGHT_DECAY * weight)
        return new_momentum, new_weight, weight_bf16[None]

    return jax.shard_map(local_step, mesh=mesh, in_specs=(P(('mp', 'dp')), P('mp', 'dp'), P('mp', 'dp')), out_specs=(P('mp', 'dp'), P('mp', 'dp'), P('mp')), check_vma=False)
```

```python
import math
import jax
import jax.numpy as jnp
from jax import lax
from jax.experimental import pallas as pl
from jax.experimental.pallas import tpu as pltpu
from jax.sharding import PartitionSpec as P

MOMENTUM = 0.95
LEARN_RATE = 2.0
WEIGHT_DECAY = 0.25
NS_STEPS = 5
COEF_A = 3.4445
COEF_B = -4.7750
COEF_C = 2.0315

MESH = pl.DeviceIdType.MESH
F32, BF16 = jnp.float32, jnp.bfloat16
CORES = 2
BLOCK = 512
CHUNK = 512
PIECE = 32
DEPTH = 4
BLOCKS = (((0, 0), (2, 0), (1, 1), (3, 1), (3, 3)), ((1, 0), (3, 0), (2, 1), (2, 2), (3, 2)))


def lookup(index, values):
    result = jnp.int32(values[0])
    for place, value in enumerate(values[1:], 1):
        result = jnp.where(index == place, jnp.int32(value), result)
    return result


def block_of(core, index):
    row = jnp.where(core == 0, lookup(index, [b[0] for b in BLOCKS[0]]), lookup(index, [b[0] for b in BLOCKS[1]]))
    col = jnp.where(core == 0, lookup(index, [b[1] for b in BLOCKS[0]]), lookup(index, [b[1] for b in BLOCKS[1]]))
    return row, col


def span(index, size):
    return pl.ds(pl.multiple_of(index * size, size), size)


def muon(group, rows, half, scale, grad_ref, mom_ref, w_ref, wb_ref, xrow_ref, nmom_ref, wcol_ref, pair_ref, arrived_ref,
         x_ref, gram, poly, part_out, part_in, o_tile, tiles, stage, own, square_acc, sq_out, sq_in,
         pair_send, pair_recv, rs_send, rs_recv, in_sem, sq_send, sq_recv, up_send, up_recv, mate_send, mate_recv, pass_send, pass_recv,
         part_send, part_recv, gram_send, gram_recv, poly_send, poly_recv,
         w_send, w_recv, w_fwd_send, w_fwd_recv, tile_sem, out_sem, out_send, out_recv, row_sem, row_send, row_recv):
    me = lax.axis_index('dp')
    core, chip = lax.rem(me, CORES), me // CORES
    chips = group // CORES
    slab = rows // group
    partner = chip * CORES + (1 - core)
    side_chip = (lax.rem(chip + 1, chips), lax.rem(chip + chips - 1, chips))
    far_chip = lax.rem(chip + 2, chips)
    num_chunks = half // CHUNK
    slots = num_chunks + 1
    pieces = slab // PIECE

    def remote(src, dst, send, recv, device):
        return pltpu.make_async_remote_copy(src, dst, send, recv, device_id={'dp': device}, device_id_type=MESH)

    barrier = pltpu.get_barrier_semaphore()
    for other in range(1, group):
        pl.semaphore_signal(barrier, inc=1, device_id={'dp': lax.rem(me + other, group)}, device_id_type=MESH)
    pl.semaphore_wait(barrier, group - 1)

    def dest_chip(order):
        return jnp.where(order == 0, far_chip, jnp.where(order == 1, side_chip[0], jnp.where(order == 2, side_chip[1], chip)))

    def piece_rows(chip_index, core_index, j):
        return pl.ds(pl.multiple_of((chip_index * CORES + core_index) * slab + j * PIECE, PIECE), PIECE)

    def pair_copy(i):
        order, j = i // pieces, lax.rem(i, pieces)
        return remote(grad_ref.at[piece_rows(dest_chip(order), 1 - core, j), :], pair_ref.at[order, span(j, PIECE), :],
                      pair_send.at[i], pair_recv.at[i], partner)

    def pair_start(i, _):
        pair_copy(i).start()
        return 0
    lax.fori_loop(0, chips * pieces, pair_start, 0)

    def columns(which):
        return pl.ds(which * half, half)

    def grad_loads(order, j, col, base):
        return (pltpu.make_async_copy(grad_ref.at[piece_rows(dest_chip(order), core, j), col], tiles.at[base], in_sem.at[base]),
                pltpu.make_async_copy(pair_ref.at[order, span(j, PIECE), col], tiles.at[base + 1], in_sem.at[base + 1]))

    def arrived_load(phase, side, j, base):
        return pltpu.make_async_copy(arrived_ref.at[phase, side, span(j, PIECE), :], tiles.at[base], in_sem.at[base])

    def rs_copy(q, side):
        phase, j = q // pieces, lax.rem(q, pieces)
        slot = lax.rem(q, DEPTH)
        return remote(stage.at[side, slot], arrived_ref.at[phase, side, span(j, PIECE), :],
                      rs_send.at[side, slot], rs_recv.at[phase, side, j], side_chip[side] * CORES + core)

    def up_copy(side, h, j, sender=None):
        where = x_ref.at[pl.ds(0, num_chunks), pl.ds(pl.multiple_of(me * slab + j * PIECE, PIECE), PIECE), :]
        return remote(own.at[pl.ds(h * num_chunks, num_chunks), span(j, PIECE), :], where,
                      up_send.at[side, h, j], up_recv.at[side, core if sender is None else sender, j], side_chip[side] * CORES + h)

    def mate_copy(j):
        where = x_ref.at[pl.ds(0, num_chunks), pl.ds(pl.multiple_of(me * slab + j * PIECE, PIECE), PIECE), :]
        return remote(own.at[pl.ds((1 - core) * num_chunks, num_chunks), span(j, PIECE), :], where,
                      mate_send.at[j], mate_recv.at[j], partner)

    def nmom_copy(j, which):
        return pltpu.make_async_copy(tiles.at[5], nmom_ref.at[span(j, PIECE), columns(which)], in_sem.at[5])

    square_acc[...] = jnp.zeros_like(square_acc)

    def send_sums(q):
        phase, j = q // pieces, lax.rem(q, pieces)

        @pl.when(phase == 0)
        def _():
            pair_copy(j).wait_recv()

        @pl.when(phase == 1)
        def _():
            pair_copy(pieces + j).wait_recv()
            pair_copy(2 * pieces + j).wait_recv()
        for side in (0, 1):
            order = jnp.where(phase == 0, 0, 1 + side)
            which = jnp.where(phase == 1, 1 - side, side)
            col = pl.ds(pl.multiple_of(which * half, half), half)
            loads = grad_loads(order, j, col, 3 * side)
            for load in loads:
                load.start()

            @pl.when(phase == 2)
            def _():
                rs_copy(j, side).wait_recv()
                arrived_load(0, side, j, 3 * side + 2).start()

        for side in (0, 1):
            slot = lax.rem(q, DEPTH)

            @pl.when(q >= DEPTH)
            def _():
                rs_copy(q - DEPTH, side).wait_send()
            order = jnp.where(phase == 0, 0, 1 + side)
            which = jnp.where(phase == 1, 1 - side, side)
            col = pl.ds(pl.multiple_of(which * half, half), half)
            for load in grad_loads(order, j, col, 3 * side):
                load.wait()

            @pl.when(phase == 2)
            def _():
                arrived_load(0, side, j, 3 * side + 2).wait()
                stage[side, slot] = (tiles[3 * side] + tiles[3 * side + 1]) + tiles[3 * side + 2]

            @pl.when(phase != 2)
            def _():
                stage[side, slot] = tiles[3 * side] + tiles[3 * side + 1]
            rs_copy(q, side).start()

    def finish(j):
        pair_copy(3 * pieces + j).wait_recv()
        for which in (0, 1):
            loads = list(grad_loads(3, j, columns(which), 0))
            for side in (0, 1):
                phase = 2 if side == which else 1
                rs_copy(phase * pieces + j, side).wait_recv()
                loads.append(arrived_load(phase, side, j, 2 + side))
            loads.append(pltpu.make_async_copy(mom_ref.at[span(j, PIECE), columns(which)], tiles.at[4], in_sem.at[4]))
            for load in loads:
                load.start()
            for load in loads:
                load.wait()
            if which == 1:
                nmom_copy(j, 0).wait()
            mean = (((tiles[0] + tiles[1]) + tiles[2]) + tiles[3]) / group
            momentum = MOMENTUM * tiles[4] + mean
            tiles[5] = momentum
            nmom_copy(j, which).start()
            update = (mean + MOMENTUM * momentum).astype(BF16)
            for c in range(num_chunks):
                own[which * num_chunks + c, span(j, PIECE), :] = update[:, c * CHUNK:(c + 1) * CHUNK]
            as_float = update.astype(F32)
            square_acc[...] += jnp.sum((as_float * as_float).reshape(PIECE // 8, 8, half), axis=0)
        nmom_copy(j, 1).wait()
        for side in (0, 1):
            for h in range(CORES):
                up_copy(side, h, j).start()
        mate_copy(j).start()

    def reduce_step(q, _):
        @pl.when(q < 3 * pieces)
        def _():
            send_sums(q)

        @pl.when(q >= 2 * pieces + DEPTH)
        def _():
            finish(q - 2 * pieces - DEPTH)
        return 0
    lax.fori_loop(0, 3 * pieces + DEPTH, reduce_step, 0)
    for side in (0, 1):
        for last in range(DEPTH):
            rs_copy(3 * pieces - DEPTH + last, side).wait_send()

    total = jnp.sum(square_acc[...])
    sq_out[...] = jnp.full(sq_out.shape, total, F32)
    sq_in[me] = jnp.full(sq_out.shape, total, F32)

    def sq_copy(other):
        return remote(sq_out, sq_in.at[me], sq_send.at[other], sq_recv.at[other], lax.rem(me + other, group))
    for other in range(1, group):
        sq_copy(other).start()
    for other in range(1, group):
        sq_copy(other).wait()
    square = sq_in[0, 0:1, 0:1]
    for i in range(1, group):
        square = square + sq_in[i, 0:1, 0:1]
    inverse = 1.0 / (jnp.sqrt(square) + 1e-7)

    def normalise(row0, size):
        r = pl.ds(pl.multiple_of(row0, size), size)
        x_ref[0:num_chunks, r, :] = (x_ref[0:num_chunks, r, :].astype(F32) * inverse).astype(BF16)

    def normalise_own(j, _):
        r = pl.ds(pl.multiple_of(me * slab + j * PIECE, PIECE), PIECE)
        x_ref[0:num_chunks, r, :] = (own[pl.ds(core * num_chunks, num_chunks), span(j, PIECE), :].astype(F32) * inverse).astype(BF16)
        return 0
    lax.fori_loop(0, pieces, normalise_own, 0)

    def normalise_mate(j, _):
        mate_copy(j).wait_recv()
        normalise(partner * slab + j * PIECE, PIECE)
        return 0
    lax.fori_loop(0, pieces, normalise_mate, 0)

    def pass_copy(side, from_core, j):
        row0 = (side_chip[1 - side] * CORES + from_core) * slab + (side * (pieces // 2) + j) * PIECE
        where = x_ref.at[pl.ds(0, num_chunks), pl.ds(pl.multiple_of(row0, PIECE), PIECE), :]
        return remote(where, where, pass_send.at[side, from_core, j], pass_recv.at[side, from_core, j], side_chip[side] * CORES + core)

    def arrive(j, _):
        for side in (0, 1):
            for from_core in range(CORES):
                up_copy(side, core, j, from_core).wait_recv()
                normalise((side_chip[1 - side] * CORES + from_core) * slab + j * PIECE, PIECE)

                @pl.when(j // (pieces // 2) == side)
                def _():
                    pass_copy(side, from_core, j - side * (pieces // 2)).start()
        return 0
    lax.fori_loop(0, pieces, arrive, 0)

    piece = slab // 2

    def w_first(side, h, part, sender=None):
        return remote(w_ref.at[pl.ds(part * piece, piece), pl.ds(h * half, half)],
                      wcol_ref.at[chip, pl.ds(pl.multiple_of(core * slab + part * piece, piece), piece), :],
                      w_send.at[side, h, part], w_recv.at[side, core if sender is None else sender, part], side_chip[side] * CORES + h)

    def w_forward(side, from_core):
        where = wcol_ref.at[side_chip[1 - side], pl.ds(from_core * slab + side * piece, piece), :]
        return remote(where, where, w_fwd_send.at[side, from_core], w_fwd_recv.at[side, from_core], side_chip[side] * CORES + core)

    def w_pair():
        return remote(w_ref.at[:, pl.ds(pl.multiple_of((1 - core) * half, half), half)],
                      wcol_ref.at[chip, pl.ds(pl.multiple_of(core * slab, slab), slab), :], tile_sem.at[3], tile_sem.at[4], partner)

    def w_own():
        return pltpu.make_async_copy(w_ref.at[:, pl.ds(pl.multiple_of(core * half, half), half)],
                                     wcol_ref.at[chip, pl.ds(pl.multiple_of(core * slab, slab), slab), :], tile_sem.at[2])
    for part in (0, 1):
        for side in (0, 1):
            for h in range(CORES):
                w_first(side, h, part if side == 0 else 1 - part).start()
    w_pair().start()
    w_own().start()

    def late(j, _):
        for side in (0, 1):
            for from_core in range(CORES):
                pass_copy(side, from_core, j).wait()
        return 0
    lax.fori_loop(0, pieces // 2, late, 0)

    def slot_of(c, t):
        return lax.rem(c + 2 * slots - t, slots)

    def gram_send_copy(b, index, row, col):
        return remote(gram.at[span(row, BLOCK), span(col, BLOCK)], gram.at[span(row, BLOCK), span(col, BLOCK)],
                      gram_send.at[index, b], gram_recv.at[index, b], partner)

    def poly_send_copy(b, index, row, col):
        return remote(poly.at[span(row, BLOCK), span(col, BLOCK)], poly.at[span(row, BLOCK), span(col, BLOCK)],
                      poly_send.at[index, b], poly_recv.at[index, b], partner)

    def both(copy, owner, index, act):
        row, col = block_of(owner, index)
        act(copy(0, index, row, col))

        @pl.when(row != col)
        def _():
            act(copy(1, index, col, row))

    def part_copy(index):
        return remote(part_out.at[index], part_in.at[index], part_send.at[index], part_recv.at[index], partner)

    def step(t, _):
        def gram_block(row, col):
            ri, rj = span(row, BLOCK), span(col, BLOCK)
            xi = jnp.concatenate([x_ref[slot_of(c, t), ri, :] for c in range(num_chunks)], axis=1)
            xj = jnp.concatenate([x_ref[slot_of(c, t), rj, :] for c in range(num_chunks)], axis=1)
            return lax.dot_general(xi, xj, (((1,), (1,)), ((), ())), preferred_element_type=F32)

        @pl.when(t == 2)
        def _():
            for side in (0, 1):
                for from_core in range(CORES):
                    w_first(side, 0, side, from_core).wait_recv()
                    w_forward(side, from_core).start()

        def gram_step(index, _):
            owner = jnp.where(index < 5, 1 - core, core)
            place = lax.rem(index, 5)
            row, col = block_of(owner, place)
            value = gram_block(row, col)

            @pl.when(index < 5)
            def _():
                part_out[place] = value
                part_copy(place).start()

            @pl.when(index >= 5)
            def _():
                part_copy(place).wait_recv()
                block = (value + part_in[place]).astype(BF16)
                gram[span(row, BLOCK), span(col, BLOCK)] = block

                @pl.when(row != col)
                def _():
                    gram[span(col, BLOCK), span(row, BLOCK)] = block.T
                both(gram_send_copy, core, place, lambda cp: cp.start())
            return 0
        lax.fori_loop(0, 10, gram_step, 0)

        def poly_step(index, _):
            @pl.when(index == 0)
            def _():
                for i in range(4):
                    both(gram_send_copy, 1 - core, i, lambda cp: cp.wait_recv())

            @pl.when(index == 1)
            def _():
                both(gram_send_copy, 1 - core, 4, lambda cp: cp.wait_recv())
            row, col = block_of(core, index)
            ri, rj = span(row, BLOCK), span(col, BLOCK)
            square = jnp.dot(gram[ri, :], gram[:, rj], preferred_element_type=F32)
            block = (COEF_B * gram[ri, rj].astype(F32) + COEF_C * square).astype(BF16)
            poly[ri, rj] = block

            @pl.when(row != col)
            def _():
                poly[rj, ri] = block.T
            both(poly_send_copy, core, index, lambda cp: cp.start())
            return 0
        lax.fori_loop(0, 5, poly_step, 0)

        def part_drain(i, _):
            part_copy(i).wait_send()
            return 0
        lax.fori_loop(0, 5, part_drain, 0)
        tall = 1024

        def poly_waits(q):
            @pl.when(q == 0)
            def _():
                for i in range(4):
                    both(poly_send_copy, 1 - core, i, lambda cp: cp.wait_recv())

            @pl.when(q == 1)
            def _():
                both(poly_send_copy, 1 - core, 4, lambda cp: cp.wait_recv())

        def apply_block(q):
            c, m = q // 2, lax.rem(q, 2)
            rm = span(m, tall)
            src, dst = slot_of(c, t), slot_of(c, t + 1)
            total = jnp.dot(poly[rm, :], x_ref[src], preferred_element_type=F32)
            return c, m, rm, dst, (COEF_A * x_ref[src, rm, :].astype(F32) + total).astype(BF16)

        @pl.when(t < NS_STEPS - 1)
        def _():
            def apply_step(q, _):
                poly_waits(q)
                c, m, rm, dst, value = apply_block(q)
                x_ref[dst, rm, :] = value
                return 0
            lax.fori_loop(0, 2 * num_chunks, apply_step, 0)

        @pl.when(t == NS_STEPS - 1)
        def _():
            for side in (0, 1):
                for from_core in range(CORES):
                    w_first(side, 0, 1 - side, from_core).wait_recv()
                    w_forward(side, from_core).wait_recv()
            w_pair().wait_recv()
            w_own().wait()

            def tile_load(q):
                c, m = q // 2, lax.rem(q, 2)
                return pltpu.make_async_copy(wcol_ref.at[pl.ds(2 * m, 2), :, span(c, CHUNK)], part_out.at[pl.ds(2 * lax.rem(q, 2), 2)], tile_sem.at[lax.rem(q, 2)])

            def out_pair(q, slot):
                c, m = q // 2, lax.rem(q, 2)
                where = wb_ref.at[span(m, tall), pl.ds(pl.multiple_of(core * half + c * CHUNK, CHUNK), CHUNK)]
                return (pltpu.make_async_copy(o_tile.at[slot], where, out_sem.at[slot]),
                        remote(o_tile.at[slot], where, out_send.at[slot], out_recv.at[q], partner))

            def row_pair(c):
                slot = slot_of(c, t + 1)
                cols = pl.ds(pl.multiple_of(core * half + c * CHUNK, CHUNK), CHUNK)
                return (pltpu.make_async_copy(x_ref.at[slot, span(me, slab), :], xrow_ref.at[:, cols], row_sem.at[c]),
                        remote(x_ref.at[slot, span(partner, slab), :], xrow_ref.at[:, cols], row_send.at[c], row_recv.at[c], partner))

            tile_load(0).start()

            def last_step(q, _):
                poly_waits(q)

                @pl.when(q + 1 < 2 * num_chunks)
                def _():
                    tile_load(q + 1).start()
                c, m, rm, dst, value = apply_block(q)
                x_ref[dst, rm, :] = value
                slot = lax.rem(q, 2)
                tile_load(q).wait()

                @pl.when(q >= 2)
                def _():
                    here, there = out_pair(q - 2, slot)
                    here.wait()
                    there.wait_send()
                old = part_out[pl.ds(2 * slot, 2)].reshape(tall, CHUNK)
                new = old - LEARN_RATE * (scale * value.astype(F32) + WEIGHT_DECAY * old)
                o_tile[slot] = new.astype(BF16)
                here, there = out_pair(q, slot)
                here.start()
                there.start()

                @pl.when(m == 1)
                def _():
                    here, there = row_pair(c)
                    here.start()
                    there.start()
                return 0
            lax.fori_loop(0, 2 * num_chunks, last_step, 0)
            for q in (2 * num_chunks - 2, 2 * num_chunks - 1):
                here, there = out_pair(q, q % 2)
                here.wait()
                there.wait_send()

            def out_arrival(q, _):
                c, m = q // 2, lax.rem(q, 2)
                where = wb_ref.at[span(m, tall), pl.ds(pl.multiple_of((1 - core) * half + c * CHUNK, CHUNK), CHUNK)]
                remote(o_tile.at[0], where, out_send.at[0], out_recv.at[q], partner).wait_recv()
                return 0
            lax.fori_loop(0, 2 * num_chunks, out_arrival, 0)

            def row_end(c, _):
                here, there = row_pair(c)
                here.wait()
                there.wait()
                return 0
            lax.fori_loop(0, num_chunks, row_end, 0)

        def drain(i, _):
            both(gram_send_copy, core, i, lambda cp: cp.wait_send())
            both(poly_send_copy, core, i, lambda cp: cp.wait_send())
            return 0
        lax.fori_loop(0, 5, drain, 0)
        return 0
    lax.fori_loop(0, NS_STEPS, step, 0)

    for part in (0, 1):
        for side in (0, 1):
            for h in range(CORES):
                w_first(side, h, part).wait_send()
    for side in (0, 1):
        for from_core in range(CORES):
            w_forward(side, from_core).wait_send()
    w_pair().wait_send()

    def sent(j, _):
        for side in (0, 1):
            for h in range(CORES):
                up_copy(side, h, j).wait_send()
        mate_copy(j).wait_send()
        return 0
    lax.fori_loop(0, pieces, sent, 0)

    def paired(i, _):
        pair_copy(i).wait_send()
        return 0
    lax.fori_loop(0, chips * pieces, paired, 0)


def solution(mesh):
    group = mesh.shape['dp']

    def local_step(grad_part, momentum, weight):
        slab, num_cols = weight.shape[1:]
        rows = slab * group
        half = num_cols // CORES
        scale = 0.2 * math.sqrt(max(rows, num_cols))
        num_chunks = half // CHUNK
        chips = group // CORES
        pieces = slab // PIECE
        anywhere = pl.BlockSpec(memory_space=pl.ANY)
        dma = pltpu.SemaphoreType.DMA
        shape = jax.ShapeDtypeStruct

        def kernel(*refs):
            muon(group, rows, half, scale, *refs)
        outs = pl.pallas_call(
            kernel,
            name='muon',
            out_shape=(shape((rows, num_cols), BF16), shape((slab, num_cols), BF16), shape((slab, num_cols), F32),
                       shape((chips, CORES * slab, half), F32), shape((chips, slab, num_cols), F32), shape((3, 2, slab, half), F32)),
            in_specs=[anywhere] * 3,
            out_specs=(anywhere,) * 6,
            scratch_shapes=[
                pltpu.VMEM((num_chunks + 1, rows, CHUNK), BF16),
                pltpu.VMEM((rows, rows), BF16),
                pltpu.VMEM((rows, rows), BF16),
                pltpu.VMEM((5, BLOCK, BLOCK), F32),
                pltpu.VMEM((5, BLOCK, BLOCK), F32),
                pltpu.VMEM((2, 1024, CHUNK), BF16),
                pltpu.VMEM((6, PIECE, half), F32),
                pltpu.VMEM((2, DEPTH, PIECE, half), F32),
                pltpu.VMEM((CORES * num_chunks, slab, CHUNK), BF16),
                pltpu.VMEM((8, half), F32),
                pltpu.VMEM((8, 128), F32),
                pltpu.VMEM((group, 8, 128), F32),
                dma((chips * pieces,)), dma((chips * pieces,)), dma((2, DEPTH)), dma((3, 2, pieces)), dma((6,)),
                dma((group,)), dma((group,)), dma((2, 2, pieces)), dma((2, 2, pieces)), dma((pieces,)), dma((pieces,)),
                dma((2, 2, pieces // 2)), dma((2, 2, pieces // 2)),
                dma((5,)), dma((5,)), dma((5, 2)), dma((5, 2)), dma((5, 2)), dma((5, 2)),
                dma((2, 2, 2)), dma((2, 2, 2)), dma((2, 2)), dma((2, 2)),
                dma((5,)),
                dma((2,)), dma((2,)), dma((2 * num_chunks,)),
                dma((num_chunks,)), dma((num_chunks,)), dma((num_chunks,)),
            ],
            compiler_params=pltpu.CompilerParams(collective_id=1, has_side_effects=True, vmem_limit_bytes=63 * 2 ** 20),
        )(grad_part[0, 0], momentum[0], weight[0])
        weight_bf16, ortho, new_momentum = outs[:3]
        new_weight = weight - LEARN_RATE * (scale * ortho[None].astype(F32) + WEIGHT_DECAY * weight)
        return new_momentum[None], new_weight, weight_bf16[None]

    return jax.shard_map(local_step, mesh=mesh, in_specs=(P(('mp', 'dp')), P('mp', 'dp'), P('mp', 'dp')), out_specs=(P('mp', 'dp'), P('mp', 'dp'), P('mp')), check_vma=False)
```

```python
import math
import jax
import jax.numpy as jnp
from jax import lax
from jax.experimental import pallas as pl
from jax.experimental.pallas import tpu as pltpu
from jax.sharding import PartitionSpec as P

MOMENTUM = 0.95
LEARN_RATE = 2.0
WEIGHT_DECAY = 0.25
NS_STEPS = 5
COEF_A = 3.4445
COEF_B = -4.7750
COEF_C = 2.0315

MESH = pl.DeviceIdType.MESH
F32, BF16 = jnp.float32, jnp.bfloat16
CORES = 2
BLOCK = 512
CHUNK = 512
PIECE = 32
DEPTH = 4
EARLY = 2
BLOCKS = (((0, 0), (2, 0), (1, 1), (2, 2), (3, 3)), ((1, 0), (3, 0), (2, 1), (3, 1), (3, 2)))
SQUARES = (((0, 0), (1, 1), (2, 0), (2, 2), (3, 3)), ((1, 0), (2, 1), (3, 0), (3, 1), (3, 2)))

OWNER = [next((core for core in range(CORES) if (max(r, c), min(r, c)) in BLOCKS[core])) for r in range(4) for c in range(4)]
PLACE = [BLOCKS[OWNER[r * 4 + c]].index((max(r, c), min(r, c))) for r in range(4) for c in range(4)]
NEAR_ONE = [0, 0, 1, 0, 1, 2]
NEAR_TWO = [0, 1, 1, 2, 2, 2]


def lookup(index, values):
    result = jnp.int32(values[0])
    for place, value in enumerate(values[1:], 1):
        result = jnp.where(index == place, jnp.int32(value), result)
    return result


def block_of(core, index, table=BLOCKS):
    row = jnp.where(core == 0, lookup(index, [b[0] for b in table[0]]), lookup(index, [b[0] for b in table[1]]))
    col = jnp.where(core == 0, lookup(index, [b[1] for b in table[0]]), lookup(index, [b[1] for b in table[1]]))
    return row, col


def span(index, size):
    return pl.ds(pl.multiple_of(index * size, size), size)


def muon(group, rows, half, scale, grad_ref, mom_ref, w_ref, wb_ref, xrow_ref, nmom_ref, wcol_ref, pair_ref, arrived_ref,
         x_ref, gram, poly, parts, part_in, tiles, stage, own, square_acc, sq_out, sq_in,
         pair_send, pair_recv, rs_send, rs_recv, in_sem, sq_send, sq_recv, up_send, up_recv, mate_send, mate_recv, pass_send, pass_recv, far_send, far_recv, share_send, share_recv,
         part_send, part_recv, gram_send, gram_recv, poly_send, poly_recv,
         w_send, w_recv, w_fwd_send, w_fwd_recv, tile_sem, out_sem, out_send, out_recv, row_sem, row_send, row_recv):
    me = lax.axis_index('dp')
    core, chip = lax.rem(me, CORES), me // CORES
    chips = group // CORES
    slab = rows // group
    partner = chip * CORES + (1 - core)
    side_chip = (lax.rem(chip + 1, chips), lax.rem(chip + chips - 1, chips))
    far_chip = lax.rem(chip + 2, chips)
    num_chunks = half // CHUNK
    slots = num_chunks + 1
    pieces = slab // PIECE

    def remote(src, dst, send, recv, device):
        return pltpu.make_async_remote_copy(src, dst, send, recv, device_id={'dp': device}, device_id_type=MESH)

    barrier = pltpu.get_barrier_semaphore()
    for other in range(1, group):
        pl.semaphore_signal(barrier, inc=1, device_id={'dp': lax.rem(me + other, group)}, device_id_type=MESH)
    pl.semaphore_wait(barrier, group - 1)

    def dest_chip(order):
        return jnp.where(order == 0, far_chip, jnp.where(order == 1, side_chip[0], jnp.where(order == 2, side_chip[1], chip)))

    def piece_rows(chip_index, core_index, j):
        return pl.ds(pl.multiple_of((chip_index * CORES + core_index) * slab + j * PIECE, PIECE), PIECE)

    def pair_copy(i):
        order, j = i // pieces, lax.rem(i, pieces)
        return remote(grad_ref.at[piece_rows(dest_chip(order), 1 - core, j), :], pair_ref.at[order, span(j, PIECE), :],
                      pair_send.at[i], pair_recv.at[i], partner)

    def pair_start(i, _):
        pair_copy(i).start()
        return 0
    lax.fori_loop(0, chips * pieces, pair_start, 0)

    def columns(which):
        return pl.ds(which * half, half)

    def grad_loads(order, j, col, base):
        return (pltpu.make_async_copy(grad_ref.at[piece_rows(dest_chip(order), core, j), col], tiles.at[base], in_sem.at[base]),
                pltpu.make_async_copy(pair_ref.at[order, span(j, PIECE), col], tiles.at[base + 1], in_sem.at[base + 1]))

    def arrived_load(phase, side, j, base):
        return pltpu.make_async_copy(arrived_ref.at[phase, side, span(j, PIECE), :], tiles.at[base], in_sem.at[base])

    def rs_copy(q, side):
        phase, j = q // pieces, lax.rem(q, pieces)
        slot = lax.rem(q, DEPTH)
        return remote(stage.at[side, slot], arrived_ref.at[phase, side, span(j, PIECE), :],
                      rs_send.at[side, slot], rs_recv.at[phase, side, j], side_chip[side] * CORES + core)

    def up_copy(side, h, j, sender=None):
        where = x_ref.at[pl.ds(0, num_chunks), pl.ds(pl.multiple_of(me * slab + j * PIECE, PIECE), PIECE), :]
        return remote(own.at[pl.ds(h * num_chunks, num_chunks), span(j, PIECE), :], where,
                      up_send.at[side, h, j], up_recv.at[side, core if sender is None else sender, j], side_chip[side] * CORES + h)

    def mate_copy(j):
        where = x_ref.at[pl.ds(0, num_chunks), pl.ds(pl.multiple_of(me * slab + j * PIECE, PIECE), PIECE), :]
        return remote(own.at[pl.ds((1 - core) * num_chunks, num_chunks), span(j, PIECE), :], where,
                      mate_send.at[j], mate_recv.at[j], partner)

    def nmom_copy(j, which):
        return pltpu.make_async_copy(tiles.at[5], nmom_ref.at[span(j, PIECE), columns(which)], in_sem.at[5])

    square_acc[...] = jnp.zeros_like(square_acc)

    def send_sums(q):
        phase, j = q // pieces, lax.rem(q, pieces)

        @pl.when(phase == 0)
        def _():
            pair_copy(j).wait_recv()

        @pl.when(phase == 1)
        def _():
            pair_copy(pieces + j).wait_recv()
            pair_copy(2 * pieces + j).wait_recv()
        for side in (0, 1):
            order = jnp.where(phase == 0, 0, 1 + side)
            which = jnp.where(phase == 1, 1 - side, side)
            col = pl.ds(pl.multiple_of(which * half, half), half)
            loads = grad_loads(order, j, col, 3 * side)
            for load in loads:
                load.start()

            @pl.when(phase == 2)
            def _():
                rs_copy(j, side).wait_recv()
                arrived_load(0, side, j, 3 * side + 2).start()

        for side in (0, 1):
            slot = lax.rem(q, DEPTH)

            @pl.when(q >= DEPTH)
            def _():
                rs_copy(q - DEPTH, side).wait_send()
            order = jnp.where(phase == 0, 0, 1 + side)
            which = jnp.where(phase == 1, 1 - side, side)
            col = pl.ds(pl.multiple_of(which * half, half), half)
            for load in grad_loads(order, j, col, 3 * side):
                load.wait()

            @pl.when(phase == 2)
            def _():
                arrived_load(0, side, j, 3 * side + 2).wait()
                stage[side, slot] = (tiles[3 * side] + tiles[3 * side + 1]) + tiles[3 * side + 2]

            @pl.when(phase != 2)
            def _():
                stage[side, slot] = tiles[3 * side] + tiles[3 * side + 1]
            rs_copy(q, side).start()

    def send_up(j):
        for side in (0, 1):
            for h in range(CORES):
                up_copy(side, h, j).start()
        mate_copy(j).start()

    def finish(j):
        pair_copy(3 * pieces + j).wait_recv()
        for which in (0, 1):
            loads = list(grad_loads(3, j, columns(which), 0))
            for side in (0, 1):
                phase = 2 if side == which else 1
                rs_copy(phase * pieces + j, side).wait_recv()
                loads.append(arrived_load(phase, side, j, 2 + side))
            loads.append(pltpu.make_async_copy(mom_ref.at[span(j, PIECE), columns(which)], tiles.at[4], in_sem.at[4]))
            for load in loads:
                load.start()
            for load in loads:
                load.wait()
            if which == 1:
                nmom_copy(j, 0).wait()
            mean = (((tiles[0] + tiles[1]) + tiles[2]) + tiles[3]) / group
            momentum = MOMENTUM * tiles[4] + mean
            tiles[5] = momentum
            nmom_copy(j, which).start()
            update = (mean + MOMENTUM * momentum).astype(BF16)
            for c in range(num_chunks):
                own[which * num_chunks + c, span(j, PIECE), :] = update[:, c * CHUNK:(c + 1) * CHUNK]
            as_float = update.astype(F32)
            square_acc[...] += jnp.sum((as_float * as_float).reshape(PIECE // 8, 8, half), axis=0)
        nmom_copy(j, 1).wait()

        @pl.when(j < pieces // 2)
        def _():
            send_up(j)

    def reduce_step(q, _):
        @pl.when(q < 3 * pieces)
        def _():
            send_sums(q)

        @pl.when(q >= 2 * pieces + DEPTH)
        def _():
            finish(q - 2 * pieces - DEPTH)
        return 0
    lax.fori_loop(0, 3 * pieces + DEPTH, reduce_step, 0)
    for side in (0, 1):
        for last in range(DEPTH):
            rs_copy(3 * pieces - DEPTH + last, side).wait_send()

    total = jnp.sum(square_acc[...])
    sq_out[...] = jnp.full(sq_out.shape, total, F32)
    sq_in[me] = jnp.full(sq_out.shape, total, F32)

    def sq_copy(other):
        return remote(sq_out, sq_in.at[me], sq_send.at[other], sq_recv.at[other], lax.rem(me + other, group))
    for other in range(1, group):
        sq_copy(other).start()

    def send_rest(j, _):
        send_up(j)
        return 0
    lax.fori_loop(pieces // 2, pieces, send_rest, 0)
    for other in range(1, group):
        sq_copy(other).wait()
    square = sq_in[0, 0:1, 0:1]
    for i in range(1, group):
        square = square + sq_in[i, 0:1, 0:1]
    inverse = 1.0 / (jnp.sqrt(square) + 1e-7)

    def normalise(row0, size):
        r = pl.ds(pl.multiple_of(row0, size), size)
        x_ref[0:num_chunks, r, :] = (x_ref[0:num_chunks, r, :].astype(F32) * inverse).astype(BF16)

    def normalise_own(j, _):
        r = pl.ds(pl.multiple_of(me * slab + j * PIECE, PIECE), PIECE)
        x_ref[0:num_chunks, r, :] = (own[pl.ds(core * num_chunks, num_chunks), span(j, PIECE), :].astype(F32) * inverse).astype(BF16)
        return 0
    lax.fori_loop(0, pieces, normalise_own, 0)

    def normalise_mate(j, _):
        mate_copy(j).wait_recv()
        normalise(partner * slab + j * PIECE, PIECE)
        return 0
    lax.fori_loop(0, pieces, normalise_mate, 0)

    def pass_copy(side, from_core, c):
        row0 = (side_chip[1 - side] * CORES + from_core) * slab + side * (slab // 2)
        where = x_ref.at[c, pl.ds(pl.multiple_of(row0, slab // 2), slab // 2), :]
        return remote(where, where, pass_send.at[side, from_core, c], pass_recv.at[side, from_core, c], side_chip[side] * CORES + core)

    def pass_on(side, c):
        for from_core in range(CORES):
            pass_copy(side, from_core, c).start()

    def arrive(j, _):
        for side in (0, 1):
            for from_core in range(CORES):
                up_copy(side, core, j, from_core).wait_recv()
                normalise((side_chip[1 - side] * CORES + from_core) * slab + j * PIECE, PIECE)

            @pl.when(j == (side + 1) * (pieces // 2) - 1)
            def _():
                for c in range(EARLY):
                    pass_on(side, c)
        return 0

    piece = slab // 2

    def w_first(side, h, part, sender=None):
        return remote(w_ref.at[pl.ds(part * piece, piece), pl.ds(h * half, half)],
                      wcol_ref.at[chip, pl.ds(pl.multiple_of(core * slab + part * piece, piece), piece), :],
                      w_send.at[side, h, part], w_recv.at[side, core if sender is None else sender, part], side_chip[side] * CORES + h)

    def w_forward(side, from_core):
        where = wcol_ref.at[side_chip[1 - side], pl.ds(from_core * slab + side * piece, piece), :]
        return remote(where, where, w_fwd_send.at[side, from_core], w_fwd_recv.at[side, from_core], side_chip[side] * CORES + core)

    def w_pair():
        return remote(w_ref.at[:, pl.ds(pl.multiple_of((1 - core) * half, half), half)],
                      wcol_ref.at[chip, pl.ds(pl.multiple_of(core * slab, slab), slab), :], tile_sem.at[3], tile_sem.at[4], partner)

    def w_own():
        return pltpu.make_async_copy(w_ref.at[:, pl.ds(pl.multiple_of(core * half, half), half)],
                                     wcol_ref.at[chip, pl.ds(pl.multiple_of(core * slab, slab), slab), :], tile_sem.at[2])
    def slot_of(c, t):
        return lax.rem(c + 2 * slots - t, slots)

    def gram_copy(b, index, row, col):
        where = gram.at[span(row, BLOCK), span(col, BLOCK)]
        return remote(where, where, gram_send.at[index, b], gram_recv.at[index, b], partner)

    def poly_copy(b, index, row, col):
        where = poly.at[span(row, BLOCK), span(col, BLOCK)]
        return remote(where, where, poly_send.at[index, b], poly_recv.at[index, b], partner)

    def both(copy, owner, index, act, table=BLOCKS):
        row, col = block_of(owner, index, table)

        @pl.when(row != col)
        def _():
            act(copy(1, index, col, row))
        act(copy(0, index, row, col))

    def start(copy):
        copy.start()

    def arrived(copy):
        copy.wait_recv()

    def left(copy):
        copy.wait_send()

    def part_copy(index):
        return remote(parts.at[index], part_in.at[index], part_send.at[index], part_recv.at[index], partner)

    def gram_value(t, row, col):
        ri, rj = span(row, BLOCK), span(col, BLOCK)
        xi = jnp.concatenate([x_ref[slot_of(c, t), ri, :] for c in range(num_chunks)], axis=1)
        xj = jnp.concatenate([x_ref[slot_of(c, t), rj, :] for c in range(num_chunks)], axis=1)
        return lax.dot_general(xi, xj, (((1,), (1,)), ((), ())), preferred_element_type=F32)

    def finish_gram(index, value):
        row, col = block_of(core, index)
        block = (value + part_in[index]).astype(BF16)
        gram[span(row, BLOCK), span(col, BLOCK)] = block
        gram[span(col, BLOCK), span(row, BLOCK)] = block.T

    def near_chip(order):
        return jnp.where(order == 0, chip, jnp.where(order == 1, side_chip[0], side_chip[1]))

    def near_block(index):
        one = near_chip(lookup(index, NEAR_ONE))
        two = near_chip(lookup(index, NEAR_TWO))
        row, col = jnp.maximum(one, two), jnp.minimum(one, two)
        cell = row * chips + col
        return row, col, lookup(cell, PLACE), lookup(cell, OWNER) == core

    def near_gram(index, _):
        row, col, place, mine = near_block(index)
        parts[jnp.where(mine, 5 + place, place)] = gram_value(0, row, col)

        @pl.when(jnp.logical_not(mine))
        def _():
            part_copy(place).start()
        return 0

    def near_finish(index, _):
        row, col, place, mine = near_block(index)

        @pl.when(mine)
        def _():
            part_copy(place).wait_recv()
            finish_gram(place, parts[5 + place])
            both(gram_copy, core, place, start)
        return 0

    def near_meet(index, _):
        row, col, place, mine = near_block(index)

        @pl.when(mine)
        def _():
            both(gram_copy, core, place, left)

        @pl.when(jnp.logical_not(mine))
        def _():
            part_copy(place).wait_send()
            both(gram_copy, 1 - core, place, arrived)
        return 0

    def far_block(chip_index, core_index, side):
        right, behind = lax.rem(chip_index + 1, chips), lax.rem(chip_index + chips - 1, chips)
        if side == 1:
            one, two = jnp.where(core_index == 0, chip_index, behind), right
        else:
            one, two = jnp.where(core_index == 0, chip_index, behind), behind
        return jnp.maximum(one, two), jnp.minimum(one, two)

    def far_copy(side):
        row, col = far_block(chip, core, side)
        where = gram.at[span(row, BLOCK), span(col, BLOCK)]
        return remote(where, where, far_send.at[side], far_recv.at[side], side_chip[side] * CORES + core)

    def share_copy(side, owner, b):
        row, col = far_block(side_chip[1 - side], owner, side)
        if b == 1:
            row, col = col, row
        where = gram.at[span(row, BLOCK), span(col, BLOCK)]
        return remote(where, where, share_send.at[side, b], share_recv.at[side, b], partner)

    def share(side, owner, act):
        act(share_copy(side, owner, 0))
        row, col = far_block(side_chip[1 - side], owner, side)

        @pl.when(row != col)
        def _():
            act(share_copy(side, owner, 1))

    near_gram(0, 0)
    lax.fori_loop(0, pieces, arrive, 0)
    lax.fori_loop(1, 6, near_gram, 0)
    lax.fori_loop(0, 6, near_finish, 0)
    lax.fori_loop(0, 6, near_meet, 0)
    for side in (0, 1):
        far_copy(side).start()
    for c in range(EARLY, num_chunks):
        for side in (0, 1):
            pass_on(side, c)
    for part in (0, 1):
        for side in (0, 1):
            for h in range(CORES):
                w_first(side, h, part if side == 0 else 1 - part).start()
    w_pair().start()
    w_own().start()
    for side in (0, 1):
        far_copy(side).wait_recv()
        row, col = far_block(side_chip[1 - side], core, side)
        turned = gram[span(row, BLOCK), span(col, BLOCK)].T

        @pl.when(row != col)
        def _():
            gram[span(col, BLOCK), span(row, BLOCK)] = turned
        share(side, core, start)
    for side in (0, 1):
        share(side, 1 - core, arrived)
        far_copy(side).wait_send()
        share(side, core, left)

    def sent(j, _):
        for side in (0, 1):
            for h in range(CORES):
                up_copy(side, h, j).wait_send()
        mate_copy(j).wait_send()
        return 0
    lax.fori_loop(0, pieces, sent, 0)

    tall = 1024
    per_tall = tall // slab

    def apply_value(q, t):
        c, m = q // 2, lax.rem(q, 2)
        rm = span(m, tall)
        src = slot_of(c, t)
        total = jnp.dot(poly[rm, :], x_ref[src], preferred_element_type=F32)
        return (COEF_A * x_ref[src, rm, :].astype(F32) + total).astype(BF16)

    def keep(q, t, value):
        x_ref[slot_of(q // 2, t + 1), span(lax.rem(q, 2), tall), :] = value

    def step(t, _):
        @pl.when(t == 2)
        def _():
            for side in (0, 1):
                for from_core in range(CORES):
                    w_first(side, 0, side, from_core).wait_recv()
                    w_forward(side, from_core).start()

        @pl.when(t > 0)
        def _():
            def gram_other(index, _):
                row, col = block_of(1 - core, index)
                parts[index] = gram_value(t, row, col)
                part_copy(index).start()
                return 0
            lax.fori_loop(0, 5, gram_other, 0)

            def gram_own(index, _):
                part_copy(index).wait_recv()
                row, col = block_of(core, index)
                finish_gram(index, gram_value(t, row, col))
                both(gram_copy, core, index, start)
                return 0
            lax.fori_loop(0, 5, gram_own, 0)

        def square(index, _):
            @pl.when((index == 0) & (t > 0))
            def _():
                for i in range(3):
                    both(gram_copy, 1 - core, i, arrived)

            @pl.when((index == 1) & (t > 0))
            def _():
                both(gram_copy, 1 - core, 3, arrived)

            @pl.when((index == 2) & (t > 0))
            def _():
                both(gram_copy, 1 - core, 4, arrived)
            row, col = block_of(core, index, SQUARES)
            ri, rj = span(row, BLOCK), span(col, BLOCK)
            value = jnp.dot(gram[ri, :], gram[:, rj], preferred_element_type=F32)
            block = (COEF_B * gram[ri, rj].astype(F32) + COEF_C * value).astype(BF16)
            poly[ri, rj] = block
            poly[rj, ri] = block.T
            both(poly_copy, core, index, start, SQUARES)
            return 0
        lax.fori_loop(0, 5, square, 0)

        def part_drain(i, carry):
            part_copy(i).wait_send()
            return carry
        pl.when(t > 0)(lambda: lax.fori_loop(0, 5, part_drain, None))

        def tile_load(q):
            c, m = q // 2, lax.rem(q, 2)
            slot = lax.rem(q, 2)
            return pltpu.make_async_copy(wcol_ref.at[pl.ds(2 * m, 2), :, span(c, CHUNK)], parts.at[pl.ds(2 * slot, 2)], tile_sem.at[slot])

        @pl.when(t == NS_STEPS - 1)
        def _():
            for side in (0, 1):
                for from_core in range(CORES):
                    w_first(side, 0, 1 - side, from_core).wait_recv()
                    w_forward(side, from_core).wait_recv()
            w_pair().wait_recv()
            w_own().wait()
            tile_load(0).start()
            tile_load(1).start()

        def poly_ready(q):
            @pl.when(q == 0)
            def _():
                for index in range(4):
                    both(poly_copy, 1 - core, index, arrived, SQUARES)

            @pl.when(q == 1)
            def _():
                both(poly_copy, 1 - core, 4, arrived, SQUARES)

        def far_ready(c):
            @pl.when(t == 0)
            def _():
                for side in (0, 1):
                    for from_core in range(CORES):
                        pass_copy(side, from_core, c).wait()

        @pl.when(t < NS_STEPS - 1)
        def _():
            def apply_half(q, _):
                pl.when(q == 0)(lambda: far_ready(0))
                poly_ready(q)
                keep(q, t, apply_value(q, t))
                return 0
            lax.fori_loop(0, 2, apply_half, 0)

            def apply_chunk(c, _):
                far_ready(c)
                src = slot_of(c, t)
                total = jnp.dot(poly[...], x_ref[src], preferred_element_type=F32)
                x_ref[slot_of(c, t + 1)] = (COEF_A * x_ref[src].astype(F32) + total).astype(BF16)
                return 0
            lax.fori_loop(1, num_chunks, apply_chunk, 0)

        @pl.when(t == NS_STEPS - 1)
        def _():
            def out_pair(q):
                c, m = q // 2, lax.rem(q, 2)
                slot = lax.rem(q, 2)
                where = wb_ref.at[pl.ds(m * per_tall, per_tall), :, pl.ds(pl.multiple_of(core * half + c * CHUNK, CHUNK), CHUNK)]
                tile = own.at[pl.ds(slot * per_tall, per_tall)]
                return (pltpu.make_async_copy(tile, where, out_sem.at[slot]),
                        remote(tile, where, out_send.at[slot], out_recv.at[q], partner))

            def row_pair(c):
                slot = slot_of(c, t + 1)
                cols = pl.ds(pl.multiple_of(core * half + c * CHUNK, CHUNK), CHUNK)
                return (pltpu.make_async_copy(x_ref.at[slot, span(me, slab), :], xrow_ref.at[:, cols], row_sem.at[c]),
                        remote(x_ref.at[slot, span(partner, slab), :], xrow_ref.at[:, cols], row_send.at[c], row_recv.at[c], partner))

            def out_ready(q):
                tile_load(q).wait()

                @pl.when(q >= 2)
                def _():
                    here, there = out_pair(q - 2)
                    here.wait()
                    there.wait_send()

            def new_weight(q):
                c, m = q // 2, lax.rem(q, 2)
                slot = lax.rem(q, 2)
                old = parts[pl.ds(2 * slot, 2)].reshape(tall, CHUNK)
                ortho = x_ref[slot_of(c, t + 1), span(m, tall), :].astype(F32)
                new = ((1.0 - LEARN_RATE * WEIGHT_DECAY) * old - (LEARN_RATE * scale) * ortho).astype(BF16)
                own[pl.ds(slot * per_tall, per_tall)] = new.reshape(per_tall, slab, CHUNK)

            def out_start(q):
                here, there = out_pair(q)
                here.start()
                there.start()

            def last_step(q, _):
                if NS_STEPS == 1:
                    pl.when(lax.rem(q, 2) == 0)(lambda: far_ready(q // 2))
                poly_ready(q)
                keep(q, t, apply_value(q, t))
                out_ready(q)
                new_weight(q)
                out_start(q)

                @pl.when(q + 2 < 2 * num_chunks)
                def _():
                    tile_load(q + 2).start()

                @pl.when(lax.rem(q, 2) == 1)
                def _():
                    here, there = row_pair(q // 2)
                    here.start()
                    there.start()
                return 0
            last = 2 * num_chunks - 1
            lax.fori_loop(0, last + 1, last_step, 0)
            for q in (last - 1, last):
                here, there = out_pair(q)
                here.wait()
                there.wait_send()

            def out_arrival(q, _):
                c, m = q // 2, lax.rem(q, 2)
                where = wb_ref.at[pl.ds(m * per_tall, per_tall), :, pl.ds(pl.multiple_of((1 - core) * half + c * CHUNK, CHUNK), CHUNK)]
                remote(own.at[pl.ds(0, per_tall)], where, out_send.at[0], out_recv.at[q], partner).wait_recv()
                return 0
            lax.fori_loop(0, 2 * num_chunks, out_arrival, 0)

            def row_end(c, _):
                here, there = row_pair(c)
                here.wait()
                there.wait()
                return 0
            lax.fori_loop(0, num_chunks, row_end, 0)

        def drain(i, _):
            @pl.when(t > 0)
            def _():
                both(gram_copy, core, i, left)
            both(poly_copy, core, i, left, SQUARES)
            return 0
        lax.fori_loop(0, 5, drain, 0)
        return 0
    lax.fori_loop(0, NS_STEPS, step, 0)

    for part in (0, 1):
        for side in (0, 1):
            for h in range(CORES):
                w_first(side, h, part).wait_send()
    for side in (0, 1):
        for from_core in range(CORES):
            w_forward(side, from_core).wait_send()
    w_pair().wait_send()

    def paired(i, _):
        pair_copy(i).wait_send()
        return 0
    lax.fori_loop(0, chips * pieces, paired, 0)


def solution(mesh):
    group = mesh.shape['dp']

    def local_step(grad_part, momentum, weight):
        slab, num_cols = weight.shape[1:]
        rows = slab * group
        half = num_cols // CORES
        scale = 0.2 * math.sqrt(max(rows, num_cols))
        num_chunks = half // CHUNK
        chips = group // CORES
        pieces = slab // PIECE
        anywhere = pl.BlockSpec(memory_space=pl.ANY)
        dma = pltpu.SemaphoreType.DMA
        shape = jax.ShapeDtypeStruct

        def kernel(*refs):
            muon(group, rows, half, scale, *refs)
        outs = pl.pallas_call(
            kernel,
            name='muon',
            out_shape=(shape((group, slab, num_cols), BF16), shape((slab, num_cols), BF16), shape((slab, num_cols), F32),
                       shape((chips, CORES * slab, half), F32), shape((chips, slab, num_cols), F32), shape((3, 2, slab, half), F32)),
            in_specs=[anywhere] * 3,
            out_specs=(anywhere,) * 6,
            scratch_shapes=[
                pltpu.VMEM((num_chunks + 1, rows, CHUNK), BF16),
                pltpu.VMEM((rows, rows), BF16),
                pltpu.VMEM((rows, rows), BF16),
                pltpu.VMEM((10, BLOCK, BLOCK), F32),
                pltpu.VMEM((5, BLOCK, BLOCK), F32),
                pltpu.VMEM((6, PIECE, half), F32),
                pltpu.VMEM((2, DEPTH, PIECE, half), F32),
                pltpu.VMEM((CORES * num_chunks, slab, CHUNK), BF16),
                pltpu.VMEM((8, half), F32),
                pltpu.VMEM((8, 128), F32),
                pltpu.VMEM((group, 8, 128), F32),
                dma((chips * pieces,)), dma((chips * pieces,)), dma((2, DEPTH)), dma((3, 2, pieces)), dma((6,)),
                dma((group,)), dma((group,)), dma((2, 2, pieces)), dma((2, 2, pieces)), dma((pieces,)), dma((pieces,)),
                dma((2, 2, num_chunks)), dma((2, 2, num_chunks)), dma((2,)), dma((2,)), dma((2, 2)), dma((2, 2)),
                dma((5,)), dma((5,)), dma((5, 2)), dma((5, 2)), dma((5, 2)), dma((5, 2)),
                dma((2, 2, 2)), dma((2, 2, 2)), dma((2, 2)), dma((2, 2)),
                dma((5,)),
                dma((2,)), dma((2,)), dma((2 * num_chunks,)),
                dma((num_chunks,)), dma((num_chunks,)), dma((num_chunks,)),
            ],
            compiler_params=pltpu.CompilerParams(collective_id=1, has_side_effects=True, vmem_limit_bytes=67043328),
        )(grad_part[0, 0], momentum[0], weight[0])
        weight_bf16, ortho, new_momentum = outs[:3]
        new_weight = weight - LEARN_RATE * (scale * ortho[None].astype(F32) + WEIGHT_DECAY * weight)
        return new_momentum[None], new_weight, weight_bf16.reshape(1, rows, num_cols)

    return jax.shard_map(local_step, mesh=mesh, in_specs=(P(('mp', 'dp')), P('mp', 'dp'), P('mp', 'dp')), out_specs=(P('mp', 'dp'), P('mp', 'dp'), P('mp')), check_vma=False)
```

```python
import math
import jax
import jax.numpy as jnp
from jax import lax
from jax.experimental import pallas as pl
from jax.experimental.pallas import tpu as pltpu
from jax.sharding import PartitionSpec as P

MOMENTUM = 0.95
LEARN_RATE = 2.0
WEIGHT_DECAY = 0.25
NS_STEPS = 5
COEF_A = 3.4445
COEF_B = -4.7750
COEF_C = 2.0315

MESH = pl.DeviceIdType.MESH
F32, BF16 = jnp.float32, jnp.bfloat16
CORES = 2
BLOCK = 512
CHUNK = 512
DEPTH = 4
EAGER = 4
EARLY = 1
W_EARLY = 5
OTHERS = ((0, 1), (2, 3, 4))
BLOCKS = (((0, 0), (2, 1), (3, 1), (2, 0), (3, 3)), ((1, 1), (1, 0), (3, 0), (3, 2), (2, 2)))
SQUARES = (((0, 0), (3, 0), (3, 1), (3, 2), (3, 3)), ((1, 1), (1, 0), (2, 0), (2, 1), (2, 2)))
NEAR = (((0, 2), (0, 1), (0, 0)), ((2, 2), (1, 2), (1, 1)))


def block_of(core, index, table=BLOCKS):
    def pick(owner, i):
        values = [block[i] for block in table[owner]]
        if isinstance(index, int):
            return values[index]
        result = jnp.int32(values[0])
        for place, value in enumerate(values[1:], 1):
            result = jnp.where(index == place, jnp.int32(value), result)
        return result
    return tuple(jnp.where(core == 0, pick(0, i), pick(1, i)) for i in range(2))


def diagonal(index):
    return isinstance(index, int) and index in (0, 4)


def span(index, size):
    return pl.ds(pl.multiple_of(index * size, size), size)


def muon(group, rows, half, scale, grad_ref, mom_ref, w_ref, wb_ref, xrow_ref, nmom_ref, wcol_ref, pair_ref, arrived_ref,
         x_ref, gram, poly, parts, part_in, square_acc, sq_out, sq_in,
         pair_send, pair_recv, rs_send, rs_recv, in_sem, sq_send, sq_recv, up_send, up_recv, mate_send, mate_recv, pass_send, pass_recv, far_send, far_recv, share_send, share_recv,
         part_send, part_recv, gram_send, gram_recv, poly_send, poly_recv,
         w_send, w_recv, w_fwd_send, w_fwd_recv, w_mate_send, w_mate_recv, w_own_sem, tile_sem, out_sem, out_send, out_recv, row_sem, row_send, row_recv):
    me = lax.axis_index('dp')
    core, chip = lax.rem(me, CORES), me // CORES
    chips = group // CORES
    slab = rows // group
    partner = chip * CORES + (1 - core)
    side_chip = (lax.rem(chip + 1, chips), lax.rem(chip + chips - 1, chips))
    far_chip = lax.rem(chip + 2, chips)
    num_chunks = half // CHUNK
    slots = num_chunks + 1

    def remote(src, dst, send, recv, device):
        return pltpu.make_async_remote_copy(src, dst, send, recv, device_id={'dp': device}, device_id_type=MESH)

    barrier = pltpu.get_barrier_semaphore()
    for other in range(1, group):
        pl.semaphore_signal(barrier, inc=1, device_id={'dp': lax.rem(me + other, group)}, device_id_type=MESH)
    pl.semaphore_wait(barrier, group - 1)

    def tile(index):
        return parts.at[index // 2, pl.ds(pl.multiple_of(lax.rem(index, 2) * slab, slab), slab), :]

    def staged(side, slot):
        return tile(6 + side * DEPTH + slot)

    def own(index):
        return poly.at[span(index // 4, slab), span(lax.rem(index, 4), CHUNK)]

    def dest_chip(order):
        return jnp.where(order == 0, far_chip, jnp.where(order == 1, side_chip[0], jnp.where(order == 2, side_chip[1], chip)))

    def rows_of(device):
        return span(device, slab)

    def columns(which, j):
        return pl.ds(pl.multiple_of(which * half + j * CHUNK, CHUNK), CHUNK)

    def pair_copy(order, j, which):
        i = (order * num_chunks + j) * 2 + which
        return remote(grad_ref.at[rows_of(dest_chip(order) * CORES + 1 - core), columns(which, j)], pair_ref.at[order, :, columns(which, j)],
                      pair_send.at[i], pair_recv.at[i], partner)

    def pair_start(i, _):
        order, j = i // num_chunks, lax.rem(i, num_chunks)
        for which in (0, 1):
            pair_copy(order, j, which).start()
        return 0
    lax.fori_loop(0, chips * num_chunks, pair_start, 0)

    def grad_loads(order, j, which, base):
        return (pltpu.make_async_copy(grad_ref.at[rows_of(dest_chip(order) * CORES + core), columns(which, j)], tile(base), in_sem.at[base]),
                pltpu.make_async_copy(pair_ref.at[order, :, columns(which, j)], tile(base + 1), in_sem.at[base + 1]))

    def arrived_load(phase, side, j, base):
        return pltpu.make_async_copy(arrived_ref.at[phase, side, j], tile(base), in_sem.at[base])

    def rs_copy(q, side):
        phase, j = q // num_chunks, lax.rem(q, num_chunks)
        slot = lax.rem(q, DEPTH)
        return remote(staged(side, slot), arrived_ref.at[phase, side, j],
                      rs_send.at[side, slot], rs_recv.at[phase, side, j], side_chip[side] * CORES + core)

    def up_copy(side, h, j, sender=None):
        return remote(own(h * num_chunks + j), x_ref.at[j, rows_of(me), :],
                      up_send.at[side, h, j], up_recv.at[side, core if sender is None else sender, j], side_chip[side] * CORES + h)

    def mate_copy(j):
        return remote(own((1 - core) * num_chunks + j), x_ref.at[j, rows_of(me), :], mate_send.at[j], mate_recv.at[j], partner)

    def nmom_copy(j, which):
        return pltpu.make_async_copy(tile(5), nmom_ref.at[:, columns(which, j)], in_sem.at[5])

    square_acc[...] = jnp.zeros_like(square_acc)

    def send_sums(q):
        phase, j = q // num_chunks, lax.rem(q, num_chunks)
        slot = lax.rem(q, DEPTH)
        for side in (0, 1):
            order = jnp.where(phase == 0, 0, 1 + side)
            which = jnp.where(phase == 1, 1 - side, side)
            pair_copy(order, j, which).wait_recv()
            for load in grad_loads(order, j, which, 3 * side):
                load.start()

            @pl.when(phase == 2)
            def _():
                rs_copy(j, side).wait_recv()
                arrived_load(0, side, j, 3 * side + 2).start()

        for side in (0, 1):
            order = jnp.where(phase == 0, 0, 1 + side)
            which = jnp.where(phase == 1, 1 - side, side)

            @pl.when(q >= DEPTH)
            def _():
                rs_copy(q - DEPTH, side).wait_send()
            for load in grad_loads(order, j, which, 3 * side):
                load.wait()

            @pl.when(phase == 2)
            def _():
                arrived_load(0, side, j, 3 * side + 2).wait()
                staged(side, slot)[...] = (tile(3 * side)[...] + tile(3 * side + 1)[...]) + tile(3 * side + 2)[...]

            @pl.when(phase != 2)
            def _():
                staged(side, slot)[...] = tile(3 * side)[...] + tile(3 * side + 1)[...]
            rs_copy(q, side).start()

    def send_up(j):
        for side in (0, 1):
            for h in range(CORES):
                up_copy(side, h, j).start()
        mate_copy(j).start()

    def finish(j):
        for which in (0, 1):
            pair_copy(3, j, which).wait_recv()
            loads = list(grad_loads(3, j, which, 0))
            for side in (0, 1):
                phase = 2 if side == which else 1
                rs_copy(phase * num_chunks + j, side).wait_recv()
                loads.append(arrived_load(phase, side, j, 2 + side))
            loads.append(pltpu.make_async_copy(mom_ref.at[:, columns(which, j)], tile(4), in_sem.at[4]))
            for load in loads:
                load.start()
            for load in loads:
                load.wait()
            if which == 1:
                nmom_copy(j, 0).wait()
            mean = (((tile(0)[...] + tile(1)[...]) + tile(2)[...]) + tile(3)[...]) / group
            momentum = MOMENTUM * tile(4)[...] + mean
            tile(5)[...] = momentum
            nmom_copy(j, which).start()
            update = (mean + MOMENTUM * momentum).astype(BF16)
            own(which * num_chunks + j)[...] = update
            as_float = update.astype(F32)
            square_acc[...] += jnp.sum((as_float * as_float).reshape(slab // 8, 8, CHUNK), axis=0)
        nmom_copy(j, 1).wait()

        @pl.when(j < EAGER)
        def _():
            send_up(j)

    def reduce_step(q, _):
        @pl.when(q < 3 * num_chunks)
        def _():
            send_sums(q)

        @pl.when(q >= 2 * num_chunks + DEPTH)
        def _():
            finish(q - 2 * num_chunks - DEPTH)
        return 0
    lax.fori_loop(0, 3 * num_chunks + DEPTH, reduce_step, 0)
    for side in (0, 1):
        for last in range(DEPTH):
            rs_copy(3 * num_chunks - DEPTH + last, side).wait_send()

    total = jnp.sum(square_acc[...])
    sq_out[...] = jnp.full(sq_out.shape, total, F32)
    sq_in[me] = jnp.full(sq_out.shape, total, F32)

    def sq_copy(other):
        return remote(sq_out, sq_in.at[me], sq_send.at[other], sq_recv.at[other], lax.rem(me + other, group))
    for other in range(1, group):
        sq_copy(other).start()

    def send_rest(j, _):
        send_up(j)
        return 0
    lax.fori_loop(EAGER, num_chunks, send_rest, 0)
    for other in range(1, group):
        sq_copy(other).wait()
    square = sq_in[0, 0:1, 0:1]
    for i in range(1, group):
        square = square + sq_in[i, 0:1, 0:1]
    inverse = 1.0 / (jnp.sqrt(square) + 1e-7)

    def normalise(j, row0, size):
        r = pl.ds(pl.multiple_of(row0, slab), size)
        x_ref[j, r, :] = (x_ref[j, r, :].astype(F32) * inverse).astype(BF16)

    def pass_copy(side, c):
        where = x_ref.at[c, rows_of(side_chip[1 - side] * CORES + side), :]
        return remote(where, where, pass_send.at[side, c], pass_recv.at[side, c], side_chip[side] * CORES + core)

    def w_first(side, h, c, sender=None):
        return remote(w_ref.at[:, columns(h, c)], wcol_ref.at[c, chip, span(core, slab), :],
                      w_send.at[side, h, c], w_recv.at[side, core if sender is None else sender, c], side_chip[side] * CORES + h)

    def w_forward(side, c):
        where = wcol_ref.at[c, side_chip[1 - side], pl.ds(side * slab, slab), :]
        return remote(where, where, w_fwd_send.at[side, c], w_fwd_recv.at[side, c], side_chip[side] * CORES + core)

    def w_pair(c):
        return remote(w_ref.at[:, columns(1 - core, c)], wcol_ref.at[c, chip, span(core, slab), :], w_mate_send.at[c], w_mate_recv.at[c], partner)

    def w_own(c):
        return pltpu.make_async_copy(w_ref.at[:, columns(core, c)], wcol_ref.at[c, chip, span(core, slab), :], w_own_sem.at[c])

    def w_pass(c):
        for side in (0, 1):
            w_first(side, 0, c, side).wait_recv()
            w_forward(side, c).start()

    def w_ready(c):
        for side in (0, 1):
            w_first(side, 0, c, 1 - side).wait_recv()
            w_forward(side, c).wait_recv()
        w_pair(c).wait_recv()
        w_own(c).wait()

    def slot_of(c, t):
        return lax.rem(c + 2 * slots - t, slots)

    def gram_copy(b, index, row, col):
        where = gram.at[span(row, BLOCK), span(col, BLOCK)]
        return remote(where, where, gram_send.at[index, b], gram_recv.at[index, b], partner)

    def poly_copy(b, index, row, col):
        where = poly.at[span(row, BLOCK), span(col, BLOCK)]
        return remote(where, where, poly_send.at[index, b], poly_recv.at[index, b], partner)

    def both(copy, owner, index, act, table=BLOCKS):
        row, col = block_of(owner, index, table)
        if not diagonal(index):
            act(copy(1, index, col, row))
        act(copy(0, index, row, col))

    def start(copy):
        copy.start()

    def arrived(copy):
        copy.wait_recv()

    def left(copy):
        copy.wait_send()

    def part_copy(index):
        return remote(parts.at[index], part_in.at[index], part_send.at[index], part_recv.at[index], partner)

    small = BLOCK // 2
    ROWS_ROWS = (((1,), (1,)), ((), ()))

    def product(rows_at, index, row, col):
        if diagonal(index):
            left = lax.dot_general(rows_at(row, 0, BLOCK), rows_at(row, 0, small), ROWS_ROWS, preferred_element_type=F32)
            corner = lax.dot_general(rows_at(row, small, small), rows_at(row, small, small), ROWS_ROWS, preferred_element_type=F32)
            return left, corner
        return (lax.dot_general(rows_at(row, 0, BLOCK), rows_at(col, 0, BLOCK), ROWS_ROWS, preferred_element_type=F32),)

    def pieces_of(ref, value):
        if len(value) == 2:
            return (ref[:, 0:small], ref[small:, small:])
        return (ref[...],)

    def put_block(ref, row, col, value):
        if len(value) == 2:
            at = ref.at[span(row, BLOCK), span(row, BLOCK)]
            left, corner = (v.astype(BF16) for v in value)
            at[:, 0:small] = left
            at[small:, small:] = corner
            at[0:small, small:] = left[small:].T
        else:
            block = value[0].astype(BF16)
            ref[span(row, BLOCK), span(col, BLOCK)] = block
            ref[span(col, BLOCK), span(row, BLOCK)] = block.T

    def x_rows(t):
        def rows_at(block, offset, size):
            r = pl.ds(pl.multiple_of(block * BLOCK + offset, small), size)
            return jnp.concatenate([x_ref[slot_of(c, t), r, :] for c in range(num_chunks)], axis=1)
        return rows_at

    def gram_rows(block, offset, size):
        return gram[pl.ds(pl.multiple_of(block * BLOCK + offset, small), size), :]

    def near_chip(order):
        return (chip, side_chip[0], side_chip[1])[order]

    def near_block(one, two):
        one, two = near_chip(one), near_chip(two)
        return jnp.maximum(one, two), jnp.minimum(one, two)

    def near_owned(owner, place):
        rows_cols = [(near_block(*NEAR[c][place])) for c in range(CORES)]
        return tuple(jnp.where(owner == 0, rows_cols[0][i], rows_cols[1][i]) for i in range(2))

    def near_sum(j, place):
        row, col = near_owned(jnp.where(place < 3, 1 - core, core), place % 3)
        value = lax.dot_general(x_ref[j, span(row, BLOCK), :], x_ref[j, span(col, BLOCK), :], (((1,), (1,)), ((), ())), preferred_element_type=F32)
        slot = place % 3 + 5 * (place // 3)

        @pl.when(j == 0)
        def _():
            parts[slot] = value

        @pl.when(j > 0)
        def _():
            parts[slot] = parts[slot] + value

    def near_copy(place, b):
        row, col = near_owned(core, place)
        if b == 1:
            row, col = col, row
        where = gram.at[span(row, BLOCK), span(col, BLOCK)]
        return remote(where, where, gram_send.at[place, b], gram_recv.at[place, b], partner)

    def near_both(place, act):
        act(near_copy(place, 0))
        row, col = near_owned(core, place)

        @pl.when(row != col)
        def _():
            act(near_copy(place, 1))

    def near_arrived(place):
        near_copy(place, 0).wait_recv()
        row, col = near_owned(1 - core, place)

        @pl.when(row != col)
        def _():
            near_copy(place, 1).wait_recv()

    def arrive(j, _):
        x_ref[j, rows_of(me), :] = (own(core * num_chunks + j)[...].astype(F32) * inverse).astype(BF16)
        mate_copy(j).wait_recv()
        normalise(j, partner * slab, slab)
        for side in (0, 1):
            for from_core in range(CORES):
                up_copy(side, core, j, from_core).wait_recv()
            normalise(j, side_chip[1 - side] * CORES * slab, CORES * slab)
        for place in range(6):
            near_sum(j, place)
        return 0

    def far_block(chip_index, core_index, side):
        right, behind = lax.rem(chip_index + 1, chips), lax.rem(chip_index + chips - 1, chips)
        if side == 1:
            one, two = jnp.where(core_index == 0, chip_index, behind), right
        else:
            one, two = jnp.where(core_index == 0, chip_index, behind), behind
        return jnp.maximum(one, two), jnp.minimum(one, two)

    def far_copy(side):
        row, col = far_block(chip, core, side)
        where = gram.at[span(row, BLOCK), span(col, BLOCK)]
        return remote(where, where, far_send.at[side], far_recv.at[side], side_chip[side] * CORES + core)

    def share_copy(side, owner, b):
        row, col = far_block(side_chip[1 - side], owner, side)
        if b == 1:
            row, col = col, row
        where = gram.at[span(row, BLOCK), span(col, BLOCK)]
        return remote(where, where, share_send.at[side, b], share_recv.at[side, b], partner)

    def share(side, owner, act):
        act(share_copy(side, owner, 0))
        row, col = far_block(side_chip[1 - side], owner, side)

        @pl.when(row != col)
        def _():
            act(share_copy(side, owner, 1))

    lax.fori_loop(0, num_chunks, arrive, 0)

    def sent(j, _):
        for side in (0, 1):
            for h in range(CORES):
                up_copy(side, h, j).wait_send()
        mate_copy(j).wait_send()
        return 0
    lax.fori_loop(0, num_chunks, sent, 0)

    for place in range(3):
        part_copy(place).start()

    for c in range(EARLY):
        for side in (0, 1):
            pass_copy(side, c).start()
    for place in range(3):
        part_copy(place).wait_recv()
        row, col = near_owned(core, place)
        block = (parts[5 + place] + part_in[place]).astype(BF16)
        gram[span(row, BLOCK), span(col, BLOCK)] = block
        if place < 2:
            far_copy(place).start()

        @pl.when(row != col)
        def _():
            gram[span(col, BLOCK), span(row, BLOCK)] = block.T
        near_both(place, start)
    for c in range(EARLY, num_chunks):
        for side in (0, 1):
            pass_copy(side, c).start()

    def w_start(c, _):
        for h in range(CORES):
            for side in (0, 1):
                w_first(side, h, c).start()
        w_pair(c).start()
        w_own(c).start()
        return 0
    lax.fori_loop(0, num_chunks, w_start, 0)
    for place in range(3):
        near_arrived(place)
    for side in (0, 1):
        far_copy(side).wait_recv()
        row, col = far_block(side_chip[1 - side], core, side)
        turned = gram[span(row, BLOCK), span(col, BLOCK)].T

        @pl.when(row != col)
        def _():
            gram[span(col, BLOCK), span(row, BLOCK)] = turned
        share(side, core, start)
    for side in (0, 1):
        share(side, 1 - core, arrived)
        far_copy(side).wait_send()
        share(side, core, left)
    for place in range(3):
        near_both(place, left)
        part_copy(place).wait_send()

    tall = 1024

    def apply_value(q, t):
        c, m = q // 2, lax.rem(q, 2)
        rm = span(m, tall)
        src = slot_of(c, t)
        total = jnp.dot(poly[rm, :], x_ref[src], preferred_element_type=F32)
        return (COEF_A * x_ref[src, rm, :].astype(F32) + total).astype(BF16)

    def keep(q, t, value):
        x_ref[slot_of(q // 2, t + 1), span(lax.rem(q, 2), tall), :] = value

    def step(t, _):
        def pass_weights(low, high):
            @pl.when(t == NS_STEPS - 2)
            def _():
                def one(c, _):
                    w_pass(c)
                    return 0
                lax.fori_loop(low, high, one, 0)
        pass_weights(0, W_EARLY)

        @pl.when(t > 0)
        def _():
            for group_of in OTHERS:
                for index in group_of:
                    row, col = block_of(1 - core, index)
                    value = product(x_rows(t), index, row, col)
                    if len(value) == 2:
                        parts[index, :, 0:small] = value[0]
                        parts[index, small:, small:] = value[1]
                    else:
                        parts[index] = value[0]
                for index in group_of:
                    part_copy(index).start()

            def gram_own(*indices):
                for index in indices:
                    part_copy(index).wait_recv()
                for index in indices:
                    row, col = block_of(core, index)
                    value = product(x_rows(t), index, row, col)
                    put_block(gram, row, col, tuple(v + w for v, w in zip(value, pieces_of(part_in.at[index], value))))
                for index in indices:
                    both(gram_copy, core, index, start)

            def gram_middle(index, _):
                gram_own(index)
                return 0
            gram_own(0, 1)
            lax.fori_loop(2, 4, gram_middle, 0)
            gram_own(4)

        def squares(indices, needs):
            @pl.when(t > 0)
            def _():
                for index in needs:
                    both(gram_copy, 1 - core, index, arrived)
            for index in indices:
                row, col = block_of(core, index, SQUARES)
                value = product(gram_rows, index, row, col)
                old = pieces_of(gram.at[span(row, BLOCK), span(col, BLOCK)], value)
                put_block(poly, row, col, tuple(COEF_B * g.astype(F32) + COEF_C * v for g, v in zip(old, value)))
            for index in indices:
                both(poly_copy, core, index, start, SQUARES)
        squares((0,), (0, 1, 2))
        squares((1,), (3,))
        squares((2,), ())
        squares((3,), (4,))
        squares((4,), ())

        def part_drain(i, carry):
            part_copy(i).wait_send()
            return carry
        pl.when(t > 0)(lambda: lax.fori_loop(0, 5, part_drain, None))

        def tile_load(q):
            c, m = q // 2, lax.rem(q, 2)
            slot = lax.rem(q, 2)
            return pltpu.make_async_copy(wcol_ref.at[c, pl.ds(2 * m, 2)], parts.at[pl.ds(2 * slot, 2)], tile_sem.at[slot])

        @pl.when(t == NS_STEPS - 1)
        def _():
            w_ready(0)
            if NS_STEPS > 1:
                for index in range(5):
                    both(gram_copy, core, index, left)
            tile_load(0).start()
            tile_load(1).start()

        def poly_ready(indices):
            for index in indices:
                both(poly_copy, 1 - core, index, arrived, SQUARES)

        def far_ready(c):
            @pl.when(t == 0)
            def _():
                for side in (0, 1):
                    pass_copy(side, c).wait()

        def apply_rows(c, low, high):
            src = slot_of(c, t)
            total = jnp.dot(poly[low:high, :], x_ref[src], preferred_element_type=F32)
            x_ref[slot_of(c, t + 1), low:high, :] = (COEF_A * x_ref[src, low:high, :].astype(F32) + total).astype(BF16)
        far_ready(0)
        poly_ready((0, 1, 2))
        apply_rows(0, 0, BLOCK)
        pass_weights(W_EARLY, num_chunks)
        poly_ready((3, 4))
        apply_rows(0, BLOCK, rows)

        @pl.when(t < NS_STEPS - 1)
        def _():
            def apply_chunk(c, _):
                far_ready(c)
                apply_rows(c, 0, rows)
                return 0
            lax.fori_loop(1, num_chunks, apply_chunk, 0)

        @pl.when(t == NS_STEPS - 1)
        def _():
            def out_pair(q):
                c, m = q // 2, lax.rem(q, 2)
                slot = lax.rem(q, 2)
                where = wb_ref.at[span(m, tall), columns(core, c)]
                new = gram.at[span(slot, tall), 0:CHUNK]
                return (pltpu.make_async_copy(new, where, out_sem.at[slot]),
                        remote(new, where, out_send.at[slot], out_recv.at[q], partner))

            def row_pair(c):
                slot = slot_of(c, t + 1)
                cols = pl.ds(pl.multiple_of(core * half + c * CHUNK, CHUNK), CHUNK)
                return (pltpu.make_async_copy(x_ref.at[slot, span(me, slab), :], xrow_ref.at[:, cols], row_sem.at[c]),
                        remote(x_ref.at[slot, span(partner, slab), :], xrow_ref.at[:, cols], row_send.at[c], row_recv.at[c], partner))

            def out_ready(q):
                tile_load(q).wait()

                @pl.when(q >= 2)
                def _():
                    here, there = out_pair(q - 2)
                    here.wait()
                    there.wait_send()

            def new_weight(q):
                c, m = q // 2, lax.rem(q, 2)
                slot = lax.rem(q, 2)
                old = parts[pl.ds(2 * slot, 2)].reshape(tall, CHUNK)
                ortho = x_ref[slot_of(c, t + 1), span(m, tall), :].astype(F32)
                new = ((1.0 - LEARN_RATE * WEIGHT_DECAY) * old - (LEARN_RATE * scale) * ortho).astype(BF16)
                gram[span(slot, tall), 0:CHUNK] = new

            def out_start(q):
                here, there = out_pair(q)
                here.start()
                there.start()

            def last_step(q, _):
                if NS_STEPS == 1:
                    pl.when(lax.rem(q, 2) == 0)(lambda: far_ready(q // 2))
                keep(q, t, apply_value(q, t))
                out_ready(q)
                new_weight(q)
                out_start(q)

                @pl.when(q + 2 < 2 * num_chunks)
                def _():
                    pl.when(lax.rem(q, 2) == 0)(lambda: w_ready(q // 2 + 1))
                    tile_load(q + 2).start()

                @pl.when(lax.rem(q, 2) == 1)
                def _():
                    here, there = row_pair(q // 2)
                    here.start()
                    there.start()
                return 0
            last = 2 * num_chunks - 1
            for q in (0, 1):
                out_ready(q)
                new_weight(q)
                out_start(q)
                if q == 0:
                    w_ready(1)
                tile_load(q + 2).start()
            for copy in row_pair(0):
                copy.start()
            lax.fori_loop(2, last + 1, last_step, 0)
            for q in (last - 1, last):
                here, there = out_pair(q)
                here.wait()
                there.wait_send()

            def out_arrival(q, _):
                c, m = q // 2, lax.rem(q, 2)
                where = wb_ref.at[span(m, tall), columns(1 - core, c)]
                remote(gram.at[0:tall, 0:CHUNK], where, out_send.at[0], out_recv.at[q], partner).wait_recv()
                return 0
            lax.fori_loop(0, 2 * num_chunks, out_arrival, 0)

            def row_end(c, _):
                here, there = row_pair(c)
                here.wait()
                there.wait()
                return 0
            lax.fori_loop(0, num_chunks, row_end, 0)

        for index in range(5):
            @pl.when((t > 0) & (t < NS_STEPS - 1))
            def _():
                both(gram_copy, core, index, left)
            both(poly_copy, core, index, left, SQUARES)
        return 0
    lax.fori_loop(0, NS_STEPS, step, 0)

    def w_end(c, _):
        for side in (0, 1):
            for h in range(CORES):
                w_first(side, h, c).wait_send()
            w_forward(side, c).wait_send()
        w_pair(c).wait_send()
        return 0
    lax.fori_loop(0, num_chunks, w_end, 0)

    def paired(i, _):
        order, j = i // num_chunks, lax.rem(i, num_chunks)
        for which in (0, 1):
            pair_copy(order, j, which).wait_send()
        return 0
    lax.fori_loop(0, chips * num_chunks, paired, 0)


def hand_over(decay, step, wide_ref, nmom_ref, xrow_ref, w_ref, wide_out, nmom_out, weight_out, wide, nmom, xrow, weight, load_sem, store_sem):
    count = wide.shape[0]
    loads = [pltpu.make_async_copy(w_ref, weight, load_sem.at[count]), pltpu.make_async_copy(xrow_ref, xrow, load_sem.at[count + 1])]
    loads += [pltpu.make_async_copy(nmom_ref, nmom, load_sem.at[count + 2])]
    loads += [pltpu.make_async_copy(wide_ref.at[i], wide.at[i], load_sem.at[i]) for i in range(count)]
    stores = [pltpu.make_async_copy(weight, weight_out, store_sem.at[count]), pltpu.make_async_copy(nmom, nmom_out, store_sem.at[count + 2])]
    stores += [pltpu.make_async_copy(wide.at[i], wide_out.at[i], store_sem.at[i]) for i in range(count)]
    for load in loads:
        load.start()
    loads[0].wait()
    loads[1].wait()

    def rows_of(i, _):
        r = span(i, 16)
        weight[r, :] = decay * weight[r, :] - step * xrow[r, :].astype(F32)
        return 0
    lax.fori_loop(0, weight.shape[0] // 16, rows_of, 0)
    stores[0].start()
    for load, store in zip(loads[2:], stores[1:]):
        load.wait()
        store.start()
    for store in stores:
        store.wait()


def solution(mesh):
    group = mesh.shape['dp']

    def local_step(grad_part, momentum, weight):
        slab, num_cols = weight.shape[1:]
        rows = slab * group
        half = num_cols // CORES
        scale = 0.2 * math.sqrt(max(rows, num_cols))
        num_chunks = half // CHUNK
        chips = group // CORES
        anywhere = pl.BlockSpec(memory_space=pl.ANY)
        dma = pltpu.SemaphoreType.DMA
        shape = jax.ShapeDtypeStruct

        def kernel(*refs):
            muon(group, rows, half, scale, *refs)
        outs = pl.pallas_call(
            kernel,
            name='muon',
            out_shape=(shape((rows, num_cols), BF16), shape((slab, num_cols), BF16), shape((slab, num_cols), F32),
                       shape((num_chunks, chips, CORES * slab, CHUNK), F32), shape((chips, slab, num_cols), F32), shape((3, 2, num_chunks, slab, CHUNK), F32)),
            in_specs=[anywhere] * 3,
            out_specs=(anywhere,) * 6,
            scratch_shapes=[
                pltpu.VMEM((num_chunks + 1, rows, CHUNK), BF16),
                pltpu.VMEM((rows, rows), BF16),
                pltpu.VMEM((rows, rows), BF16),
                pltpu.VMEM((10, BLOCK, BLOCK), F32),
                pltpu.VMEM((5, BLOCK, BLOCK), F32),
                pltpu.VMEM((8, CHUNK), F32),
                pltpu.VMEM((8, 128), F32),
                pltpu.VMEM((group, 8, 128), F32),
                dma((chips * num_chunks * 2,)), dma((chips * num_chunks * 2,)), dma((2, DEPTH)), dma((3, 2, num_chunks)), dma((6,)),
                dma((group,)), dma((group,)), dma((2, 2, num_chunks)), dma((2, 2, num_chunks)), dma((num_chunks,)), dma((num_chunks,)),
                dma((2, num_chunks)), dma((2, num_chunks)), dma((2,)), dma((2,)), dma((2, 2)), dma((2, 2)),
                dma((5,)), dma((5,)), dma((5, 2)), dma((5, 2)), dma((5, 2)), dma((5, 2)),
                dma((2, 2, num_chunks)), dma((2, 2, num_chunks)), dma((2, num_chunks)), dma((2, num_chunks)),
                dma((num_chunks,)), dma((num_chunks,)), dma((num_chunks,)), dma((2,)),
                dma((2,)), dma((2,)), dma((2 * num_chunks,)),
                dma((num_chunks,)), dma((num_chunks,)), dma((num_chunks,)),
            ],
            compiler_params=pltpu.CompilerParams(collective_id=1, has_side_effects=True, vmem_limit_bytes=67043328),
        )(grad_part[0, 0], momentum[0], weight[0])
        weight_bf16, ortho, new_momentum = outs[:3]

        def last_kernel(*refs):
            hand_over(1.0 - LEARN_RATE * WEIGHT_DECAY, LEARN_RATE * scale, *refs)
        weight_bf16, new_momentum, new_weight = pl.pallas_call(
            last_kernel,
            name='hand_over',
            out_shape=(shape((group, slab, num_cols), BF16), shape((slab, num_cols), F32), shape((slab, num_cols), F32)),
            in_specs=[anywhere] * 4,
            out_specs=(anywhere,) * 3,
            scratch_shapes=[
                pltpu.VMEM((group, slab, num_cols), BF16),
                pltpu.VMEM((slab, num_cols), F32),
                pltpu.VMEM((slab, num_cols), BF16),
                pltpu.VMEM((slab, num_cols), F32),
                dma((group + 3,)), dma((group + 3,)),
            ],
            compiler_params=pltpu.CompilerParams(vmem_limit_bytes=56 * 2 ** 20),
        )(weight_bf16.reshape(group, slab, num_cols), new_momentum, ortho, weight[0])
        return new_momentum[None], new_weight[None], weight_bf16.reshape(1, rows, num_cols)

    return jax.shard_map(local_step, mesh=mesh, in_specs=(P(('mp', 'dp')), P('mp', 'dp'), P('mp', 'dp')), out_specs=(P('mp', 'dp'), P('mp', 'dp'), P('mp')), check_vma=False)
```

```python
import math
import jax
import jax.numpy as jnp
from jax import lax
from jax.experimental import pallas as pl
from jax.experimental.pallas import tpu as pltpu
from jax.sharding import PartitionSpec as P

MOMENTUM = 0.95
LEARN_RATE = 2.0
WEIGHT_DECAY = 0.25
NS_STEPS = 5
COEF_A = 3.4445
COEF_B = -4.7750
COEF_C = 2.0315

MESH = pl.DeviceIdType.MESH
F32, BF16 = jnp.float32, jnp.bfloat16
CORES = 2
BLOCK = 512
CHUNK = 512
DEPTH = 4
KEPT = 4
VMEM_ROOM = 67 * 2 ** 18
EAGER = 4
EARLY = 1
W_EARLY = 5
OTHERS = ((0, 1), (2, 3, 4))
BLOCKS = (((0, 0), (2, 1), (3, 1), (2, 0), (3, 3)), ((1, 1), (1, 0), (3, 0), (3, 2), (2, 2)))
SQUARES = (((0, 0), (3, 0), (3, 1), (3, 2), (3, 3)), ((1, 1), (1, 0), (2, 0), (2, 1), (2, 2)))
NEAR = (((0, 2), (0, 1), (0, 0)), ((2, 2), (1, 2), (1, 1)))


def block_of(core, index, table=BLOCKS):
    def pick(owner, i):
        values = [block[i] for block in table[owner]]
        if isinstance(index, int):
            return values[index]
        result = jnp.int32(values[0])
        for place, value in enumerate(values[1:], 1):
            result = jnp.where(index == place, jnp.int32(value), result)
        return result
    return tuple(jnp.where(core == 0, pick(0, i), pick(1, i)) for i in range(2))


def diagonal(index):
    return isinstance(index, int) and index in (0, 4)


def span(index, size):
    return pl.ds(pl.multiple_of(index * size, size), size)


def muon(group, rows, half, scale, grad_ref, mom_ref, w_ref, x_ref, gram, parts, nmom_ref, wide_ref, rest_ref, wcol_ref, pair_ref, arrived_ref,
         poly, square_acc, sq_out, sq_in,
         pair_send, pair_recv, rs_send, rs_recv, in_sem, sq_send, sq_recv, up_send, up_recv, mate_send, mate_recv, pass_send, pass_recv,
         far_send, far_recv, share_send, share_recv, part_send, part_recv, gram_send, gram_recv, poly_send, poly_recv,
         w_send, w_recv, w_fwd_send, w_fwd_recv, w_mate_send, w_mate_recv, w_own_sem, tile_sem, out_send, out_recv, row_send, row_recv):
    me = lax.axis_index('dp')
    core, chip = lax.rem(me, CORES), me // CORES
    chips = group // CORES
    slab = rows // group
    partner = chip * CORES + (1 - core)
    side_chip = (lax.rem(chip + 1, chips), lax.rem(chip + chips - 1, chips))
    far_chip = lax.rem(chip + 2, chips)
    num_chunks = half // CHUNK
    slots = num_chunks + 1

    def remote(src, dst, send, recv, device):
        return pltpu.make_async_remote_copy(src, dst, send, recv, device_id={'dp': device}, device_id_type=MESH)

    barrier = pltpu.get_barrier_semaphore()
    for other in range(1, group):
        pl.semaphore_signal(barrier, inc=1, device_id={'dp': lax.rem(me + other, group)}, device_id_type=MESH)
    pl.semaphore_wait(barrier, group - 1)

    def tile(index):
        return parts.at[index // 2, pl.ds(pl.multiple_of(lax.rem(index, 2) * slab, slab), slab), :]

    def staged(side, slot):
        return tile(6 + side * DEPTH + slot)

    def own(index):
        return poly.at[span(index // 4, slab), span(lax.rem(index, 4), CHUNK)]

    def dest_chip(order):
        return jnp.where(order == 0, far_chip, jnp.where(order == 1, side_chip[0], jnp.where(order == 2, side_chip[1], chip)))

    def rows_of(device):
        return span(device, slab)

    def columns(which, j):
        return pl.ds(pl.multiple_of(which * half + j * CHUNK, CHUNK), CHUNK)

    def pair_copy(order, j, which):
        i = (order * num_chunks + j) * 2 + which
        return remote(grad_ref.at[rows_of(dest_chip(order) * CORES + 1 - core), columns(which, j)], pair_ref.at[order, :, columns(which, j)],
                      pair_send.at[i], pair_recv.at[i], partner)

    def pair_start(i, _):
        order, j = i // num_chunks, lax.rem(i, num_chunks)
        for which in (0, 1):
            pair_copy(order, j, which).start()
        return 0
    lax.fori_loop(0, chips * num_chunks, pair_start, 0)

    def grad_loads(order, j, which, base):
        return (pltpu.make_async_copy(grad_ref.at[rows_of(dest_chip(order) * CORES + core), columns(which, j)], tile(base), in_sem.at[base]),
                pltpu.make_async_copy(pair_ref.at[order, :, columns(which, j)], tile(base + 1), in_sem.at[base + 1]))

    def arrived_load(phase, side, j, base):
        return pltpu.make_async_copy(arrived_ref.at[phase, side, j], tile(base), in_sem.at[base])

    def rs_copy(q, side):
        phase, j = q // num_chunks, lax.rem(q, num_chunks)
        slot = lax.rem(q, DEPTH)
        return remote(staged(side, slot), arrived_ref.at[phase, side, j],
                      rs_send.at[side, slot], rs_recv.at[phase, side, j], side_chip[side] * CORES + core)

    def up_copy(side, h, j, sender=None):
        return remote(own(h * num_chunks + j), x_ref.at[j, rows_of(me), :],
                      up_send.at[side, h, j], up_recv.at[side, core if sender is None else sender, j], side_chip[side] * CORES + h)

    def mate_copy(j):
        return remote(own((1 - core) * num_chunks + j), x_ref.at[j, rows_of(me), :], mate_send.at[j], mate_recv.at[j], partner)

    square_acc[...] = jnp.zeros_like(square_acc)

    def send_sums(q):
        phase, j = q // num_chunks, lax.rem(q, num_chunks)
        slot = lax.rem(q, DEPTH)
        for side in (0, 1):
            order = jnp.where(phase == 0, 0, 1 + side)
            which = jnp.where(phase == 1, 1 - side, side)
            pair_copy(order, j, which).wait_recv()
            for load in grad_loads(order, j, which, 3 * side):
                load.start()

            @pl.when(phase == 2)
            def _():
                rs_copy(j, side).wait_recv()
                arrived_load(0, side, j, 3 * side + 2).start()

        for side in (0, 1):
            order = jnp.where(phase == 0, 0, 1 + side)
            which = jnp.where(phase == 1, 1 - side, side)

            @pl.when(q >= DEPTH)
            def _():
                rs_copy(q - DEPTH, side).wait_send()
            for load in grad_loads(order, j, which, 3 * side):
                load.wait()

            @pl.when(phase == 2)
            def _():
                arrived_load(0, side, j, 3 * side + 2).wait()
                staged(side, slot)[...] = (tile(3 * side)[...] + tile(3 * side + 1)[...]) + tile(3 * side + 2)[...]

            @pl.when(phase != 2)
            def _():
                staged(side, slot)[...] = tile(3 * side)[...] + tile(3 * side + 1)[...]
            rs_copy(q, side).start()

    def send_up(j):
        for side in (0, 1):
            for h in range(CORES):
                up_copy(side, h, j).start()
        mate_copy(j).start()

    def finish(j):
        for which in (0, 1):
            pair_copy(3, j, which).wait_recv()
            loads = list(grad_loads(3, j, which, 0))
            for side in (0, 1):
                phase = 2 if side == which else 1
                rs_copy(phase * num_chunks + j, side).wait_recv()
                loads.append(arrived_load(phase, side, j, 2 + side))
            loads.append(pltpu.make_async_copy(mom_ref.at[:, columns(which, j)], tile(4), in_sem.at[4]))
            for load in loads:
                load.start()
            for load in loads:
                load.wait()
            mean = (((tile(0)[...] + tile(1)[...]) + tile(2)[...]) + tile(3)[...]) / group
            momentum = MOMENTUM * tile(4)[...] + mean
            nmom_ref[which * num_chunks + j] = momentum
            update = (mean + MOMENTUM * momentum).astype(BF16)
            own(which * num_chunks + j)[...] = update
            as_float = update.astype(F32)
            square_acc[...] += jnp.sum((as_float * as_float).reshape(slab // 8, 8, CHUNK), axis=0)
        @pl.when(j < EAGER)
        def _():
            send_up(j)

    def reduce_step(q, _):
        @pl.when(q < 3 * num_chunks)
        def _():
            send_sums(q)

        @pl.when(q >= 2 * num_chunks + DEPTH)
        def _():
            finish(q - 2 * num_chunks - DEPTH)
        return 0
    lax.fori_loop(0, 3 * num_chunks + DEPTH, reduce_step, 0)
    for side in (0, 1):
        for last in range(DEPTH):
            rs_copy(3 * num_chunks - DEPTH + last, side).wait_send()

    total = jnp.sum(square_acc[...])
    sq_out[...] = jnp.full(sq_out.shape, total, F32)
    sq_in[me] = jnp.full(sq_out.shape, total, F32)

    def sq_copy(other):
        return remote(sq_out, sq_in.at[me], sq_send.at[other], sq_recv.at[other], lax.rem(me + other, group))
    for other in range(1, group):
        sq_copy(other).start()

    def send_rest(j, _):
        send_up(j)
        return 0
    lax.fori_loop(EAGER, num_chunks, send_rest, 0)
    for other in range(1, group):
        sq_copy(other).wait()
    square = sq_in[0, 0:1, 0:1]
    for i in range(1, group):
        square = square + sq_in[i, 0:1, 0:1]
    inverse = 1.0 / (jnp.sqrt(square) + 1e-7)

    def normalise(j, row0, size):
        r = pl.ds(pl.multiple_of(row0, slab), size)
        x_ref[j, r, :] = (x_ref[j, r, :].astype(F32) * inverse).astype(BF16)

    def pass_copy(side, c):
        where = x_ref.at[c, rows_of(side_chip[1 - side] * CORES + side), :]
        return remote(where, where, pass_send.at[side, c], pass_recv.at[side, c], side_chip[side] * CORES + core)

    def w_first(side, h, c, sender=None):
        return remote(w_ref.at[:, columns(h, c)], wcol_ref.at[c, chip, span(core, slab), :],
                      w_send.at[side, h, c], w_recv.at[side, core if sender is None else sender, c], side_chip[side] * CORES + h)

    def w_forward(side, c):
        where = wcol_ref.at[c, side_chip[1 - side], pl.ds(side * slab, slab), :]
        return remote(where, where, w_fwd_send.at[side, c], w_fwd_recv.at[side, c], side_chip[side] * CORES + core)

    def w_pair(c):
        return remote(w_ref.at[:, columns(1 - core, c)], wcol_ref.at[c, chip, span(core, slab), :], w_mate_send.at[c], w_mate_recv.at[c], partner)

    def w_own(c):
        return pltpu.make_async_copy(w_ref.at[:, columns(core, c)], wcol_ref.at[c, chip, span(core, slab), :], w_own_sem.at[c])

    def w_pass(c):
        for side in (0, 1):
            w_first(side, 0, c, side).wait_recv()
            w_forward(side, c).start()

    def w_ready(c):
        for side in (0, 1):
            w_first(side, 0, c, 1 - side).wait_recv()
            w_forward(side, c).wait_recv()
        w_pair(c).wait_recv()
        w_own(c).wait()

    def slot_of(c, t):
        return lax.rem(c + 2 * slots - t, slots)

    def gram_copy(b, index, row, col):
        where = gram.at[span(row, BLOCK), span(col, BLOCK)]
        return remote(where, where, gram_send.at[index, b], gram_recv.at[index, b], partner)

    def poly_copy(b, index, row, col):
        where = poly.at[span(row, BLOCK), span(col, BLOCK)]
        return remote(where, where, poly_send.at[index, b], poly_recv.at[index, b], partner)

    def both(copy, owner, index, act, table=BLOCKS):
        row, col = block_of(owner, index, table)
        if not diagonal(index):
            act(copy(1, index, col, row))
        act(copy(0, index, row, col))

    def start(copy):
        copy.start()

    def arrived(copy):
        copy.wait_recv()

    def left(copy):
        copy.wait_send()

    def part_copy(index):
        return remote(parts.at[index], parts.at[5 + index], part_send.at[index], part_recv.at[index], partner)

    small = BLOCK // 2
    ROWS_ROWS = (((1,), (1,)), ((), ()))

    def product(rows_at, index, row, col):
        def rows_rows(left, right):
            terms = [lax.dot_general(a, b, ROWS_ROWS, preferred_element_type=F32) for a, b in zip(rows_at(*left), rows_at(*right))]
            return sum(terms[1:], terms[0])
        if diagonal(index):
            return rows_rows((row, 0, BLOCK), (row, 0, small)), rows_rows((row, small, small), (row, small, small))
        return (rows_rows((row, 0, BLOCK), (col, 0, BLOCK)),)

    def pieces_of(ref, value):
        if len(value) == 2:
            return (ref[:, 0:small], ref[small:, small:])
        return (ref[...],)

    def put_block(ref, row, col, value):
        if len(value) == 2:
            at = ref.at[span(row, BLOCK), span(row, BLOCK)]
            left, corner = (v.astype(BF16) for v in value)
            at[:, 0:small] = left
            at[small:, small:] = corner
            at[0:small, small:] = left[small:].T
        else:
            block = value[0].astype(BF16)
            ref[span(row, BLOCK), span(col, BLOCK)] = block
            ref[span(col, BLOCK), span(row, BLOCK)] = block.T

    def x_rows(t):
        def rows_at(block, offset, size):
            r = pl.ds(pl.multiple_of(block * BLOCK + offset, small), size)
            return (x_ref[slot_of(c, t), r, :] for c in range(num_chunks))
        return rows_at

    def gram_rows(block, offset, size):
        return (gram[pl.ds(pl.multiple_of(block * BLOCK + offset, small), size), :],)

    def near_chip(order):
        return (chip, side_chip[0], side_chip[1])[order]

    def near_block(one, two):
        one, two = near_chip(one), near_chip(two)
        return jnp.maximum(one, two), jnp.minimum(one, two)

    def near_owned(owner, place):
        rows_cols = [(near_block(*NEAR[c][place])) for c in range(CORES)]
        return tuple(jnp.where(owner == 0, rows_cols[0][i], rows_cols[1][i]) for i in range(2))

    def near_sum(j, place):
        row, col = near_owned(jnp.where(place < 3, 1 - core, core), place % 3)
        value = lax.dot_general(x_ref[j, span(row, BLOCK), :], x_ref[j, span(col, BLOCK), :], (((1,), (1,)), ((), ())), preferred_element_type=F32)
        slot = place % 3 + 8 * (place // 3)

        @pl.when(j == 0)
        def _():
            parts[slot] = value

        @pl.when(j > 0)
        def _():
            parts[slot] = parts[slot] + value

    def near_copy(place, b):
        row, col = near_owned(core, place)
        if b == 1:
            row, col = col, row
        where = gram.at[span(row, BLOCK), span(col, BLOCK)]
        return remote(where, where, gram_send.at[place, b], gram_recv.at[place, b], partner)

    def near_both(place, act):
        act(near_copy(place, 0))
        row, col = near_owned(core, place)

        @pl.when(row != col)
        def _():
            act(near_copy(place, 1))

    def near_arrived(place):
        near_copy(place, 0).wait_recv()
        row, col = near_owned(1 - core, place)

        @pl.when(row != col)
        def _():
            near_copy(place, 1).wait_recv()

    def arrive(j, _):
        x_ref[j, rows_of(me), :] = (own(core * num_chunks + j)[...].astype(F32) * inverse).astype(BF16)
        mate_copy(j).wait_recv()
        normalise(j, partner * slab, slab)
        for side in (0, 1):
            for from_core in range(CORES):
                up_copy(side, core, j, from_core).wait_recv()
            normalise(j, side_chip[1 - side] * CORES * slab, CORES * slab)
        for place in range(6):
            near_sum(j, place)
        return 0

    def far_block(chip_index, core_index, side):
        right, behind = lax.rem(chip_index + 1, chips), lax.rem(chip_index + chips - 1, chips)
        if side == 1:
            one, two = jnp.where(core_index == 0, chip_index, behind), right
        else:
            one, two = jnp.where(core_index == 0, chip_index, behind), behind
        return jnp.maximum(one, two), jnp.minimum(one, two)

    def far_copy(side):
        row, col = far_block(chip, core, side)
        where = gram.at[span(row, BLOCK), span(col, BLOCK)]
        return remote(where, where, far_send.at[side], far_recv.at[side], side_chip[side] * CORES + core)

    def share_copy(side, owner, b):
        row, col = far_block(side_chip[1 - side], owner, side)
        if b == 1:
            row, col = col, row
        where = gram.at[span(row, BLOCK), span(col, BLOCK)]
        return remote(where, where, share_send.at[side, b], share_recv.at[side, b], partner)

    def share(side, owner, act):
        act(share_copy(side, owner, 0))
        row, col = far_block(side_chip[1 - side], owner, side)

        @pl.when(row != col)
        def _():
            act(share_copy(side, owner, 1))

    lax.fori_loop(0, num_chunks, arrive, 0)

    def sent(j, _):
        for side in (0, 1):
            for h in range(CORES):
                up_copy(side, h, j).wait_send()
        mate_copy(j).wait_send()
        return 0
    lax.fori_loop(0, num_chunks, sent, 0)

    for place in range(3):
        part_copy(place).start()

    for c in range(EARLY):
        for side in (0, 1):
            pass_copy(side, c).start()
    for place in range(3):
        part_copy(place).wait_recv()
        row, col = near_owned(core, place)
        block = (parts[8 + place] + parts[5 + place]).astype(BF16)
        gram[span(row, BLOCK), span(col, BLOCK)] = block
        if place < 2:
            far_copy(place).start()

        @pl.when(row != col)
        def _():
            gram[span(col, BLOCK), span(row, BLOCK)] = block.T
        near_both(place, start)
    for c in range(EARLY, num_chunks):
        for side in (0, 1):
            pass_copy(side, c).start()

    def w_start(c, _):
        for h in range(CORES):
            for side in (0, 1):
                w_first(side, h, c).start()
        w_pair(c).start()
        w_own(c).start()
        return 0
    lax.fori_loop(0, num_chunks, w_start, 0)
    for place in range(3):
        near_arrived(place)
    for side in (0, 1):
        far_copy(side).wait_recv()
        row, col = far_block(side_chip[1 - side], core, side)
        turned = gram[span(row, BLOCK), span(col, BLOCK)].T

        @pl.when(row != col)
        def _():
            gram[span(col, BLOCK), span(row, BLOCK)] = turned
        share(side, core, start)
    for side in (0, 1):
        share(side, 1 - core, arrived)
        far_copy(side).wait_send()
        share(side, core, left)
    for place in range(3):
        near_both(place, left)
        part_copy(place).wait_send()

    tall = 1024
    decay, step_size = 1.0 - LEARN_RATE * WEIGHT_DECAY, LEARN_RATE * scale

    def step(t, _):
        def pass_weights(low, high):
            @pl.when(t == NS_STEPS - 2)
            def _():
                def one(c, _):
                    w_pass(c)
                    return 0
                lax.fori_loop(low, high, one, 0)
        pass_weights(0, W_EARLY)

        def gram_other(*indices):
            for index in indices:
                row, col = block_of(1 - core, index)
                value = product(x_rows(t), index, row, col)
                if len(value) == 2:
                    parts[index, :, 0:small] = value[0]
                    parts[index, small:, small:] = value[1]
                else:
                    parts[index] = value[0]
            for index in indices:
                part_copy(index).start()

        def gram_own(*indices):
            for index in indices:
                part_copy(index).wait_recv()
            for index in indices:
                row, col = block_of(core, index)
                value = product(x_rows(t), index, row, col)
                put_block(gram, row, col, tuple(v + w for v, w in zip(value, pieces_of(parts.at[5 + index], value))))
            for index in indices:
                both(gram_copy, core, index, start)

        def gram_middle(index, _):
            gram_own(index)
            return 0
        later = jnp.minimum(t, 1)

        def alone(act, *indices):
            def once(_, carry):
                act(*indices)
                return carry
            lax.fori_loop(0, later, once, None)
        for group_of in OTHERS:
            alone(gram_other, *group_of)
        alone(gram_own, 0, 1)

        @pl.when(t > 0)
        def _():
            lax.fori_loop(2, 4, gram_middle, 0)
        alone(gram_own, 4)

        def squares(indices, needs):
            @pl.when(t > 0)
            def _():
                for index in needs:
                    both(gram_copy, 1 - core, index, arrived)
            for index in indices:
                row, col = block_of(core, index, SQUARES)
                value = product(gram_rows, index, row, col)
                old = pieces_of(gram.at[span(row, BLOCK), span(col, BLOCK)], value)
                put_block(poly, row, col, tuple(COEF_B * g.astype(F32) + COEF_C * v for g, v in zip(old, value)))
            for index in indices:
                both(poly_copy, core, index, start, SQUARES)
        def part_drain(i, carry):
            part_copy(i).wait_send()
            return carry
        pl.when(t > 0)(lambda: lax.fori_loop(0, 5, part_drain, None))

        squares((0,), (0, 1, 2))
        squares((1,), (3,))
        squares((2,), ())
        squares((3,), (4,))

        @pl.when((t == NS_STEPS - 1) & (t > 0))
        def _():
            for index in range(5):
                both(gram_copy, core, index, left)
        squares((4,), ())

        def tile_load(q):
            c, m = q // 2, lax.rem(q, 2)
            slot = lax.rem(q, 2)
            return pltpu.make_async_copy(wcol_ref.at[c, pl.ds(2 * m, 2)], parts.at[pl.ds(2 * slot, 2)], tile_sem.at[slot])

        @pl.when(t == NS_STEPS - 1)
        def _():
            w_ready(0)
            tile_load(0).start()
            tile_load(1).start()

        def poly_ready(indices):
            for index in indices:
                both(poly_copy, 1 - core, index, arrived, SQUARES)

        def far_ready(c):
            @pl.when(t == 0)
            def _():
                for side in (0, 1):
                    pass_copy(side, c).wait()

        def apply_rows(c, r):
            src = slot_of(c, t)
            total = jnp.dot(poly[r, :], x_ref[src], preferred_element_type=F32)
            x_ref[slot_of(c, t + 1), r, :] = (COEF_A * x_ref[src, r, :].astype(F32) + total).astype(BF16)
        far_ready(0)
        poly_ready((0, 1, 2))
        apply_rows(0, slice(0, BLOCK))
        pass_weights(W_EARLY, num_chunks)
        poly_ready((3, 4))
        apply_rows(0, slice(BLOCK, tall))
        apply_rows(0, slice(tall, rows))

        @pl.when(t < NS_STEPS - 1)
        def _():
            def apply_half(q, _):
                pl.when(lax.rem(q, 2) == 0)(lambda: far_ready(q // 2))
                apply_rows(q // 2, span(lax.rem(q, 2), tall))
                return 0
            lax.fori_loop(2, 2 * num_chunks, apply_half, 0)

        @pl.when(t == NS_STEPS - 1)
        def _():
            def out_copy(q, act):
                c, m = q // 2, lax.rem(q, 2)
                new = x_ref.at[slot_of(c, t + 1), span(m, tall), :]

                @pl.when(c < KEPT)
                def _():
                    act(remote(new, gram.at[span(m, tall), span(c, CHUNK)], out_send.at[q], out_recv.at[q], partner))

                @pl.when((c >= KEPT) & (c < num_chunks - 1))
                def _():
                    act(remote(new, wide_ref.at[c - KEPT, span(m, tall), :], out_send.at[q], out_recv.at[q], partner))

                @pl.when(c == num_chunks - 1)
                def _():
                    act(remote(new, rest_ref.at[span(m, tall), :], out_send.at[q], out_recv.at[q], partner))

            def kept_rows(which, c):
                place = which * num_chunks + c
                return parts.at[4 + place // 2, pl.ds(pl.multiple_of(lax.rem(place, 2) * slab, slab), slab), :]

            def row_copy(c):
                return remote(parts.at[11, span(lax.rem(c, 2), slab), :], kept_rows(core, c), row_send.at[c], row_recv.at[c], partner)

            def new_rows(c, tile_index, owner):
                old = parts[tile_index, span(owner, slab), :]
                ortho = x_ref[slot_of(c, t + 1), span(chip * CORES + owner, slab), :]
                return decay * old - step_size * ortho.astype(F32)

            def new_weight(q):
                c, m = q // 2, lax.rem(q, 2)
                slot = lax.rem(q, 2)
                tile_load(q).wait()

                @pl.when(m == chip // 2)
                def _():
                    kept_rows(core, c)[...] = new_rows(c, 2 * slot + lax.rem(chip, 2), core)

                    @pl.when(c >= 2)
                    def _():
                        row_copy(c - 2).wait_send()
                    parts[11, span(lax.rem(c, 2), slab), :] = new_rows(c, 2 * slot + lax.rem(chip, 2), 1 - core)
                    row_copy(c).start()
                old = parts[pl.ds(2 * slot, 2)].reshape(tall, CHUNK)
                dst = slot_of(c, t + 1)
                x_ref[dst, span(m, tall), :] = (decay * old - step_size * x_ref[dst, span(m, tall), :].astype(F32)).astype(BF16)
                out_copy(q, start)

            def next_tile(q):
                @pl.when(q + 2 < 2 * num_chunks)
                def _():
                    pl.when(lax.rem(q, 2) == 0)(lambda: w_ready(q // 2 + 1))
                    tile_load(q + 2).start()

            def last_step(q, _):
                if NS_STEPS == 1:
                    pl.when(lax.rem(q, 2) == 0)(lambda: far_ready(q // 2))
                apply_rows(q // 2, span(lax.rem(q, 2), tall))
                new_weight(q)
                next_tile(q)
                return 0

            def first_tiles(q, _):
                new_weight(q)
                next_tile(q)
                return 0
            lax.fori_loop(0, 2, first_tiles, 0)
            lax.fori_loop(2, 2 * num_chunks, last_step, 0)

            def out_end(q, _):
                out_copy(q, lambda copy: copy.wait())
                return 0
            lax.fori_loop(0, 2 * num_chunks, out_end, 0)
            for c in range(num_chunks):
                if c >= num_chunks - 2:
                    row_copy(c).wait_send()
                row_copy(c).wait_recv()

        for index in range(5):
            @pl.when((t > 0) & (t < NS_STEPS - 1))
            def _():
                both(gram_copy, core, index, left)
            both(poly_copy, core, index, left, SQUARES)
        return 0
    lax.fori_loop(0, NS_STEPS, step, 0)

    def w_end(c, _):
        for side in (0, 1):
            for h in range(CORES):
                w_first(side, h, c).wait_send()
            w_forward(side, c).wait_send()
        w_pair(c).wait_send()
        return 0
    lax.fori_loop(0, num_chunks, w_end, 0)

    def paired(i, _):
        order, j = i // num_chunks, lax.rem(i, num_chunks)
        for which in (0, 1):
            pair_copy(order, j, which).wait_send()
        return 0
    lax.fori_loop(0, chips * num_chunks, paired, 0)


def hand_over(half, x_ref, gram, parts, nmom_ref, wide_ref, rest_ref, wide_out, nmom_out, weight_out, rest, wide_sem, load_sem, nmom_sem, weight_sem):
    core = lax.rem(lax.axis_index('dp'), CORES)
    slab = nmom_ref.shape[1]
    num_chunks = half // CHUNK
    slots = num_chunks + 1

    def columns(which, c):
        return pl.ds(pl.multiple_of(which * half + c * CHUNK, CHUNK), CHUNK)
    load = pltpu.make_async_copy(rest_ref, rest, load_sem)
    load.start()
    stores = []
    for c in range(num_chunks):
        stores.append(pltpu.make_async_copy(x_ref.at[(c + 2 * slots - NS_STEPS) % slots], wide_out.at[:, columns(core, c)], wide_sem.at[0, c]))
        there = gram.at[:, span(c, CHUNK)] if c < KEPT else wide_ref.at[c - KEPT] if c < num_chunks - 1 else rest
        stores.append(pltpu.make_async_copy(there, wide_out.at[:, columns(1 - core, c)], wide_sem.at[1, c]))
    last = stores.pop()
    for place in range(CORES * num_chunks):
        where = (slice(None), pl.ds(place * CHUNK, CHUNK))
        stores.append(pltpu.make_async_copy(nmom_ref.at[place], nmom_out.at[where], nmom_sem.at[place]))
        stores.append(pltpu.make_async_copy(parts.at[4 + place // 2, pl.ds(place % 2 * slab, slab), :], weight_out.at[where], weight_sem.at[place]))
    for store in stores:
        store.start()
    load.wait()
    last.start()
    for store in stores + [last]:
        store.wait()


def solution(mesh):
    group = mesh.shape['dp']

    def local_step(grad_part, momentum, weight):
        slab, num_cols = weight.shape[1:]
        rows = slab * group
        half = num_cols // CORES
        scale = 0.2 * math.sqrt(max(rows, num_cols))
        num_chunks = half // CHUNK
        chips = group // CORES
        anywhere = pl.BlockSpec(memory_space=pl.ANY)
        dma = pltpu.SemaphoreType.DMA
        shape = jax.ShapeDtypeStruct

        def kernel(*refs):
            muon(group, rows, half, scale, *refs)
        kept = pl.BlockSpec(memory_space=pltpu.VMEM)
        outs = pl.pallas_call(
            kernel,
            name='muon',
            out_shape=(pltpu.VMEM((num_chunks + 1, rows, CHUNK), BF16), pltpu.VMEM((rows, rows), BF16), pltpu.VMEM((12, BLOCK, BLOCK), F32),
                       pltpu.VMEM((CORES * num_chunks, slab, CHUNK), F32), pltpu.VMEM((num_chunks - 1 - KEPT, rows, CHUNK), BF16), pltpu.HBM((rows, CHUNK), BF16),
                       shape((num_chunks, chips, CORES * slab, CHUNK), F32), shape((chips, slab, num_cols), F32),
                       shape((3, 2, num_chunks, slab, CHUNK), F32)),
            in_specs=[anywhere] * 3,
            out_specs=(kept,) * 5 + (anywhere,) * 4,
            scratch_shapes=[
                pltpu.VMEM((rows, rows), BF16),
                pltpu.VMEM((8, CHUNK), F32),
                pltpu.VMEM((8, 128), F32),
                pltpu.VMEM((group, 8, 128), F32),
                dma((chips * num_chunks * 2,)), dma((chips * num_chunks * 2,)), dma((2, DEPTH)), dma((3, 2, num_chunks)), dma((6,)),
                dma((group,)), dma((group,)), dma((2, 2, num_chunks)), dma((2, 2, num_chunks)), dma((num_chunks,)), dma((num_chunks,)),
                dma((2, num_chunks)), dma((2, num_chunks)), dma((2,)), dma((2,)), dma((2, 2)), dma((2, 2)),
                dma((5,)), dma((5,)), dma((5, 2)), dma((5, 2)), dma((5, 2)), dma((5, 2)),
                dma((2, 2, num_chunks)), dma((2, 2, num_chunks)), dma((2, num_chunks)), dma((2, num_chunks)),
                dma((num_chunks,)), dma((num_chunks,)), dma((num_chunks,)), dma((2,)),
                dma((2 * num_chunks,)), dma((2 * num_chunks,)), dma((num_chunks,)), dma((num_chunks,)),
            ],
            compiler_params=pltpu.CompilerParams(collective_id=1, has_side_effects=True, vmem_limit_bytes=VMEM_ROOM),
        )(grad_part[0, 0], momentum[0], weight[0])

        def last_kernel(*refs):
            hand_over(half, *refs)
        weight_bf16, new_momentum, new_weight = pl.pallas_call(
            last_kernel,
            name='hand_over',
            out_shape=(shape((rows, num_cols), BF16), shape((slab, num_cols), F32), shape((slab, num_cols), F32)),
            in_specs=[kept] * 5 + [pl.BlockSpec(memory_space=pltpu.HBM)],
            out_specs=(anywhere,) * 3,
            scratch_shapes=[
                pltpu.VMEM((rows, CHUNK), BF16),
                dma((CORES, num_chunks)), dma(()), dma((CORES * num_chunks,)), dma((CORES * num_chunks,)),
            ],
            compiler_params=pltpu.CompilerParams(vmem_limit_bytes=VMEM_ROOM),
        )(*(pltpu.with_memory_space_constraint(out, pltpu.VMEM) for out in outs[:5]), pltpu.with_memory_space_constraint(outs[5], pltpu.HBM))
        return new_momentum[None], new_weight[None], weight_bf16[None]

    return jax.shard_map(local_step, mesh=mesh, in_specs=(P(('mp', 'dp')), P('mp', 'dp'), P('mp', 'dp')), out_specs=(P('mp', 'dp'), P('mp', 'dp'), P('mp')), check_vma=False)
```

```python
import math
import jax
import jax.numpy as jnp
from jax import lax
from jax.experimental import pallas as pl
from jax.experimental.pallas import tpu as pltpu
from jax.sharding import PartitionSpec as P

MOMENTUM = 0.95
LEARN_RATE = 2.0
WEIGHT_DECAY = 0.25
NS_STEPS = 5
COEF_A = 3.4445
COEF_B = -4.7750
COEF_C = 2.0315

MESH = pl.DeviceIdType.MESH
F32, BF16 = jnp.float32, jnp.bfloat16
CORES = 2
BLOCK = 512
CHUNK = 512
DEPTH = 4
KEPT = 4
VMEM_ROOM = 17305 * 2 ** 10
EAGER = 4
EARLY = 1
W_EARLY = 5
OTHERS = ((0, 1), (2, 3, 4))
BLOCKS = (((0, 0), (2, 1), (3, 1), (2, 0), (3, 3)), ((1, 1), (1, 0), (3, 0), (3, 2), (2, 2)))
SQUARES = (((0, 0), (3, 0), (3, 1), (3, 2), (3, 3)), ((1, 1), (1, 0), (2, 0), (2, 1), (2, 2)))
NEAR = (((0, 2), (0, 1), (0, 0)), ((2, 2), (1, 2), (1, 1)))


def block_of(core, index, table=BLOCKS):
    def pick(owner, i):
        values = [block[i] for block in table[owner]]
        if isinstance(index, int):
            return values[index]
        result = jnp.int32(values[0])
        for place, value in enumerate(values[1:], 1):
            result = jnp.where(index == place, jnp.int32(value), result)
        return result
    return tuple(jnp.where(core == 0, pick(0, i), pick(1, i)) for i in range(2))


def diagonal(index):
    return isinstance(index, int) and index in (0, 4)


def span(index, size):
    return pl.ds(pl.multiple_of(index * size, size), size)


def muon(group, rows, half, scale, grad_ref, mom_ref, w_ref, x_ref, gram, parts, nmom_ref, wide_ref, rest_ref, wcol_ref, pair_ref, arrived_ref,
         poly, square_acc, sq_out, sq_in,
         pair_send, pair_recv, rs_send, rs_recv, in_sem, sq_send, sq_recv, up_send, up_recv, mate_send, mate_recv, pass_send, pass_recv,
         far_send, far_recv, share_send, share_recv, part_send, part_recv, gram_send, gram_recv, poly_send, poly_recv,
         w_send, w_recv, w_fwd_send, w_fwd_recv, w_mate_send, w_mate_recv, w_own_sem, tile_sem, out_send, out_recv, row_send, row_recv):
    me = lax.axis_index('dp')
    core, chip = lax.rem(me, CORES), me // CORES
    chips = group // CORES
    slab = rows // group
    partner = chip * CORES + (1 - core)
    side_chip = (lax.rem(chip + 1, chips), lax.rem(chip + chips - 1, chips))
    far_chip = lax.rem(chip + 2, chips)
    num_chunks = half // CHUNK
    slots = num_chunks + 1

    def remote(src, dst, send, recv, device):
        return pltpu.make_async_remote_copy(src, dst, send, recv, device_id={'dp': device}, device_id_type=MESH)

    barrier = pltpu.get_barrier_semaphore()
    for other in range(1, group):
        pl.semaphore_signal(barrier, inc=1, device_id={'dp': lax.rem(me + other, group)}, device_id_type=MESH)
    pl.semaphore_wait(barrier, group - 1)

    def tile(index):
        return parts.at[index // 2, pl.ds(pl.multiple_of(lax.rem(index, 2) * slab, slab), slab), :]

    def staged(side, slot):
        return tile(6 + side * DEPTH + slot)

    def own(index):
        return poly.at[span(index // 4, slab), span(lax.rem(index, 4), CHUNK)]

    def dest_chip(order):
        return jnp.where(order == 0, far_chip, jnp.where(order == 1, side_chip[0], jnp.where(order == 2, side_chip[1], chip)))

    def rows_of(device):
        return span(device, slab)

    def columns(which, j):
        return pl.ds(pl.multiple_of(which * half + j * CHUNK, CHUNK), CHUNK)

    def pair_copy(order, j, which):
        i = (order * num_chunks + j) * 2 + which
        return remote(grad_ref.at[rows_of(dest_chip(order) * CORES + 1 - core), columns(which, j)], pair_ref.at[order, :, columns(which, j)],
                      pair_send.at[i], pair_recv.at[i], partner)

    def pair_start(i, _):
        order, j = i // num_chunks, lax.rem(i, num_chunks)
        for which in (0, 1):
            pair_copy(order, j, which).start()
        return 0
    lax.fori_loop(0, chips * num_chunks, pair_start, 0)

    def grad_loads(order, j, which, base):
        return (pltpu.make_async_copy(grad_ref.at[rows_of(dest_chip(order) * CORES + core), columns(which, j)], tile(base), in_sem.at[base]),
                pltpu.make_async_copy(pair_ref.at[order, :, columns(which, j)], tile(base + 1), in_sem.at[base + 1]))

    def arrived_load(phase, side, j, base):
        return pltpu.make_async_copy(arrived_ref.at[phase, side, j], tile(base), in_sem.at[base])

    def rs_copy(q, side):
        phase, j = q // num_chunks, lax.rem(q, num_chunks)
        slot = lax.rem(q, DEPTH)
        return remote(staged(side, slot), arrived_ref.at[phase, side, j],
                      rs_send.at[side, slot], rs_recv.at[phase, side, j], side_chip[side] * CORES + core)

    def up_copy(side, h, j, sender=None):
        return remote(own(h * num_chunks + j), x_ref.at[j, rows_of(me), :],
                      up_send.at[side, h, j], up_recv.at[side, core if sender is None else sender, j], side_chip[side] * CORES + h)

    def mate_copy(j):
        return remote(own((1 - core) * num_chunks + j), x_ref.at[j, rows_of(me), :], mate_send.at[j], mate_recv.at[j], partner)

    square_acc[...] = jnp.zeros_like(square_acc)

    def send_sums(q):
        phase, j = q // num_chunks, lax.rem(q, num_chunks)
        slot = lax.rem(q, DEPTH)
        for side in (0, 1):
            order = jnp.where(phase == 0, 0, 1 + side)
            which = jnp.where(phase == 1, 1 - side, side)
            pair_copy(order, j, which).wait_recv()
            for load in grad_loads(order, j, which, 3 * side):
                load.start()

            @pl.when(phase == 2)
            def _():
                rs_copy(j, side).wait_recv()
                arrived_load(0, side, j, 3 * side + 2).start()

        for side in (0, 1):
            order = jnp.where(phase == 0, 0, 1 + side)
            which = jnp.where(phase == 1, 1 - side, side)

            @pl.when(q >= DEPTH)
            def _():
                rs_copy(q - DEPTH, side).wait_send()
            for load in grad_loads(order, j, which, 3 * side):
                load.wait()

            @pl.when(phase == 2)
            def _():
                arrived_load(0, side, j, 3 * side + 2).wait()
                staged(side, slot)[...] = (tile(3 * side)[...] + tile(3 * side + 1)[...]) + tile(3 * side + 2)[...]

            @pl.when(phase != 2)
            def _():
                staged(side, slot)[...] = tile(3 * side)[...] + tile(3 * side + 1)[...]
            rs_copy(q, side).start()

    def send_up(j):
        for side in (0, 1):
            for h in range(CORES):
                up_copy(side, h, j).start()
        mate_copy(j).start()

    def finish(j):
        for which in (0, 1):
            pair_copy(3, j, which).wait_recv()
            loads = list(grad_loads(3, j, which, 0))
            for side in (0, 1):
                phase = 2 if side == which else 1
                rs_copy(phase * num_chunks + j, side).wait_recv()
                loads.append(arrived_load(phase, side, j, 2 + side))
            loads.append(pltpu.make_async_copy(mom_ref.at[:, columns(which, j)], tile(4), in_sem.at[4]))
            for load in loads:
                load.start()
            for load in loads:
                load.wait()
            mean = (((tile(0)[...] + tile(1)[...]) + tile(2)[...]) + tile(3)[...]) / group
            momentum = MOMENTUM * tile(4)[...] + mean
            nmom_ref[which * num_chunks + j] = momentum
            update = (mean + MOMENTUM * momentum).astype(BF16)
            own(which * num_chunks + j)[...] = update
            as_float = update.astype(F32)
            square_acc[...] += jnp.sum((as_float * as_float).reshape(slab // 8, 8, CHUNK), axis=0)
        @pl.when(j < EAGER)
        def _():
            send_up(j)

    def reduce_step(q, _):
        @pl.when(q < 3 * num_chunks)
        def _():
            send_sums(q)

        @pl.when(q >= 2 * num_chunks + DEPTH)
        def _():
            finish(q - 2 * num_chunks - DEPTH)
        return 0
    lax.fori_loop(0, 3 * num_chunks + DEPTH, reduce_step, 0)
    for side in (0, 1):
        for last in range(DEPTH):
            rs_copy(3 * num_chunks - DEPTH + last, side).wait_send()

    total = jnp.sum(square_acc[...])
    sq_out[...] = jnp.full(sq_out.shape, total, F32)
    sq_in[me] = jnp.full(sq_out.shape, total, F32)

    def sq_copy(other):
        return remote(sq_out, sq_in.at[me], sq_send.at[other], sq_recv.at[other], lax.rem(me + other, group))
    for other in range(1, group):
        sq_copy(other).start()

    def send_rest(j, _):
        send_up(j)
        return 0
    lax.fori_loop(EAGER, num_chunks, send_rest, 0)
    for other in range(1, group):
        sq_copy(other).wait()
    square = sq_in[0, 0:1, 0:1]
    for i in range(1, group):
        square = square + sq_in[i, 0:1, 0:1]
    inverse = 1.0 / (jnp.sqrt(square) + 1e-7)

    def normalise(j, row0, size):
        r = pl.ds(pl.multiple_of(row0, slab), size)
        x_ref[j, r, :] = (x_ref[j, r, :].astype(F32) * inverse).astype(BF16)

    def pass_copy(side, c):
        where = x_ref.at[c, rows_of(side_chip[1 - side] * CORES + side), :]
        return remote(where, where, pass_send.at[side, c], pass_recv.at[side, c], side_chip[side] * CORES + core)

    def w_first(side, h, c, sender=None):
        return remote(w_ref.at[:, columns(h, c)], wcol_ref.at[c, chip, span(core, slab), :],
                      w_send.at[side, h, c], w_recv.at[side, core if sender is None else sender, c], side_chip[side] * CORES + h)

    def w_forward(side, c):
        where = wcol_ref.at[c, side_chip[1 - side], pl.ds(side * slab, slab), :]
        return remote(where, where, w_fwd_send.at[side, c], w_fwd_recv.at[side, c], side_chip[side] * CORES + core)

    def w_pair(c):
        return remote(w_ref.at[:, columns(1 - core, c)], wcol_ref.at[c, chip, span(core, slab), :], w_mate_send.at[c], w_mate_recv.at[c], partner)

    def w_own(c):
        return pltpu.make_async_copy(w_ref.at[:, columns(core, c)], wcol_ref.at[c, chip, span(core, slab), :], w_own_sem.at[c])

    def w_pass(c):
        for side in (0, 1):
            w_first(side, 0, c, side).wait_recv()
            w_forward(side, c).start()

    def w_ready(c):
        for side in (0, 1):
            w_first(side, 0, c, 1 - side).wait_recv()
            w_forward(side, c).wait_recv()
        w_pair(c).wait_recv()
        w_own(c).wait()

    def slot_of(c, t):
        return lax.rem(c + 2 * slots - t, slots)

    def gram_copy(b, index, row, col):
        where = gram.at[span(row, BLOCK), span(col, BLOCK)]
        return remote(where, where, gram_send.at[index, b], gram_recv.at[index, b], partner)

    def poly_copy(b, index, row, col):
        where = poly.at[span(row, BLOCK), span(col, BLOCK)]
        return remote(where, where, poly_send.at[index, b], poly_recv.at[index, b], partner)

    def both(copy, owner, index, act, table=BLOCKS):
        row, col = block_of(owner, index, table)
        if not diagonal(index):
            act(copy(1, index, col, row))
        act(copy(0, index, row, col))

    def start(copy):
        copy.start()

    def arrived(copy):
        copy.wait_recv()

    def left(copy):
        copy.wait_send()

    def part_copy(index):
        return remote(parts.at[index], parts.at[5 + index], part_send.at[index], part_recv.at[index], partner)

    small = BLOCK // 2
    ROWS_ROWS = (((1,), (1,)), ((), ()))

    def product(rows_at, index, row, col):
        def rows_rows(left, right):
            terms = [lax.dot_general(a, b, ROWS_ROWS, preferred_element_type=F32) for a, b in zip(rows_at(*left), rows_at(*right))]
            return sum(terms[1:], terms[0])
        if diagonal(index):
            low = rows_rows((row, small, small), (row, 0, BLOCK))
            top = rows_rows((row, 0, small), (row, 0, small))
            return jnp.concatenate([top, low[:, :small]], axis=0), low[:, small:]
        return (rows_rows((row, 0, BLOCK), (col, 0, BLOCK)),)

    def pieces_of(ref, value):
        if len(value) == 2:
            return (ref[:, 0:small], ref[small:, small:])
        return (ref[...],)

    def turn_poly(index):
        row, col = block_of(1 - core, index, SQUARES)
        poly[span(col, BLOCK), span(row, BLOCK)] = poly[span(row, BLOCK), span(col, BLOCK)].T

    def put_block(ref, row, col, value):
        if len(value) == 2:
            at = ref.at[span(row, BLOCK), span(row, BLOCK)]
            left, corner = (v.astype(BF16) for v in value)
            at[:, 0:small] = left
            at[small:, small:] = corner
            at[0:small, small:] = left[small:].T
        else:
            block = value[0].astype(BF16)
            ref[span(row, BLOCK), span(col, BLOCK)] = block
            ref[span(col, BLOCK), span(row, BLOCK)] = block.T

    def x_rows(t):
        def rows_at(block, offset, size):
            r = pl.ds(pl.multiple_of(block * BLOCK + offset, small), size)
            return (x_ref[slot_of(c, t), r, :] for c in range(num_chunks))
        return rows_at

    def gram_rows(block, offset, size):
        return (gram[pl.ds(pl.multiple_of(block * BLOCK + offset, small), size), :],)

    def near_chip(order):
        return (chip, side_chip[0], side_chip[1])[order]

    def near_block(one, two):
        one, two = near_chip(one), near_chip(two)
        return jnp.maximum(one, two), jnp.minimum(one, two)

    def near_owned(owner, place):
        rows_cols = [(near_block(*NEAR[c][place])) for c in range(CORES)]
        return tuple(jnp.where(owner == 0, rows_cols[0][i], rows_cols[1][i]) for i in range(2))

    def near_sum(j, place):
        row, col = near_owned(jnp.where(place < 3, 1 - core, core), place % 3)
        value = lax.dot_general(x_ref[j, span(row, BLOCK), :], x_ref[j, span(col, BLOCK), :], (((1,), (1,)), ((), ())), preferred_element_type=F32)
        slot = place % 3 + 8 * (place // 3)

        if isinstance(j, int):
            parts[slot] = parts[slot] + value
            return

        @pl.when(j == 0)
        def _():
            parts[slot] = value

        @pl.when(j > 0)
        def _():
            parts[slot] = parts[slot] + value

    def near_copy(place, b):
        row, col = near_owned(core, place)
        if b == 1:
            row, col = col, row
        where = gram.at[span(row, BLOCK), span(col, BLOCK)]
        return remote(where, where, gram_send.at[place, b], gram_recv.at[place, b], partner)

    def near_both(place, act):
        act(near_copy(place, 0))
        row, col = near_owned(core, place)

        @pl.when(row != col)
        def _():
            act(near_copy(place, 1))

    def near_arrived(place):
        near_copy(place, 0).wait_recv()
        row, col = near_owned(1 - core, place)

        @pl.when(row != col)
        def _():
            near_copy(place, 1).wait_recv()

    def land(j):
        x_ref[j, rows_of(me), :] = (own(core * num_chunks + j)[...].astype(F32) * inverse).astype(BF16)
        mate_copy(j).wait_recv()
        normalise(j, partner * slab, slab)
        for side in (0, 1):
            for from_core in range(CORES):
                up_copy(side, core, j, from_core).wait_recv()
            normalise(j, side_chip[1 - side] * CORES * slab, CORES * slab)

    def arrive(j, _):
        land(j)
        for place in range(6):
            near_sum(j, place)
        return 0

    def far_block(chip_index, core_index, side):
        right, behind = lax.rem(chip_index + 1, chips), lax.rem(chip_index + chips - 1, chips)
        if side == 1:
            one, two = jnp.where(core_index == 0, chip_index, behind), right
        else:
            one, two = jnp.where(core_index == 0, chip_index, behind), behind
        return jnp.maximum(one, two), jnp.minimum(one, two)

    def far_copy(side):
        row, col = far_block(chip, core, side)
        where = gram.at[span(row, BLOCK), span(col, BLOCK)]
        return remote(where, where, far_send.at[side], far_recv.at[side], side_chip[side] * CORES + core)

    def share_copy(side, owner):
        row, col = far_block(side_chip[1 - side], owner, side)
        where = gram.at[span(row, BLOCK), span(col, BLOCK)]
        return remote(where, where, share_send.at[side], share_recv.at[side], partner)

    def turn(side, owner):
        row, col = far_block(side_chip[1 - side], owner, side)

        @pl.when(row != col)
        def _():
            gram[span(col, BLOCK), span(row, BLOCK)] = gram[span(row, BLOCK), span(col, BLOCK)].T

    lax.fori_loop(0, num_chunks - 1, arrive, 0)
    land(num_chunks - 1)
    for place in range(3):
        near_sum(num_chunks - 1, place)
        part_copy(place).start()
    for place in range(3, 6):
        near_sum(num_chunks - 1, place)

    def sent(j, _):
        for side in (0, 1):
            for h in range(CORES):
                up_copy(side, h, j).wait_send()
        mate_copy(j).wait_send()
        return 0
    lax.fori_loop(0, num_chunks, sent, 0)


    for c in range(EARLY):
        for side in (0, 1):
            pass_copy(side, c).start()
    for place in range(3):
        part_copy(place).wait_recv()
        row, col = near_owned(core, place)
        block = (parts[8 + place] + parts[5 + place]).astype(BF16)
        gram[span(row, BLOCK), span(col, BLOCK)] = block
        if place < 2:
            far_copy(place).start()

        @pl.when(row != col)
        def _():
            gram[span(col, BLOCK), span(row, BLOCK)] = block.T
        near_both(place, start)
    for c in range(EARLY, num_chunks):
        for side in (0, 1):
            pass_copy(side, c).start()

    def w_start(c, _):
        for h in range(CORES):
            for side in (0, 1):
                w_first(side, h, c).start()
        w_pair(c).start()
        w_own(c).start()
        return 0
    lax.fori_loop(0, num_chunks, w_start, 0)
    for place in range(3):
        near_arrived(place)
    for side in (0, 1):
        far_copy(side).wait_recv()
        share_copy(side, core).start()
    for side in (0, 1):
        turn(side, core)
    for side in (0, 1):
        share_copy(side, 1 - core).wait_recv()
        turn(side, 1 - core)
    for side in (0, 1):
        far_copy(side).wait_send()
        share_copy(side, core).wait_send()
    for place in range(3):
        near_both(place, left)
        part_copy(place).wait_send()

    tall = 1024
    decay, step_size = 1.0 - LEARN_RATE * WEIGHT_DECAY, LEARN_RATE * scale

    def step(t, _):
        def pass_weights(low, high):
            @pl.when(t == NS_STEPS - 2)
            def _():
                def one(c, _):
                    w_pass(c)
                    return 0
                lax.fori_loop(low, high, one, 0)
        pass_weights(0, W_EARLY)

        def gram_other(*indices):
            for index in indices:
                row, col = block_of(1 - core, index)
                value = product(x_rows(t), index, row, col)
                if len(value) == 2:
                    parts[index, :, 0:small] = value[0]
                    parts[index, small:, small:] = value[1]
                else:
                    parts[index] = value[0]
            for index in indices:
                part_copy(index).start()

        def gram_own(*indices):
            for index in indices:
                part_copy(index).wait_recv()
            for index in indices:
                row, col = block_of(core, index)
                value = product(x_rows(t), index, row, col)
                put_block(gram, row, col, tuple(v + w for v, w in zip(value, pieces_of(parts.at[5 + index], value))))
            for index in indices:
                both(gram_copy, core, index, start)

        def gram_middle(index, _):
            gram_own(index)
            return 0
        later = jnp.minimum(t, 1)

        def alone(act, *indices):
            def once(_, carry):
                act(*indices)
                return carry
            lax.fori_loop(0, later, once, None)
        for group_of in OTHERS:
            alone(gram_other, *group_of)
        alone(gram_own, 0, 1)

        @pl.when(t > 0)
        def _():
            lax.fori_loop(2, 4, gram_middle, 0)
        alone(gram_own, 4)

        def once(owner, index, act):
            row, col = block_of(owner, index, SQUARES)
            act(poly_copy(0, index, row, col))

        def squares(indices, needs):
            @pl.when(t > 0)
            def _():
                for index in needs:
                    both(gram_copy, 1 - core, index, arrived)
            if 4 in indices:
                once(1 - core, 1, arrived)
            for index in indices:
                row, col = block_of(core, index, SQUARES)
                value = product(gram_rows, index, row, col)
                old = pieces_of(gram.at[span(row, BLOCK), span(col, BLOCK)], value)
                put_block(poly, row, col, tuple(COEF_B * g.astype(F32) + COEF_C * v for g, v in zip(old, value)))
                if index == 4:
                    turn_poly(1)
            for index in indices:
                once(core, index, start)
        def part_drain(i, carry):
            part_copy(i).wait_send()
            return carry
        pl.when(t > 0)(lambda: lax.fori_loop(0, 5, part_drain, None))

        squares((0,), (0, 1, 2))
        squares((1,), (3,))
        squares((2,), ())
        squares((3,), (4,))

        @pl.when((t == NS_STEPS - 1) & (t > 0))
        def _():
            for index in range(5):
                both(gram_copy, core, index, left)
        squares((4,), ())

        def tile_load(q):
            c, m = q // 2, lax.rem(q, 2)
            slot = lax.rem(q, 2)
            return pltpu.make_async_copy(wcol_ref.at[c, pl.ds(2 * m, 2)], parts.at[pl.ds(2 * slot, 2)], tile_sem.at[slot])

        @pl.when(t == NS_STEPS - 1)
        def _():
            w_ready(0)
            tile_load(0).start()
            tile_load(1).start()

        def far_ready(c):
            @pl.when(t == 0)
            def _():
                for side in (0, 1):
                    pass_copy(side, c).wait()

        def apply_rows(c, r):
            src = slot_of(c, t)
            total = jnp.dot(poly[r, :], x_ref[src], preferred_element_type=F32)
            x_ref[slot_of(c, t + 1), r, :] = (COEF_A * x_ref[src, r, :].astype(F32) + total).astype(BF16)
        far_ready(0)
        once(1 - core, 0, arrived)
        once(1 - core, 2, arrived)
        turn_poly(2)
        once(1 - core, 3, arrived)
        turn_poly(3)
        apply_rows(0, slice(0, BLOCK))
        pass_weights(W_EARLY, num_chunks)
        once(1 - core, 4, arrived)
        apply_rows(0, slice(BLOCK, tall))
        apply_rows(0, slice(tall, rows))

        @pl.when(t < NS_STEPS - 1)
        def _():
            def apply_chunk(c, _):
                far_ready(c)
                for half_rows in range(2):
                    apply_rows(c, slice(half_rows * tall, (half_rows + 1) * tall))
                return 0
            lax.fori_loop(1, num_chunks, apply_chunk, 0)

        @pl.when(t == NS_STEPS - 1)
        def _():
            def out_copy(q, act):
                c, m = q // 2, lax.rem(q, 2)
                new = x_ref.at[slot_of(c, t + 1), span(m, tall), :]

                @pl.when(c < KEPT)
                def _():
                    act(remote(new, gram.at[span(m, tall), span(c, CHUNK)], out_send.at[q], out_recv.at[q], partner))

                @pl.when((c >= KEPT) & (c < num_chunks - 1))
                def _():
                    act(remote(new, wide_ref.at[c - KEPT, span(m, tall), :], out_send.at[q], out_recv.at[q], partner))

                @pl.when(c == num_chunks - 1)
                def _():
                    act(remote(new, rest_ref.at[span(m, tall), :], out_send.at[q], out_recv.at[q], partner))

            def kept_rows(which, c):
                place = which * num_chunks + c
                return parts.at[4 + place // 2, pl.ds(pl.multiple_of(lax.rem(place, 2) * slab, slab), slab), :]

            def row_copy(c):
                return remote(parts.at[11, span(lax.rem(c, 2), slab), :], kept_rows(core, c), row_send.at[c], row_recv.at[c], partner)

            def new_rows(c, tile_index, owner):
                old = parts[tile_index, span(owner, slab), :]
                ortho = x_ref[slot_of(c, t + 1), span(chip * CORES + owner, slab), :]
                return decay * old - step_size * ortho.astype(F32)

            def new_weight(q):
                c, m = q // 2, lax.rem(q, 2)
                slot = lax.rem(q, 2)
                tile_load(q).wait()

                @pl.when(m == chip // 2)
                def _():
                    kept_rows(core, c)[...] = new_rows(c, 2 * slot + lax.rem(chip, 2), core)

                    @pl.when(c >= 2)
                    def _():
                        row_copy(c - 2).wait_send()
                    parts[11, span(lax.rem(c, 2), slab), :] = new_rows(c, 2 * slot + lax.rem(chip, 2), 1 - core)
                    row_copy(c).start()
                old = parts[pl.ds(2 * slot, 2)].reshape(tall, CHUNK)
                dst = slot_of(c, t + 1)
                x_ref[dst, span(m, tall), :] = (decay * old - step_size * x_ref[dst, span(m, tall), :].astype(F32)).astype(BF16)
                out_copy(q, start)

            def next_tile(q):
                @pl.when(q + 2 < 2 * num_chunks)
                def _():
                    pl.when(lax.rem(q, 2) == 0)(lambda: w_ready(q // 2 + 1))
                    tile_load(q + 2).start()

            def last_step(q, _):
                if NS_STEPS == 1:
                    pl.when(lax.rem(q, 2) == 0)(lambda: far_ready(q // 2))
                apply_rows(q // 2, span(lax.rem(q, 2), tall))
                new_weight(q)
                next_tile(q)
                return 0

            def first_tiles(q, _):
                new_weight(q)
                next_tile(q)
                return 0
            lax.fori_loop(0, 2, first_tiles, 0)
            lax.fori_loop(2, 2 * num_chunks, last_step, 0)

            def out_end(q, _):
                out_copy(q, lambda copy: copy.wait())
                return 0
            lax.fori_loop(0, 2 * num_chunks, out_end, 0)
            for c in range(num_chunks):
                if c >= num_chunks - 2:
                    row_copy(c).wait_send()
                row_copy(c).wait_recv()

        for index in range(5):
            @pl.when((t > 0) & (t < NS_STEPS - 1))
            def _():
                both(gram_copy, core, index, left)
            once(core, index, left)
        return 0
    lax.fori_loop(0, NS_STEPS, step, 0)

    def w_end(c, _):
        for side in (0, 1):
            for h in range(CORES):
                w_first(side, h, c).wait_send()
            w_forward(side, c).wait_send()
        w_pair(c).wait_send()
        return 0
    lax.fori_loop(0, num_chunks, w_end, 0)

    def paired(i, _):
        order, j = i // num_chunks, lax.rem(i, num_chunks)
        for which in (0, 1):
            pair_copy(order, j, which).wait_send()
        return 0
    lax.fori_loop(0, chips * num_chunks, paired, 0)


def hand_over(half, x_ref, gram, parts, nmom_ref, wide_ref, rest_ref, wide_out, nmom_out, weight_out, rest, wide_sem, load_sem, nmom_sem, weight_sem):
    core = lax.rem(lax.axis_index('dp'), CORES)
    slab = nmom_ref.shape[1]
    num_chunks = half // CHUNK
    slots = num_chunks + 1

    def columns(which, c):
        return pl.ds(pl.multiple_of(which * half + c * CHUNK, CHUNK), CHUNK)
    load = pltpu.make_async_copy(rest_ref, rest, load_sem)
    load.start()
    stores = []
    for c in range(num_chunks):
        stores.append(pltpu.make_async_copy(x_ref.at[(c + 2 * slots - NS_STEPS) % slots], wide_out.at[:, columns(core, c)], wide_sem.at[0, c]))
        there = gram.at[:, span(c, CHUNK)] if c < KEPT else wide_ref.at[c - KEPT] if c < num_chunks - 1 else rest
        stores.append(pltpu.make_async_copy(there, wide_out.at[:, columns(1 - core, c)], wide_sem.at[1, c]))
    last = stores.pop()
    for place in range(CORES * num_chunks):
        where = (slice(None), pl.ds(place * CHUNK, CHUNK))
        stores.append(pltpu.make_async_copy(nmom_ref.at[place], nmom_out.at[where], nmom_sem.at[place]))
        stores.append(pltpu.make_async_copy(parts.at[4 + place // 2, pl.ds(place % 2 * slab, slab), :], weight_out.at[where], weight_sem.at[place]))
    for store in stores:
        store.start()
    load.wait()
    last.start()
    for store in stores + [last]:
        store.wait()


def solution(mesh):
    group = mesh.shape['dp']

    def local_step(grad_part, momentum, weight):
        slab, num_cols = weight.shape[1:]
        rows = slab * group
        half = num_cols // CORES
        scale = 0.2 * math.sqrt(max(rows, num_cols))
        num_chunks = half // CHUNK
        chips = group // CORES
        anywhere = pl.BlockSpec(memory_space=pl.ANY)
        dma = pltpu.SemaphoreType.DMA
        shape = jax.ShapeDtypeStruct

        def kernel(*refs):
            muon(group, rows, half, scale, *refs)
        kept = pl.BlockSpec(memory_space=pltpu.VMEM)
        outs = pl.pallas_call(
            kernel,
            name='muon',
            out_shape=(pltpu.VMEM((num_chunks + 1, rows, CHUNK), BF16), pltpu.VMEM((rows, rows), BF16), pltpu.VMEM((12, BLOCK, BLOCK), F32),
                       pltpu.VMEM((CORES * num_chunks, slab, CHUNK), F32), pltpu.VMEM((num_chunks - 1 - KEPT, rows, CHUNK), BF16), pltpu.HBM((rows, CHUNK), BF16),
                       shape((num_chunks, chips, CORES * slab, CHUNK), F32), shape((chips, slab, num_cols), F32),
                       shape((3, 2, num_chunks, slab, CHUNK), F32)),
            in_specs=[anywhere] * 3,
            out_specs=(kept,) * 5 + (anywhere,) * 4,
            scratch_shapes=[
                pltpu.VMEM((rows, rows), BF16),
                pltpu.VMEM((8, CHUNK), F32),
                pltpu.VMEM((8, 128), F32),
                pltpu.VMEM((group, 8, 128), F32),
                dma((chips * num_chunks * 2,)), dma((chips * num_chunks * 2,)), dma((2, DEPTH)), dma((3, 2, num_chunks)), dma((6,)),
                dma((group,)), dma((group,)), dma((2, 2, num_chunks)), dma((2, 2, num_chunks)), dma((num_chunks,)), dma((num_chunks,)),
                dma((2, num_chunks)), dma((2, num_chunks)), dma((2,)), dma((2,)), dma((2,)), dma((2,)),
                dma((5,)), dma((5,)), dma((5, 2)), dma((5, 2)), dma((5, 2)), dma((5, 2)),
                dma((2, 2, num_chunks)), dma((2, 2, num_chunks)), dma((2, num_chunks)), dma((2, num_chunks)),
                dma((num_chunks,)), dma((num_chunks,)), dma((num_chunks,)), dma((2,)),
                dma((2 * num_chunks,)), dma((2 * num_chunks,)), dma((num_chunks,)), dma((num_chunks,)),
            ],
            compiler_params=pltpu.CompilerParams(collective_id=1, has_side_effects=True, vmem_limit_bytes=VMEM_ROOM),
        )(grad_part[0, 0], momentum[0], weight[0])

        def last_kernel(*refs):
            hand_over(half, *refs)
        weight_bf16, new_momentum, new_weight = pl.pallas_call(
            last_kernel,
            name='hand_over',
            out_shape=(shape((rows, num_cols), BF16), shape((slab, num_cols), F32), shape((slab, num_cols), F32)),
            in_specs=[kept] * 5 + [pl.BlockSpec(memory_space=pltpu.HBM)],
            out_specs=(anywhere,) * 3,
            scratch_shapes=[
                pltpu.VMEM((rows, CHUNK), BF16),
                dma((CORES, num_chunks)), dma(()), dma((CORES * num_chunks,)), dma((CORES * num_chunks,)),
            ],
            compiler_params=pltpu.CompilerParams(vmem_limit_bytes=VMEM_ROOM),
        )(*(pltpu.with_memory_space_constraint(out, pltpu.VMEM) for out in outs[:5]), pltpu.with_memory_space_constraint(outs[5], pltpu.HBM))
        return new_momentum[None], new_weight[None], weight_bf16[None]

    return jax.shard_map(local_step, mesh=mesh, in_specs=(P(('mp', 'dp')), P('mp', 'dp'), P('mp', 'dp')), out_specs=(P('mp', 'dp'), P('mp', 'dp'), P('mp')), check_vma=False)
```

```python
import math
import jax
import jax.numpy as jnp
from jax import lax
from jax.experimental import pallas as pl
from jax.experimental.pallas import tpu as pltpu
from jax.sharding import PartitionSpec as P

MOMENTUM = 0.95
LEARN_RATE = 2.0
WEIGHT_DECAY = 0.25
NS_STEPS = 5
COEF_A = 3.4445
COEF_B = -4.7750
COEF_C = 2.0315

MESH = pl.DeviceIdType.MESH
F32, BF16 = jnp.float32, jnp.bfloat16
CORES = 2
BLOCK = 512
CHUNK = 512
DEPTH = 4
KEPT = 4
VMEM_ROOM = 17216 * 2 ** 10
EAGER = 4
EARLY = 1
W_EARLY = 5
OTHERS = ((0, 1), (2, 3, 4))
BLOCKS = (((0, 0), (2, 1), (3, 1), (2, 0), (3, 3)), ((1, 1), (1, 0), (3, 0), (3, 2), (2, 2)))
SQUARES = (((0, 0), (3, 0), (3, 1), (3, 2), (3, 3)), ((1, 1), (1, 0), (2, 0), (2, 1), (2, 2)))
NEAR = (((0, 2), (0, 1), (0, 0)), ((2, 2), (1, 2), (1, 1)))


def block_of(core, index, table=BLOCKS):
    def pick(owner, i):
        values = [block[i] for block in table[owner]]
        if isinstance(index, int):
            return values[index]
        result = jnp.int32(values[0])
        for place, value in enumerate(values[1:], 1):
            result = jnp.where(index == place, jnp.int32(value), result)
        return result
    return tuple(jnp.where(core == 0, pick(0, i), pick(1, i)) for i in range(2))


def diagonal(index):
    return isinstance(index, int) and index in (0, 4)


def span(index, size):
    return pl.ds(pl.multiple_of(index * size, size), size)


def muon(group, rows, half, scale, grad_ref, mom_ref, w_ref, x_ref, gram, parts, nmom_ref, wide_ref, rest_ref, wcol_ref, pair_ref, arrived_ref,
         poly, square_acc, sq_out, sq_in,
         pair_send, pair_recv, rs_send, rs_recv, in_sem, sq_send, sq_recv, up_send, up_recv, mate_send, mate_recv, pass_send, pass_recv,
         far_send, far_recv, share_send, share_recv, part_send, part_recv, gram_send, gram_recv, poly_send, poly_recv,
         w_send, w_recv, w_fwd_send, w_fwd_recv, w_mate_send, w_mate_recv, w_own_sem, tile_sem, out_send, out_recv, row_send, row_recv):
    me = lax.axis_index('dp')
    core, chip = lax.rem(me, CORES), me // CORES
    chips = group // CORES
    slab = rows // group
    partner = chip * CORES + (1 - core)
    side_chip = (lax.rem(chip + 1, chips), lax.rem(chip + chips - 1, chips))
    far_chip = lax.rem(chip + 2, chips)
    num_chunks = half // CHUNK
    slots = num_chunks + 1

    def remote(src, dst, send, recv, device):
        return pltpu.make_async_remote_copy(src, dst, send, recv, device_id={'dp': device}, device_id_type=MESH)

    barrier = pltpu.get_barrier_semaphore()
    for other in range(1, group):
        pl.semaphore_signal(barrier, inc=1, device_id={'dp': lax.rem(me + other, group)}, device_id_type=MESH)
    pl.semaphore_wait(barrier, group - 1)

    def tile(index):
        return parts.at[index // 2, pl.ds(pl.multiple_of(lax.rem(index, 2) * slab, slab), slab), :]

    def staged(side, slot):
        return tile(6 + side * DEPTH + slot)

    def own(index):
        return poly.at[span(index // 4, slab), span(lax.rem(index, 4), CHUNK)]

    def dest_chip(order):
        return jnp.where(order == 0, far_chip, jnp.where(order == 1, side_chip[0], jnp.where(order == 2, side_chip[1], chip)))

    def rows_of(device):
        return span(device, slab)

    def columns(which, j):
        return pl.ds(pl.multiple_of(which * half + j * CHUNK, CHUNK), CHUNK)

    def pair_copy(order, j, which):
        i = (order * num_chunks + j) * 2 + which
        return remote(grad_ref.at[rows_of(dest_chip(order) * CORES + 1 - core), columns(which, j)], pair_ref.at[order, :, columns(which, j)],
                      pair_send.at[i], pair_recv.at[i], partner)

    def pair_start(i, _):
        order, j = i // num_chunks, lax.rem(i, num_chunks)
        for which in (0, 1):
            pair_copy(order, j, which).start()
        return 0
    lax.fori_loop(0, chips * num_chunks, pair_start, 0)

    def grad_loads(order, j, which, base):
        return (pltpu.make_async_copy(grad_ref.at[rows_of(dest_chip(order) * CORES + core), columns(which, j)], tile(base), in_sem.at[base]),
                pltpu.make_async_copy(pair_ref.at[order, :, columns(which, j)], tile(base + 1), in_sem.at[base + 1]))

    def arrived_load(phase, side, j, base):
        return pltpu.make_async_copy(arrived_ref.at[phase, side, j], tile(base), in_sem.at[base])

    def rs_copy(q, side):
        phase, j = q // num_chunks, lax.rem(q, num_chunks)
        slot = lax.rem(q, DEPTH)
        return remote(staged(side, slot), arrived_ref.at[phase, side, j],
                      rs_send.at[side, slot], rs_recv.at[phase, side, j], side_chip[side] * CORES + core)

    def up_copy(side, h, j, sender=None):
        return remote(own(h * num_chunks + j), x_ref.at[j, rows_of(me), :],
                      up_send.at[side, h, j], up_recv.at[side, core if sender is None else sender, j], side_chip[side] * CORES + h)

    def mate_copy(j):
        return remote(own((1 - core) * num_chunks + j), x_ref.at[j, rows_of(me), :], mate_send.at[j], mate_recv.at[j], partner)

    square_acc[...] = jnp.zeros_like(square_acc)

    def send_sums(q):
        phase, j = q // num_chunks, lax.rem(q, num_chunks)
        slot = lax.rem(q, DEPTH)
        for side in (0, 1):
            order = jnp.where(phase == 0, 0, 1 + side)
            which = jnp.where(phase == 1, 1 - side, side)
            pair_copy(order, j, which).wait_recv()
            for load in grad_loads(order, j, which, 3 * side):
                load.start()

            @pl.when(phase == 2)
            def _():
                rs_copy(j, side).wait_recv()
                arrived_load(0, side, j, 3 * side + 2).start()

        for side in (0, 1):
            order = jnp.where(phase == 0, 0, 1 + side)
            which = jnp.where(phase == 1, 1 - side, side)

            @pl.when(q >= DEPTH)
            def _():
                rs_copy(q - DEPTH, side).wait_send()
            for load in grad_loads(order, j, which, 3 * side):
                load.wait()

            @pl.when(phase == 2)
            def _():
                arrived_load(0, side, j, 3 * side + 2).wait()
                staged(side, slot)[...] = (tile(3 * side)[...] + tile(3 * side + 1)[...]) + tile(3 * side + 2)[...]

            @pl.when(phase != 2)
            def _():
                staged(side, slot)[...] = tile(3 * side)[...] + tile(3 * side + 1)[...]
            rs_copy(q, side).start()

    def send_up(j):
        for side in (0, 1):
            for h in range(CORES):
                up_copy(side, h, j).start()
        mate_copy(j).start()

    def finish(j):
        for which in (0, 1):
            pair_copy(3, j, which).wait_recv()
            loads = list(grad_loads(3, j, which, 0))
            for side in (0, 1):
                phase = 2 if side == which else 1
                rs_copy(phase * num_chunks + j, side).wait_recv()
                loads.append(arrived_load(phase, side, j, 2 + side))
            loads.append(pltpu.make_async_copy(mom_ref.at[:, columns(which, j)], tile(4), in_sem.at[4]))
            for load in loads:
                load.start()
            for load in loads:
                load.wait()
            mean = (((tile(0)[...] + tile(1)[...]) + tile(2)[...]) + tile(3)[...]) / group
            momentum = MOMENTUM * tile(4)[...] + mean
            nmom_ref[which * num_chunks + j] = momentum
            update = (mean + MOMENTUM * momentum).astype(BF16)
            own(which * num_chunks + j)[...] = update
            as_float = update.astype(F32)
            square_acc[...] += jnp.sum((as_float * as_float).reshape(slab // 8, 8, CHUNK), axis=0)
        @pl.when(j < EAGER)
        def _():
            send_up(j)

    def reduce_step(q, _):
        @pl.when(q < 3 * num_chunks)
        def _():
            send_sums(q)

        @pl.when(q >= 2 * num_chunks + DEPTH)
        def _():
            finish(q - 2 * num_chunks - DEPTH)
        return 0
    lax.fori_loop(0, 3 * num_chunks + DEPTH, reduce_step, 0)
    for side in (0, 1):
        for last in range(DEPTH):
            rs_copy(3 * num_chunks - DEPTH + last, side).wait_send()

    total = jnp.sum(square_acc[...])
    sq_out[...] = jnp.full(sq_out.shape, total, F32)
    sq_in[me] = jnp.full(sq_out.shape, total, F32)

    def sq_copy(other):
        return remote(sq_out, sq_in.at[me], sq_send.at[other], sq_recv.at[other], lax.rem(me + other, group))
    for other in range(1, group):
        sq_copy(other).start()

    def send_rest(j, _):
        send_up(j)
        return 0
    lax.fori_loop(EAGER, num_chunks, send_rest, 0)
    for other in range(1, group):
        sq_copy(other).wait()
    square = sq_in[0, 0:1, 0:1]
    for i in range(1, group):
        square = square + sq_in[i, 0:1, 0:1]
    inverse = 1.0 / (jnp.sqrt(square) + 1e-7)

    def normalise(j, row0, size):
        r = pl.ds(pl.multiple_of(row0, slab), size)
        x_ref[j, r, :] = (x_ref[j, r, :].astype(F32) * inverse).astype(BF16)

    def pass_copy(side, c):
        where = x_ref.at[c, rows_of(side_chip[1 - side] * CORES + side), :]
        return remote(where, where, pass_send.at[side, c], pass_recv.at[side, c], side_chip[side] * CORES + core)

    def w_first(side, h, c, sender=None):
        return remote(w_ref.at[:, columns(h, c)], wcol_ref.at[c, chip, span(core, slab), :],
                      w_send.at[side, h, c], w_recv.at[side, core if sender is None else sender, c], side_chip[side] * CORES + h)

    def w_forward(side, c):
        where = wcol_ref.at[c, side_chip[1 - side], pl.ds(side * slab, slab), :]
        return remote(where, where, w_fwd_send.at[side, c], w_fwd_recv.at[side, c], side_chip[side] * CORES + core)

    def w_pair(c):
        return remote(w_ref.at[:, columns(1 - core, c)], wcol_ref.at[c, chip, span(core, slab), :], w_mate_send.at[c], w_mate_recv.at[c], partner)

    def w_own(c):
        return pltpu.make_async_copy(w_ref.at[:, columns(core, c)], wcol_ref.at[c, chip, span(core, slab), :], w_own_sem.at[c])

    def w_pass(c):
        for side in (0, 1):
            w_first(side, 0, c, side).wait_recv()
            w_forward(side, c).start()

    def w_ready(c):
        for side in (0, 1):
            w_first(side, 0, c, 1 - side).wait_recv()
            w_forward(side, c).wait_recv()
        w_pair(c).wait_recv()
        w_own(c).wait()

    def slot_of(c, t):
        return lax.rem(c + 2 * slots - t, slots)

    def gram_copy(b, index, row, col):
        where = gram.at[span(row, BLOCK), span(col, BLOCK)]
        return remote(where, where, gram_send.at[index, b], gram_recv.at[index, b], partner)

    def poly_copy(b, index, row, col):
        where = poly.at[span(row, BLOCK), span(col, BLOCK)]
        return remote(where, where, poly_send.at[index, b], poly_recv.at[index, b], partner)

    def both(copy, owner, index, act, table=BLOCKS):
        row, col = block_of(owner, index, table)
        if not diagonal(index):
            act(copy(1, index, col, row))
        act(copy(0, index, row, col))

    def start(copy):
        copy.start()

    def arrived(copy):
        copy.wait_recv()

    def left(copy):
        copy.wait_send()

    def part_copy(index):
        return remote(parts.at[index], parts.at[5 + index], part_send.at[index], part_recv.at[index], partner)

    small = BLOCK // 2
    ROWS_ROWS = (((1,), (1,)), ((), ()))

    def product(rows_at, index, row, col):
        def rows_rows(left, right):
            terms = [lax.dot_general(a, b, ROWS_ROWS, preferred_element_type=F32) for a, b in zip(rows_at(*left), rows_at(*right))]
            return sum(terms[1:], terms[0])
        if diagonal(index):
            low = rows_rows((row, small, small), (row, 0, BLOCK))
            top = rows_rows((row, 0, small), (row, 0, small))
            return jnp.concatenate([top, low[:, :small]], axis=0), low[:, small:]
        return (rows_rows((row, 0, BLOCK), (col, 0, BLOCK)),)

    def pieces_of(ref, value):
        if len(value) == 2:
            return (ref[:, 0:small], ref[small:, small:])
        return (ref[...],)

    def turn_poly(index):
        row, col = block_of(1 - core, index, SQUARES)
        poly[span(col, BLOCK), span(row, BLOCK)] = poly[span(row, BLOCK), span(col, BLOCK)].T

    def put_block(ref, row, col, value):
        if len(value) == 2:
            at = ref.at[span(row, BLOCK), span(row, BLOCK)]
            left, corner = (v.astype(BF16) for v in value)
            at[:, 0:small] = left
            at[small:, small:] = corner
            at[0:small, small:] = left[small:].T
        else:
            block = value[0].astype(BF16)
            ref[span(row, BLOCK), span(col, BLOCK)] = block
            ref[span(col, BLOCK), span(row, BLOCK)] = block.T

    def x_rows(t):
        def rows_at(block, offset, size):
            r = pl.ds(pl.multiple_of(block * BLOCK + offset, small), size)
            return (x_ref[slot_of(c, t), r, :] for c in range(num_chunks))
        return rows_at

    def gram_rows(block, offset, size):
        return (gram[pl.ds(pl.multiple_of(block * BLOCK + offset, small), size), :],)

    def near_chip(order):
        return (chip, side_chip[0], side_chip[1])[order]

    def near_block(one, two):
        one, two = near_chip(one), near_chip(two)
        return jnp.maximum(one, two), jnp.minimum(one, two)

    def near_owned(owner, place):
        rows_cols = [(near_block(*NEAR[c][place])) for c in range(CORES)]
        return tuple(jnp.where(owner == 0, rows_cols[0][i], rows_cols[1][i]) for i in range(2))

    def near_sum(j, place):
        row, col = near_owned(jnp.where(place < 3, 1 - core, core), place % 3)
        value = lax.dot_general(x_ref[j, span(row, BLOCK), :], x_ref[j, span(col, BLOCK), :], (((1,), (1,)), ((), ())), preferred_element_type=F32)
        slot = place % 3 + 8 * (place // 3)

        if isinstance(j, int):
            parts[slot] = parts[slot] + value
            return

        @pl.when(j == 0)
        def _():
            parts[slot] = value

        @pl.when(j > 0)
        def _():
            parts[slot] = parts[slot] + value

    def near_copy(place, b):
        row, col = near_owned(core, place)
        if b == 1:
            row, col = col, row
        where = gram.at[span(row, BLOCK), span(col, BLOCK)]
        return remote(where, where, gram_send.at[place, b], gram_recv.at[place, b], partner)

    def near_both(place, act):
        act(near_copy(place, 0))
        row, col = near_owned(core, place)

        @pl.when(row != col)
        def _():
            act(near_copy(place, 1))

    def near_arrived(place):
        near_copy(place, 0).wait_recv()
        row, col = near_owned(1 - core, place)

        @pl.when(row != col)
        def _():
            near_copy(place, 1).wait_recv()

    def land(j):
        x_ref[j, rows_of(me), :] = (own(core * num_chunks + j)[...].astype(F32) * inverse).astype(BF16)
        mate_copy(j).wait_recv()
        normalise(j, partner * slab, slab)
        for side in (0, 1):
            for from_core in range(CORES):
                up_copy(side, core, j, from_core).wait_recv()
            normalise(j, side_chip[1 - side] * CORES * slab, CORES * slab)

    def arrive(j, _):
        land(j)
        for place in range(6):
            near_sum(j, place)
        return 0

    def far_block(chip_index, core_index, side):
        right, behind = lax.rem(chip_index + 1, chips), lax.rem(chip_index + chips - 1, chips)
        if side == 1:
            one, two = jnp.where(core_index == 0, chip_index, behind), right
        else:
            one, two = jnp.where(core_index == 0, chip_index, behind), behind
        return jnp.maximum(one, two), jnp.minimum(one, two)

    def far_copy(side):
        row, col = far_block(chip, core, side)
        where = gram.at[span(row, BLOCK), span(col, BLOCK)]
        return remote(where, where, far_send.at[side], far_recv.at[side], side_chip[side] * CORES + core)

    def share_copy(side, owner):
        row, col = far_block(side_chip[1 - side], owner, side)
        where = gram.at[span(row, BLOCK), span(col, BLOCK)]
        return remote(where, where, share_send.at[side], share_recv.at[side], partner)

    def turn(side, owner):
        row, col = far_block(side_chip[1 - side], owner, side)

        @pl.when(row != col)
        def _():
            gram[span(col, BLOCK), span(row, BLOCK)] = gram[span(row, BLOCK), span(col, BLOCK)].T

    lax.fori_loop(0, num_chunks - 1, arrive, 0)
    land(num_chunks - 1)
    for place in range(3):
        near_sum(num_chunks - 1, place)
        part_copy(place).start()
    for place in range(3, 6):
        near_sum(num_chunks - 1, place)

    def sent(j, _):
        for side in (0, 1):
            for h in range(CORES):
                up_copy(side, h, j).wait_send()
        mate_copy(j).wait_send()
        return 0
    lax.fori_loop(0, num_chunks, sent, 0)


    for c in range(EARLY):
        for side in (0, 1):
            pass_copy(side, c).start()
    for place in range(3):
        part_copy(place).wait_recv()
        row, col = near_owned(core, place)
        block = (parts[8 + place] + parts[5 + place]).astype(BF16)
        gram[span(row, BLOCK), span(col, BLOCK)] = block
        if place < 2:
            far_copy(place).start()

        @pl.when(row != col)
        def _():
            gram[span(col, BLOCK), span(row, BLOCK)] = block.T
        near_both(place, start)
    for c in range(EARLY, num_chunks):
        for side in (0, 1):
            pass_copy(side, c).start()

    def w_start(c, _):
        for h in range(CORES):
            for side in (0, 1):
                w_first(side, h, c).start()
        w_pair(c).start()
        w_own(c).start()
        return 0
    lax.fori_loop(0, num_chunks, w_start, 0)
    for place in range(3):
        near_arrived(place)
    for side in (0, 1):
        far_copy(side).wait_recv()
        share_copy(side, core).start()
    for side in (0, 1):
        turn(side, core)
    for side in (0, 1):
        share_copy(side, 1 - core).wait_recv()
        turn(side, 1 - core)
    for side in (0, 1):
        far_copy(side).wait_send()
        share_copy(side, core).wait_send()
    for place in range(3):
        near_both(place, left)
        part_copy(place).wait_send()

    tall = 1024
    decay, step_size = 1.0 - LEARN_RATE * WEIGHT_DECAY, LEARN_RATE * scale

    def step(t, _):
        def pass_weights(low, high):
            @pl.when(t == NS_STEPS - 2)
            def _():
                def one(c, _):
                    w_pass(c)
                    return 0
                lax.fori_loop(low, high, one, 0)
        pass_weights(0, W_EARLY)

        def gram_other(*indices):
            for index in indices:
                row, col = block_of(1 - core, index)
                value = product(x_rows(t), index, row, col)
                if len(value) == 2:
                    parts[index, :, 0:small] = value[0]
                    parts[index, small:, small:] = value[1]
                else:
                    parts[index] = value[0]
            for index in indices:
                part_copy(index).start()

        def gram_own(*indices):
            for index in indices:
                part_copy(index).wait_recv()
            for index in indices:
                row, col = block_of(core, index)
                value = product(x_rows(t), index, row, col)
                put_block(gram, row, col, tuple(v + w for v, w in zip(value, pieces_of(parts.at[5 + index], value))))
            for index in indices:
                both(gram_copy, core, index, start)

        def gram_middle(index, _):
            gram_own(index)
            return 0
        later = jnp.minimum(t, 1)

        def alone(act, *indices):
            def once(_, carry):
                act(*indices)
                return carry
            lax.fori_loop(0, later, once, None)
        for group_of in OTHERS:
            alone(gram_other, *group_of)
        alone(gram_own, 0, 1)

        @pl.when(t > 0)
        def _():
            lax.fori_loop(2, 4, gram_middle, 0)
        alone(gram_own, 4)

        def once(owner, index, act):
            row, col = block_of(owner, index, SQUARES)
            act(poly_copy(0, index, row, col))

        always = jnp.minimum(t + 1, 1)

        def squares(indices, needs):
            @pl.when(t > 0)
            def _():
                for index in needs:
                    both(gram_copy, 1 - core, index, arrived)
            if 4 in indices:
                once(1 - core, 1, arrived)

            def take(_, carry):
                for index in indices:
                    row, col = block_of(core, index, SQUARES)
                    value = product(gram_rows, index, row, col)
                    old = pieces_of(gram.at[span(row, BLOCK), span(col, BLOCK)], value)
                    put_block(poly, row, col, tuple(COEF_B * g.astype(F32) + COEF_C * v for g, v in zip(old, value)))
                    if index == 4:
                        turn_poly(1)
                return carry
            lax.fori_loop(0, always, take, None)
            for index in indices:
                once(core, index, start)
        def part_drain(i, carry):
            part_copy(i).wait_send()
            return carry
        pl.when(t > 0)(lambda: lax.fori_loop(0, 5, part_drain, None))

        squares((0,), (0, 1, 2))
        squares((1, 2), (3,))
        squares((3,), (4,))

        @pl.when((t == NS_STEPS - 1) & (t > 0))
        def _():
            for index in range(5):
                both(gram_copy, core, index, left)
        squares((4,), ())

        def tile_load(q):
            c, m = q // 2, lax.rem(q, 2)
            slot = lax.rem(q, 2)
            return pltpu.make_async_copy(wcol_ref.at[c, pl.ds(2 * m, 2)], parts.at[pl.ds(2 * slot, 2)], tile_sem.at[slot])

        @pl.when(t == NS_STEPS - 1)
        def _():
            w_ready(0)
            tile_load(0).start()
            tile_load(1).start()

        def far_ready(c):
            @pl.when(t == 0)
            def _():
                for side in (0, 1):
                    pass_copy(side, c).wait()

        def apply_rows(c, r):
            src = slot_of(c, t)
            total = jnp.dot(poly[r, :], x_ref[src], preferred_element_type=F32)
            x_ref[slot_of(c, t + 1), r, :] = (COEF_A * x_ref[src, r, :].astype(F32) + total).astype(BF16)
        far_ready(0)
        once(1 - core, 0, arrived)
        once(1 - core, 2, arrived)
        turn_poly(2)
        once(1 - core, 3, arrived)
        turn_poly(3)
        apply_rows(0, slice(0, BLOCK))
        pass_weights(W_EARLY, num_chunks)
        once(1 - core, 4, arrived)
        apply_rows(0, slice(BLOCK, tall))
        apply_rows(0, slice(tall, rows))

        @pl.when(t < NS_STEPS - 1)
        def _():
            def apply_chunk(c, _):
                far_ready(c)
                for half_rows in range(2):
                    apply_rows(c, slice(half_rows * tall, (half_rows + 1) * tall))
                return 0
            lax.fori_loop(1, num_chunks, apply_chunk, 0)

        @pl.when(t == NS_STEPS - 1)
        def _():
            def out_copy(q, act):
                c, m = q // 2, lax.rem(q, 2)
                new = x_ref.at[slot_of(c, t + 1), span(m, tall), :]

                @pl.when(c < KEPT)
                def _():
                    act(remote(new, gram.at[span(m, tall), span(c, CHUNK)], out_send.at[q], out_recv.at[q], partner))

                @pl.when((c >= KEPT) & (c < num_chunks - 1))
                def _():
                    act(remote(new, wide_ref.at[c - KEPT, span(m, tall), :], out_send.at[q], out_recv.at[q], partner))

                @pl.when(c == num_chunks - 1)
                def _():
                    act(remote(new, rest_ref.at[span(m, tall), :], out_send.at[q], out_recv.at[q], partner))

            def kept_rows(which, c):
                place = which * num_chunks + c
                return parts.at[4 + place // 2, pl.ds(pl.multiple_of(lax.rem(place, 2) * slab, slab), slab), :]

            def row_copy(c):
                return remote(parts.at[11, span(lax.rem(c, 2), slab), :], kept_rows(core, c), row_send.at[c], row_recv.at[c], partner)

            def new_rows(c, tile_index, owner):
                old = parts[tile_index, span(owner, slab), :]
                ortho = x_ref[slot_of(c, t + 1), span(chip * CORES + owner, slab), :]
                return decay * old - step_size * ortho.astype(F32)

            def new_weight(q):
                c, m = q // 2, lax.rem(q, 2)
                slot = lax.rem(q, 2)
                tile_load(q).wait()

                @pl.when(m == chip // 2)
                def _():
                    kept_rows(core, c)[...] = new_rows(c, 2 * slot + lax.rem(chip, 2), core)

                    @pl.when(c >= 2)
                    def _():
                        row_copy(c - 2).wait_send()
                    parts[11, span(lax.rem(c, 2), slab), :] = new_rows(c, 2 * slot + lax.rem(chip, 2), 1 - core)
                    row_copy(c).start()
                old = parts[pl.ds(2 * slot, 2)].reshape(tall, CHUNK)
                dst = slot_of(c, t + 1)
                x_ref[dst, span(m, tall), :] = (decay * old - step_size * x_ref[dst, span(m, tall), :].astype(F32)).astype(BF16)
                out_copy(q, start)

            def next_tile(q):
                @pl.when(q + 2 < 2 * num_chunks)
                def _():
                    pl.when(lax.rem(q, 2) == 0)(lambda: w_ready(q // 2 + 1))
                    tile_load(q + 2).start()

            def last_step(q, _):
                if NS_STEPS == 1:
                    pl.when(lax.rem(q, 2) == 0)(lambda: far_ready(q // 2))
                apply_rows(q // 2, span(lax.rem(q, 2), tall))
                new_weight(q)
                next_tile(q)
                return 0

            def first_tiles(q, _):
                new_weight(q)
                next_tile(q)
                return 0
            lax.fori_loop(0, 2, first_tiles, 0)
            lax.fori_loop(2, 2 * num_chunks, last_step, 0)

            def out_end(q, _):
                out_copy(q, lambda copy: copy.wait())
                return 0
            lax.fori_loop(0, 2 * num_chunks, out_end, 0)
            for c in range(num_chunks):
                if c >= num_chunks - 2:
                    row_copy(c).wait_send()
                row_copy(c).wait_recv()

        for index in range(5):
            @pl.when((t > 0) & (t < NS_STEPS - 1))
            def _():
                both(gram_copy, core, index, left)
            once(core, index, left)
        return 0
    lax.fori_loop(0, NS_STEPS, step, 0)

    def w_end(c, _):
        for side in (0, 1):
            for h in range(CORES):
                w_first(side, h, c).wait_send()
            w_forward(side, c).wait_send()
        w_pair(c).wait_send()
        return 0
    lax.fori_loop(0, num_chunks, w_end, 0)

    def paired(i, _):
        order, j = i // num_chunks, lax.rem(i, num_chunks)
        for which in (0, 1):
            pair_copy(order, j, which).wait_send()
        return 0
    lax.fori_loop(0, chips * num_chunks, paired, 0)


def hand_over(half, x_ref, gram, parts, nmom_ref, wide_ref, rest_ref, wide_out, nmom_out, weight_out, rest, wide_sem, load_sem, nmom_sem, weight_sem):
    core = lax.rem(lax.axis_index('dp'), CORES)
    slab = nmom_ref.shape[1]
    num_chunks = half // CHUNK
    slots = num_chunks + 1

    def columns(which, c):
        return pl.ds(pl.multiple_of(which * half + c * CHUNK, CHUNK), CHUNK)
    load = pltpu.make_async_copy(rest_ref, rest, load_sem)
    load.start()
    stores = []
    for c in range(num_chunks):
        stores.append(pltpu.make_async_copy(x_ref.at[(c + 2 * slots - NS_STEPS) % slots], wide_out.at[:, columns(core, c)], wide_sem.at[0, c]))
        there = gram.at[:, span(c, CHUNK)] if c < KEPT else wide_ref.at[c - KEPT] if c < num_chunks - 1 else rest
        stores.append(pltpu.make_async_copy(there, wide_out.at[:, columns(1 - core, c)], wide_sem.at[1, c]))
    last = stores.pop()
    for place in range(CORES * num_chunks):
        where = (slice(None), pl.ds(place * CHUNK, CHUNK))
        stores.append(pltpu.make_async_copy(nmom_ref.at[place], nmom_out.at[where], nmom_sem.at[place]))
        stores.append(pltpu.make_async_copy(parts.at[4 + place // 2, pl.ds(place % 2 * slab, slab), :], weight_out.at[where], weight_sem.at[place]))
    for store in stores:
        store.start()
    load.wait()
    last.start()
    for store in stores + [last]:
        store.wait()


def solution(mesh):
    group = mesh.shape['dp']

    def local_step(grad_part, momentum, weight):
        slab, num_cols = weight.shape[1:]
        rows = slab * group
        half = num_cols // CORES
        scale = 0.2 * math.sqrt(max(rows, num_cols))
        num_chunks = half // CHUNK
        chips = group // CORES
        anywhere = pl.BlockSpec(memory_space=pl.ANY)
        dma = pltpu.SemaphoreType.DMA
        shape = jax.ShapeDtypeStruct

        def kernel(*refs):
            muon(group, rows, half, scale, *refs)
        kept = pl.BlockSpec(memory_space=pltpu.VMEM)
        outs = pl.pallas_call(
            kernel,
            name='muon',
            out_shape=(pltpu.VMEM((num_chunks + 1, rows, CHUNK), BF16), pltpu.VMEM((rows, rows), BF16), pltpu.VMEM((12, BLOCK, BLOCK), F32),
                       pltpu.VMEM((CORES * num_chunks, slab, CHUNK), F32), pltpu.VMEM((num_chunks - 1 - KEPT, rows, CHUNK), BF16), pltpu.HBM((rows, CHUNK), BF16),
                       shape((num_chunks, chips, CORES * slab, CHUNK), F32), shape((chips, slab, num_cols), F32),
                       shape((3, 2, num_chunks, slab, CHUNK), F32)),
            in_specs=[anywhere] * 3,
            out_specs=(kept,) * 5 + (anywhere,) * 4,
            scratch_shapes=[
                pltpu.VMEM((rows, rows), BF16),
                pltpu.VMEM((8, CHUNK), F32),
                pltpu.VMEM((8, 128), F32),
                pltpu.VMEM((group, 8, 128), F32),
                dma((chips * num_chunks * 2,)), dma((chips * num_chunks * 2,)), dma((2, DEPTH)), dma((3, 2, num_chunks)), dma((6,)),
                dma((group,)), dma((group,)), dma((2, 2, num_chunks)), dma((2, 2, num_chunks)), dma((num_chunks,)), dma((num_chunks,)),
                dma((2, num_chunks)), dma((2, num_chunks)), dma((2,)), dma((2,)), dma((2,)), dma((2,)),
                dma((5,)), dma((5,)), dma((5, 2)), dma((5, 2)), dma((5, 2)), dma((5, 2)),
                dma((2, 2, num_chunks)), dma((2, 2, num_chunks)), dma((2, num_chunks)), dma((2, num_chunks)),
                dma((num_chunks,)), dma((num_chunks,)), dma((num_chunks,)), dma((2,)),
                dma((2 * num_chunks,)), dma((2 * num_chunks,)), dma((num_chunks,)), dma((num_chunks,)),
            ],
            compiler_params=pltpu.CompilerParams(collective_id=1, has_side_effects=True, vmem_limit_bytes=VMEM_ROOM),
        )(grad_part[0, 0], momentum[0], weight[0])

        def last_kernel(*refs):
            hand_over(half, *refs)
        weight_bf16, new_momentum, new_weight = pl.pallas_call(
            last_kernel,
            name='hand_over',
            out_shape=(shape((rows, num_cols), BF16), shape((slab, num_cols), F32), shape((slab, num_cols), F32)),
            in_specs=[kept] * 5 + [pl.BlockSpec(memory_space=pltpu.HBM)],
            out_specs=(anywhere,) * 3,
            scratch_shapes=[
                pltpu.VMEM((rows, CHUNK), BF16),
                dma((CORES, num_chunks)), dma(()), dma((CORES * num_chunks,)), dma((CORES * num_chunks,)),
            ],
            compiler_params=pltpu.CompilerParams(vmem_limit_bytes=VMEM_ROOM),
        )(*(pltpu.with_memory_space_constraint(out, pltpu.VMEM) for out in outs[:5]), pltpu.with_memory_space_constraint(outs[5], pltpu.HBM))
        return new_momentum[None], new_weight[None], weight_bf16[None]

    return jax.shard_map(local_step, mesh=mesh, in_specs=(P(('mp', 'dp')), P('mp', 'dp'), P('mp', 'dp')), out_specs=(P('mp', 'dp'), P('mp', 'dp'), P('mp')), check_vma=False)
```
